32 devices in a mesh: wide: 8 (over z, core), narrow: 4 (over y, x).
Axes of the slice: x: 2, y: 2, z: 4, core: 2. Of those that a mesh axis runs over, the one named last changes fastest.
Arguments:
- activations: bfloat16 [512, 16384], P(None, 'wide'), may hold values from -6 to 6
- enc_weight: bfloat16 [16384, 4096], P('wide', 'narrow'), may hold values from -0.046875 to 0.046875
- enc_bias: float32 [4096], P('narrow'), may hold values from -4 to 4
- dec_weight: bfloat16 [4096, 16384], P('narrow', 'wide'), may hold values from -0.375 to 0.375
- dec_bias: float32 [16384], P('wide'), may hold values from -4 to 4
- active_ids: int32 [512, 64], replicated, may hold values from 0 to 4095, all different within a row
Outputs:
- dec_grad: bfloat16 [4096, 16384], P('narrow', 'wide')
- latent_grad: float32 [512, 4096], P('wide', 'narrow')
The draws below stay inside these ranges and needn't reach their ends.
Inputs may be any that keep to these rules, and one draw needn't show every extreme that they name: `active_ids`: each row names 64 different latents; every latent is named by some row.
All inputs are finite; a program needn't handle non-finite values.
Results may differ from the reference program's by a relative error of at most 0.0058.
Values may be sent and summed in bfloat16 or wider, within the bound.
A program may use at most 128 MiB of HBM per device.

```python
import jax
import jax.numpy as jnp
from jax import lax

LAT_DEV = 1024
K = 64
TOKENS = 512
CHANNELS = 16384
GROUPS = 4
LATENTS = 4096


def steps_of(rng, shape, shards, least, top_value):
    loudness = 1.0
    for axis_at, parts in shards:
        heights = jax.random.uniform(jax.random.fold_in(jax.random.fold_in(rng, 6), axis_at), (parts,), jnp.float32, least / len(shards), top_value / len(shards))
        loudness = loudness * jnp.repeat(jnp.exp(heights), shape[axis_at] // parts).reshape((-1,) + (1,) * (len(shape) - 1 - axis_at))
    return loudness


def picks_of(key, rows, amount, top, lift):
    sequence = jax.random.permutation(jax.random.fold_in(key, 1), amount)
    favour = sequence
    for power in range(3):
        favour = favour * favour // amount
    favour = favour * lift // amount
    tickets = jax.random.randint(jax.random.fold_in(key, 2), (rows, amount), 0, 4096) + favour
    sure = jax.random.permutation(jax.random.fold_in(key, 3), rows)[jnp.arange(amount) % rows]
    tickets = jnp.where(jnp.arange(rows)[:, None] == sure[None, :], 1 << 14, tickets)
    merit = tickets * amount + jnp.arange(amount)
    return lax.top_k(merit.astype(jnp.int32), top)[1].astype(jnp.int32)


def normal_values(rng, dims, spread, bound, split=(), kind=jnp.bfloat16):
    array = jax.random.normal(rng, dims, jnp.float32) * spread
    if len(split) > 0:
        array = steps_of(rng, dims, split, -0.22, 0.18) * array
    return jnp.clip(array, min=-bound, max=bound).astype(kind)


def setup_inputs(seed: int = 0) -> dict:
    splits = jax.random.split(jax.random.key(seed), 7)
    return {
        "activations": normal_values(splits[0], (TOKENS, CHANNELS), 1.0, 6.0, ((1, 8),)),
        "enc_weight": normal_values(splits[1], (CHANNELS, LATENTS), CHANNELS ** -0.5, 0.046875, ((0, 8), (1, 4))),
        "enc_bias": normal_values(splits[2], (LATENTS,), 0.3, 4.0, ((0, 4),), jnp.float32),
        "dec_weight": normal_values(splits[3], (LATENTS, CHANNELS), 256 ** -0.5, 0.375, ((0, 4), (1, 8))),
        "dec_bias": normal_values(splits[4], (CHANNELS,), 0.3, 4.0, ((0, 8),), jnp.float32),
        "active_ids": picks_of(splits[5], TOKENS, LATENTS, K, 256),
    }


def reference(activations, enc_weight, enc_bias, dec_weight, dec_bias, active_ids):
    token_count = activations.shape[0]
    preact = jnp.dot(activations, enc_weight, preferred_element_type=jnp.float32) + enc_bias.astype(jnp.float32)
    row_index = jnp.arange(token_count, dtype=jnp.int32)[:, None]
    active_mask = jnp.zeros(preact.shape, jnp.float32).at[row_index, active_ids].set(1.0)
    latents = (active_mask * preact).astype(jnp.bfloat16)
    target = activations.astype(jnp.float32)
    dec_shift = dec_bias.astype(jnp.float32)
    group_list = jnp.arange(GROUPS, dtype=jnp.int32)

    def pieces(group_index):
        first_latent = (group_index * LAT_DEV).astype(jnp.int32)
        latent_cols = lax.dynamic_slice_in_dim(latents, first_latent, LAT_DEV, 1)
        dec_rows = lax.dynamic_slice_in_dim(dec_weight, first_latent, LAT_DEV, 0)
        mask_cols = lax.dynamic_slice_in_dim(active_mask, first_latent, LAT_DEV, 1)
        recon_part = jnp.dot(latent_cols, dec_rows, preferred_element_type=jnp.float32)
        return latent_cols, dec_rows, mask_cols, recon_part

    nothing = jnp.zeros(target.shape, jnp.float32)

    def first_pass(carry, group_index):
        running, summed = carry
        running = running + pieces(group_index)[3]
        return (running, summed + running), None

    (unused_run, summed), unused_out = lax.scan(first_pass, (nothing, nothing), group_list)
    total_recon = summed + GROUPS * dec_shift

    def second_pass(carry, group_index):
        running, before = carry
        latent_cols, dec_rows, mask_cols, recon_part = pieces(group_index)
        running = running + recon_part
        recon_here = dec_shift + running
        remaining = (GROUPS - group_index).astype(jnp.float32)
        suffix = total_recon - before - remaining * target
        errors = (suffix / GROUPS).astype(jnp.bfloat16)
        grad_rows = lax.dot_general(latent_cols, errors, (((0,), (0,)), ((), ())), preferred_element_type=jnp.float32).astype(jnp.bfloat16)
        grad_cols = mask_cols * lax.dot_general(errors, dec_rows, (((1,), (1,)), ((), ())), preferred_element_type=jnp.float32)
        return (running, before + recon_here), (grad_rows, grad_cols)

    unused_carry, (grad_stack, latent_stack) = lax.scan(second_pass, (nothing, nothing), group_list)
    dec_grad = grad_stack.reshape(GROUPS * LAT_DEV, target.shape[1])
    latent_grad = jnp.transpose(latent_stack, (1, 0, 2)).reshape(token_count, GROUPS * LAT_DEV)
    return dec_grad, latent_grad
```

```python
import functools

import jax
import jax.numpy as jnp
from jax import lax
from jax.experimental import pallas as pl
from jax.experimental.pallas import tpu as pltpu
from jax.sharding import PartitionSpec as P

LANES = 128
MESH = pl.DeviceIdType.MESH
F32, BF16 = jnp.float32, jnp.bfloat16


def lookup(table, index):
    return jnp.take_along_axis(table, index, axis=1, mode="promise_in_bounds")


def pick(tables, ids, fold, top):
    tile, lane = ids >> 7, ids & (LANES - 1)
    half = lax.broadcasted_iota(jnp.int32, ids.shape, 1) // top
    picked = jnp.zeros(ids.shape, F32)
    for part in range(fold):
        here = jnp.where(half == part, tile, -1)
        for j, table in enumerate(tables(part)):
            picked = jnp.where(here == j, lookup(table, lane), picked)
    return picked


def step_kernel(
    W, N, fold, top, chunk, pieces,
    ids_t_ref, bias_ref, shift_ref, act_hbm, enc_hbm, dec_hbm,
    dg_ref, grad_ref,
    ids, act, enc, dec, slot, total, mine, part, wide_in, values, lat, lat_t,
    rec, rec_in, err_out, err, lg_packed, grad_in,
    load_sem, ws1, wr1, ws2, wr2, ws3, wr3, ns1, nr1, ns2, nr2,
):
    wide, narrow = lax.axis_index("wide"), lax.axis_index("narrow")
    tokens, latents = lat.shape
    channels = act.shape[1]
    own, rows = tokens // N, part.shape[1]
    chunks = channels // chunk
    piece = latents // pieces
    low = narrow * latents

    def piece_cols(n):
        return pl.ds(pl.multiple_of(n * piece, LANES), piece)

    load_act = pltpu.make_async_copy(act_hbm, act, load_sem.at[0])
    load_dec = pltpu.make_async_copy(dec_hbm, dec, load_sem.at[1])

    def load_enc(n):
        return pltpu.make_async_copy(enc_hbm.at[:, piece_cols(n)], enc.at[:, piece_cols(n)], load_sem.at[2 + n])

    load_act.start()
    for n in range(pieces):
        load_enc(n).start()
    load_dec.start()

    barrier = pltpu.get_barrier_semaphore()
    for d in range(1, W):
        pl.semaphore_signal(barrier, inc=1, device_id={"wide": lax.rem(wide + d, W)}, device_id_type=MESH)
    for d in range(1, N):
        pl.semaphore_signal(barrier, inc=1, device_id={"narrow": lax.rem(narrow + d, N)}, device_id_type=MESH)

    stacked = jnp.concatenate([ids_t_ref[...]] * fold, axis=0) - low
    ids[...] = stacked.T

    GROUP = 16
    groups = tokens // GROUP

    def slots_of(i, carry):
        at = pl.ds(pl.multiple_of(i * GROUP, GROUP), GROUP)
        mine_ids = ids[at, :]
        place = lax.broadcasted_iota(jnp.int32, (GROUP, LANES), 1)
        places = [(place + j * LANES).astype(jnp.int16) for j in range(latents // LANES)]
        found = [jnp.full((GROUP, LANES), -1, jnp.int16) for _ in places]
        for k in range(top):
            here = jnp.broadcast_to(mine_ids[:, k : k + 1], (GROUP, LANES)).astype(jnp.int16)
            found = [jnp.where(here == p, jnp.int16(k), f) for p, f in zip(places, found)]
        for j, f in enumerate(found):
            slot[at, j * LANES : (j + 1) * LANES] = f
        return carry

    lax.fori_loop(0, groups // 4, slots_of, 0)

    load_act.wait()

    def encode(n, carry):
        pltpu.make_async_copy(enc_hbm.at[:, piece_cols(n)], enc.at[:, piece_cols(n)], load_sem.at[2 + n]).wait()
        total[:, piece_cols(n)] = jnp.dot(act[...], enc[:, piece_cols(n)], preferred_element_type=F32)
        return carry

    lax.fori_loop(0, pieces, encode, 0)

    half = lax.broadcasted_iota(jnp.int32, (rows, LANES), 1) // top

    def packed_ids(w):
        out = ids[pl.ds(pl.multiple_of(w * (rows * fold), rows), rows), :]
        for p in range(1, fold):
            other = ids[pl.ds(pl.multiple_of((w * fold + p) * rows, rows), rows), :]
            out = jnp.where(half == p, other, out)
        return out

    def pick_dense(w):
        def tables(p):
            at = pl.ds(pl.multiple_of((w * fold + p) * rows, rows), rows)
            return [total[at, j * LANES : (j + 1) * LANES] for j in range(latents // LANES)]

        return pick(tables, packed_ids(w), fold, top)

    def pick_block(w, carry):
        picked = pick_dense(w)
        mine[w] = picked
        part[w] = picked.astype(BF16)
        return carry

    lax.fori_loop(0, W, pick_block, 0)

    pl.semaphore_wait(barrier, W + N - 2)

    def wide_copy(d, source, target, send, recv):
        return pltpu.make_async_remote_copy(
            src_ref=source, dst_ref=target, send_sem=send.at[d], recv_sem=recv.at[d],
            device_id={"wide": lax.rem(wide + d, W)}, device_id_type=MESH,
        )

    def scatter_copy(d, source, target, send, recv):
        return wide_copy(d, source.at[lax.rem(wide + d, W)], target.at[d], send, recv)

    for d in range(1, W):
        scatter_copy(d, part, wide_in, ws1, wr1).start()

    def bias_tables(p):
        return [jnp.broadcast_to(bias_ref[:, j * LANES : (j + 1) * LANES], (rows, LANES)) for j in range(latents // LANES)]

    summed = mine[wide] + pick(bias_tables, packed_ids(wide), fold, top)

    lax.fori_loop(groups // 4, groups * 5 // 8, slots_of, 0)

    for d in range(1, W):
        scatter_copy(d, part, wide_in, ws1, wr1).wait_recv()
        summed = summed + wide_in[d].astype(F32)
    values[wide] = summed.astype(BF16)
    for d in range(1, W):
        wide_copy(d, values.at[wide], values.at[wide], ws2, wr2).start()

    lax.fori_loop(groups * 5 // 8, groups, slots_of, 0)
    for d in range(1, W):
        wide_copy(d, values.at[wide], values.at[wide], ws2, wr2).wait_recv()

    def spread(table, block, p):
        at = pl.ds(pl.multiple_of((block * fold + p) * rows, rows), rows)
        out = []
        for j in range(latents // LANES):
            index = slot[at, j * LANES : (j + 1) * LANES].astype(jnp.int32)
            found = lookup(table, jnp.maximum(index, 0) + p * top)
            out.append(jnp.where(index >= 0, found, 0.0))
        return jnp.concatenate(out, axis=1)

    def fill(block, carry):
        table = values[block].astype(F32)
        both = jnp.concatenate([spread(table, block, p) for p in range(fold)], axis=0)
        at = pl.ds(pl.multiple_of(block * (fold * rows), fold * rows), fold * rows)
        lat[at, :] = both.astype(BF16)
        return carry

    lax.fori_loop(0, W, fill, 0)
    load_dec.wait()

    def narrow_copy(d, source, target, send, recv):
        return pltpu.make_async_remote_copy(
            src_ref=source, dst_ref=target, send_sem=send, recv_sem=recv,
            device_id={"narrow": lax.rem(narrow + d, N)}, device_id_type=MESH,
        )

    def rec_copy(c, d):
        return narrow_copy(d, rec.at[c, lax.rem(narrow + d, N)], rec_in.at[c, d], ns1.at[c, d], nr1.at[c, d])

    def columns(c):
        return pl.ds(pl.multiple_of(c * chunk, chunk), chunk)

    def own_rows(i):
        return pl.ds(pl.multiple_of(i * own, own), own)

    def err_copy(c, d):
        return narrow_copy(d, err_out.at[c, d], err.at[own_rows(narrow), columns(c)], ns2.at[c, d], nr2.at[c, d])

    def decode(c, carry):
        product = jnp.dot(lat[...], dec[:, columns(c)], preferred_element_type=F32)
        rec[c] = product.astype(BF16).reshape(N, own, chunk)
        for d in range(1, N):
            rec_copy(c, d).start()
        return carry

    lax.fori_loop(0, chunks, decode, 0)

    def flip(j, carry):
        at = pl.ds(pl.multiple_of(j * LANES, LANES), LANES)
        lat_t[at, :] = lat[:, at].T
        return carry

    def combine(c, carry):
        for d in range(1, N):
            rec_copy(c, d).wait_recv()
        shift = shift_ref[:, columns(c)] - act[own_rows(narrow), columns(c)].astype(F32)
        terms = [rec[c, narrow].astype(F32)]
        terms += [rec_in[c, d].astype(F32) for d in range(1, N)]
        for e in range(N):
            goal = lax.rem(narrow + e, N)
            back = (N - goal).astype(F32) * shift
            for d in range(N):
                origin = lax.rem(narrow + N - d, N)
                back = back + (N - jnp.maximum(goal, origin)).astype(F32) * terms[d]
            back = (back / N).astype(BF16)
            if e == 0:
                err[own_rows(narrow), columns(c)] = back
            else:
                err_out[c, e] = back
                err_copy(c, e).start()
        return carry

    lax.fori_loop(0, chunks, combine, 0)
    lax.fori_loop(0, latents // LANES, flip, 0)

    def contract(c):
        for d in range(1, N):
            err_copy(c, d).wait_recv()
        return lax.dot_general(
            err[:, columns(c)], dec[:, columns(c)], (((1,), (1,)), ((), ())), preferred_element_type=F32
        )

    def outer(c):
        dg_ref[:, columns(c)] = jnp.dot(lat_t[...], err[:, columns(c)], preferred_element_type=F32).astype(BF16)

    total[...] = contract(0)

    def more(c, carry):
        outer(c - 1)
        total[...] += contract(c)
        return carry

    lax.fori_loop(1, chunks, more, 0)

    def pack(w, carry):
        picked = pick_dense(w)
        mine[w] = picked
        lg_packed[w] = picked.astype(BF16)
        return carry

    lax.fori_loop(0, W, pack, 0)
    for d in range(1, W):
        scatter_copy(d, lg_packed, grad_in, ws3, wr3).start()
    outer(chunks - 1)
    summed = mine[wide]
    for d in range(1, W):
        scatter_copy(d, lg_packed, grad_in, ws3, wr3).wait_recv()
        summed = summed + grad_in[d].astype(F32)
    for p in range(fold):
        grad_ref[p * rows : (p + 1) * rows, :] = spread(summed, wide, p)

    for d in range(1, W):
        scatter_copy(d, part, wide_in, ws1, wr1).wait_send()
        wide_copy(d, values.at[wide], values.at[wide], ws2, wr2).wait_send()
        scatter_copy(d, lg_packed, grad_in, ws3, wr3).wait_send()

    def drain(c, carry):
        for d in range(1, N):
            rec_copy(c, d).wait_send()
            err_copy(c, d).wait_send()
        return carry

    lax.fori_loop(0, chunks, drain, 0)


def local(activations, enc_weight, enc_bias, dec_weight, dec_bias, active_ids):
    W, N = lax.axis_size("wide"), lax.axis_size("narrow")
    tokens, channels = activations.shape
    latents = enc_weight.shape[1]
    top = active_ids.shape[1]
    fold = LANES // top
    rows = tokens // W // fold
    chunk = min(channels, 256)
    chunks = channels // chunk
    pieces = 4
    own = tokens // N
    packed_shape = (W, rows, LANES)
    vmem = pl.BlockSpec(memory_space=pltpu.VMEM)
    hbm = pl.BlockSpec(memory_space=pl.ANY)
    dma = pltpu.SemaphoreType.DMA
    dec_grad, latent_grad = pl.pallas_call(
        functools.partial(step_kernel, W, N, fold, top, chunk, pieces),
        out_shape=(
            pltpu.VMEM((latents, channels), BF16),
            pltpu.VMEM((tokens // W, latents), F32),
        ),
        in_specs=[vmem, vmem, vmem, hbm, hbm, hbm],
        out_specs=(vmem, vmem),
        scratch_shapes=[
            pltpu.VMEM((tokens, LANES), jnp.int32),
            pltpu.VMEM((tokens, channels), BF16),
            pltpu.VMEM((channels, latents), BF16),
            pltpu.VMEM((latents, channels), BF16),
            pltpu.VMEM((tokens, latents), jnp.int16),
            pltpu.VMEM((tokens, latents), F32),
            pltpu.VMEM(packed_shape, F32),
            pltpu.VMEM(packed_shape, BF16),
            pltpu.VMEM(packed_shape, BF16),
            pltpu.VMEM(packed_shape, BF16),
            pltpu.VMEM((tokens, latents), BF16),
            pltpu.VMEM((latents, tokens), BF16),
            pltpu.VMEM((chunks, N, own, chunk), BF16),
            pltpu.VMEM((chunks, N, own, chunk), BF16),
            pltpu.VMEM((chunks, N, own, chunk), BF16),
            pltpu.VMEM((tokens, channels), BF16),
            pltpu.VMEM(packed_shape, BF16),
            pltpu.VMEM(packed_shape, BF16),
            dma((2 + pieces,)),
            dma((W,)), dma((W,)), dma((W,)), dma((W,)), dma((W,)), dma((W,)),
            dma((chunks, N)), dma((chunks, N)), dma((chunks, N)), dma((chunks, N)),
        ],
        compiler_params=pltpu.CompilerParams(collective_id=0, has_side_effects=True, vmem_limit_bytes=56 * 2**20),
        cost_estimate=pl.CostEstimate(
            flops=8 * tokens * channels * latents, bytes_accessed=6 * channels * (tokens + latents), transcendentals=0
        ),
        name="step",
    )(active_ids.T, enc_bias.reshape(1, -1), dec_bias.reshape(1, -1), activations, enc_weight, dec_weight)
    return dec_grad, latent_grad


def solution(mesh):
    in_specs = (
        P(None, "wide"),
        P("wide", "narrow"),
        P("narrow"),
        P("narrow", "wide"),
        P("wide"),
        P(),
    )
    out_specs = (P("narrow", "wide"), P("wide", "narrow"))
    return jax.shard_map(local, mesh=mesh, in_specs=in_specs, out_specs=out_specs, check_vma=False)
```

```python
import functools

import jax
import jax.numpy as jnp
from jax import lax
from jax.experimental import pallas as pl
from jax.experimental.pallas import tpu as pltpu
from jax.sharding import PartitionSpec as P

LANES = 128
MESH = pl.DeviceIdType.MESH
F32, BF16 = jnp.float32, jnp.bfloat16


def lookup(table, index):
    return jnp.take_along_axis(table, index, axis=1, mode="promise_in_bounds")


def pick(tables, ids, fold, top):
    tile, lane = ids >> 7, ids & (LANES - 1)
    half = lax.broadcasted_iota(jnp.int32, ids.shape, 1) // top
    picked = jnp.zeros(ids.shape, F32)
    for part in range(fold):
        here = jnp.where(half == part, tile, -1)
        for j, table in enumerate(tables(part)):
            picked = jnp.where(here == j, lookup(table, lane), picked)
    return picked


def step_kernel(
    W, N, fold, top, chunk, pieces, early,
    ids_t_ref, bias_ref, shift_ref, act_hbm, enc_hbm, dec_hbm,
    dg_ref, grad_ref,
    ids, act, enc, dec, slot, total, mine, part, wide_in, values, lat, lat_t,
    err, lg_packed, grad_in,
    load_sem, ws1, wr1, ws2, wr2, ws3, wr3, *scratch,
):
    wide, narrow = lax.axis_index("wide"), lax.axis_index("narrow")
    tokens, latents = lat.shape
    channels = act.shape[1]
    own, rows = tokens // N, part.shape[1]
    chunks = channels // chunk
    piece = latents // pieces
    low = narrow * latents

    def piece_cols(n):
        return pl.ds(pl.multiple_of(n * piece, LANES), piece)

    load_act = pltpu.make_async_copy(act_hbm, act, load_sem.at[0])
    head = channels - early * chunk
    load_dec = pltpu.make_async_copy(dec_hbm.at[:, :head], dec.at[:, :head], load_sem.at[1])

    def load_enc(n):
        return pltpu.make_async_copy(enc_hbm.at[:, piece_cols(n)], enc.at[:, piece_cols(n)], load_sem.at[2 + n])

    if early:
        load_rest = pltpu.make_async_copy(dec_hbm.at[:, head:], dec.at[:, head:], load_sem.at[2 + pieces])
        load_rest.start()
    load_act.start()
    for n in range(pieces):
        load_enc(n).start()
    load_dec.start()

    barrier = pltpu.get_barrier_semaphore()
    for d in range(1, W):
        pl.semaphore_signal(barrier, inc=1, device_id={"wide": lax.rem(wide + d, W)}, device_id_type=MESH)
    for d in range(1, N):
        pl.semaphore_signal(barrier, inc=1, device_id={"narrow": lax.rem(narrow + d, N)}, device_id_type=MESH)

    stacked = jnp.concatenate([ids_t_ref[...]] * fold, axis=0)
    ids[...] = stacked.T

    GROUP, TALL = 16, 256
    bands = latents // TALL
    groups = bands * (tokens // LANES)

    def fill_slots(i, slot, low):
        band, side = i % bands, i // bands
        at = pl.ds(pl.multiple_of(side * LANES, LANES), LANES)
        offset = low + band * TALL
        place = lax.broadcasted_iota(jnp.int32, (GROUP, LANES), 0)
        places = [(place + j * GROUP).astype(jnp.int16) for j in range(TALL // GROUP)]
        found = [jnp.full((GROUP, LANES), top, jnp.int16) for _ in places]
        for k in range(top):
            here = jnp.broadcast_to(ids_t_ref[k : k + 1, at] - offset, (GROUP, LANES)).astype(jnp.int16)
            found = [jnp.where(here == p, jnp.int16(k), f) for p, f in zip(places, found)]
        slot[at, pl.ds(pl.multiple_of(band * TALL, TALL), TALL)] = jnp.concatenate(found, axis=0).T

    def slots_of(i, carry):
        fill_slots(i, slot, low)
        return carry

    lax.fori_loop(0, groups // 4, slots_of, 0)
    pl.semaphore_wait(barrier, W + N - 2)

    def narrow_copy(goal, source, target, send, recv):
        return pltpu.make_async_remote_copy(
            src_ref=source, dst_ref=target, send_sem=send, recv_sem=recv,
            device_id={"narrow": goal}, device_id_type=MESH,
        )

    def wide_copy(d, source, target, send, recv):
        return pltpu.make_async_remote_copy(
            src_ref=source, dst_ref=target, send_sem=send.at[d], recv_sem=recv.at[d],
            device_id={"wide": lax.rem(wide + d, W)}, device_id_type=MESH,
        )

    def columns(c):
        return pl.ds(pl.multiple_of(c * chunk, chunk), chunk)

    if early:
        (
            dec_in, slot_in, values_in, lat_in, rec, rec_in, msg, msg_in, err_out, full, full_in, base,
            ds, dr, vs, vr, vws, vwr, ns1, nr1, ns2, nr2, ns3, nr3, fs, fr,
        ) = scratch
        side, pair = lax.rem(narrow, 2), narrow // 2
        across, along = narrow + 1 - 2 * side, narrow + 2 - 4 * pair
        plain = chunks - early

        PARTS = 2
        tall = latents // PARTS

        def dec_copy(i):
            c, at = i // PARTS, pl.ds(i % PARTS * tall, tall)
            return narrow_copy(
                across, dec.at[at, columns(plain + c)], dec_in.at[at, columns(c)], ds.at[i], dr.at[i]
            )

        load_rest.wait()
        for i in range(early * PARTS - 1):
            dec_copy(i).start()
    else:
        rec, rec_in, err_out, ns1, nr1, ns2, nr2 = scratch

    load_act.wait()

    def encode(n, carry):
        pltpu.make_async_copy(enc_hbm.at[:, piece_cols(n)], enc.at[:, piece_cols(n)], load_sem.at[2 + n]).wait()
        total[:, piece_cols(n)] = jnp.dot(act[...], enc[:, piece_cols(n)], preferred_element_type=F32)
        return carry

    lax.fori_loop(0, pieces, encode, 0)

    half = lax.broadcasted_iota(jnp.int32, (rows, LANES), 1) // top

    def packed_ids(w):
        out = ids[pl.ds(w * (rows * fold), rows), :]
        for p in range(1, fold):
            other = ids[pl.ds((w * fold + p) * rows, rows), :]
            out = jnp.where(half == p, other, out)
        return out - low

    def pick_dense(w):
        def tables(p):
            at = pl.ds((w * fold + p) * rows, rows)
            return [total[at, j * LANES : (j + 1) * LANES] for j in range(latents // LANES)]

        return pick(tables, packed_ids(w), fold, top)

    def pick_block(w, carry):
        picked = pick_dense(w)
        mine[w] = picked
        part[w] = picked.astype(BF16)
        return carry

    for w in range(W):
        pick_block(w, 0)

    def scatter_copy(d, source, target, send, recv):
        return wide_copy(d, source.at[lax.rem(wide + d, W)], target.at[d], send, recv)

    for d in range(1, W):
        scatter_copy(d, part, wide_in, ws1, wr1).start()

    def bias_tables(p):
        return [jnp.broadcast_to(bias_ref[:, j * LANES : (j + 1) * LANES], (rows, LANES)) for j in range(latents // LANES)]

    summed = mine[wide] + pick(bias_tables, packed_ids(wide), fold, top)

    lax.fori_loop(groups // 4, groups * 5 // 8, slots_of, 0)

    for d in range(1, W):
        scatter_copy(d, part, wide_in, ws1, wr1).wait_recv()
        summed = summed + wide_in[d].astype(F32)
    values[wide] = summed.astype(BF16)
    for d in range(1, W):
        wide_copy(d, values.at[wide], values.at[wide], ws2, wr2).start()
    if early:
        def pair_values():
            return narrow_copy(across, values.at[wide], values_in.at[wide], vs.at[0], vr.at[0])

        pair_values().start()
        dec_copy(early * PARTS - 1).start()

    lax.fori_loop(groups * 5 // 8, groups, slots_of, 0)
    for d in range(1, W):
        wide_copy(d, values.at[wide], values.at[wide], ws2, wr2).wait_recv()

    def spread(table, slot, block, p):
        start = (block * fold + p) * rows
        at = pl.ds(start if isinstance(start, int) else pl.multiple_of(start, rows), rows)
        table = table[:, p * top : (p + 1) * top]
        table = jnp.concatenate([table, jnp.zeros((rows, LANES - top), F32)], axis=1)
        out = []
        for j in range(latents // LANES):
            out.append(lookup(table, slot[at, j * LANES : (j + 1) * LANES].astype(jnp.int32)))
        return jnp.concatenate(out, axis=1)

    def fill(values, slot, lat):
        for block in range(W):
            table = values[block].astype(F32)
            both = jnp.concatenate([spread(table, slot, block, p) for p in range(fold)], axis=0)
            lat[block * (fold * rows) : (block + 1) * (fold * rows), :] = both.astype(BF16)

    fill(values, slot, lat)
    load_dec.wait()

    def own_rows(i):
        return pl.ds(pl.multiple_of(i * own, own), own)

    def flip(j, carry):
        at = pl.ds(pl.multiple_of(j * LANES, LANES), LANES)
        lat_t[at, :] = lat[:, at].T
        return carry

    def decode(c):
        return jnp.dot(lat[...], dec[:, columns(c)], preferred_element_type=F32)

    if early:
        mates = N // 2
        share = tokens // mates
        here = pl.ds(pl.multiple_of(side * share, share), share)

        def scale(count):
            return count.astype(F32)

        own_scale, mate_scale = scale(N - narrow), scale(N - across)
        least = scale(N - jnp.maximum(narrow, across))
        own_use, mate_use = scale(1 + pair * (N - 1 - narrow)), scale(1 + pair * (N - 1 - across))

        def rec_copy(c):
            return narrow_copy(across, rec.at[c, 1 - side], rec_in.at[c], ns1.at[c], nr1.at[c])

        def msg_copy(c):
            return narrow_copy(along, msg.at[c], msg_in.at[c], ns2.at[c], nr2.at[c])

        def err_copy(c):
            return narrow_copy(across, err_out.at[c], err.at[here, columns(c)], ns3.at[c], nr3.at[c])

        def full_copy(c):
            return narrow_copy(along, full.at[c], full_in.at[c], fs.at[c], fr.at[c])

        def send_rec(c, carry):
            rec[c] = decode(c).astype(BF16).reshape(mates, share, chunk)
            rec_copy(c).start()
            return carry

        lax.fori_loop(0, plain, send_rec, 0)

        def more_slots(i, carry):
            fill_slots(i, slot_in, across * latents)
            return carry

        def send_msg(c, carry):
            rec_copy(c).wait_recv()
            msg[c] = (own_use * rec[c, side].astype(F32) + mate_use * rec_in[c].astype(F32)).astype(BF16)
            msg_copy(c).start()
            return carry

        def send_err(c, carry):
            msg_copy(c).wait_recv()
            shift = shift_ref[:, columns(c)] - act[here, columns(c)].astype(F32)
            mine_rec, mate_rec = rec[c, side].astype(F32), rec_in[c].astype(F32)
            other = msg_in[c].astype(F32)
            back = own_scale * (shift + mine_rec) + least * mate_rec + own_use * other
            err[here, columns(c)] = (back / N).astype(BF16)
            back = mate_scale * (shift + mate_rec) + least * mine_rec + mate_use * other
            err_out[c] = (back / N).astype(BF16)
            err_copy(c).start()
            return carry

        def send_full(c, carry):
            mine_rec = decode(plain + c)
            mate_rec = jnp.dot(lat_in[...], dec_in[:, columns(c)], preferred_element_type=F32)
            full[c] = (own_use * mine_rec + mate_use * mate_rec).astype(BF16)
            full_copy(c).start()
            shift = shift_ref[:, columns(plain + c)] - act[:, columns(plain + c)].astype(F32)
            base[c] = own_scale * (shift + mine_rec) + least * mate_rec
            return carry

        def take_full(c, carry):
            full_copy(c).wait_recv()
            err[:, columns(plain + c)] = ((base[c] + own_use * full_in[c].astype(F32)) / N).astype(BF16)
            return carry

        def values_copies():
            return [wide_copy(d, values_in.at[wide], values_in.at[wide], vws, vwr) for d in range(1, W)]

        LAG, HEAD, PER = 2, groups // 2, groups // 4
        lax.fori_loop(0, latents // LANES, flip, 0)
        lax.fori_loop(0, HEAD, more_slots, 0)
        for c in range(plain):
            send_msg(c, 0)
            if c >= LAG:
                send_err(c - LAG, 0)
            if c == 0:
                pair_values().wait_recv()
                for copy in values_copies():
                    copy.start()
            if c < 2:
                lax.fori_loop(HEAD + c * PER, HEAD + (c + 1) * PER, more_slots, 0)
            if c == 2:
                for copy in values_copies():
                    copy.wait_recv()
                fill(values_in, slot_in, lat_in)
        for i in range(early * PARTS):
            dec_copy(i).wait_recv()
        lax.fori_loop(0, early, send_full, 0)
        for c in range(plain - LAG, plain):
            send_err(c, 0)

        def arrive(c):
            err_copy(c).wait_recv()

        def finish(c, carry):
            rec_copy(c).wait_send()
            msg_copy(c).wait_send()
            err_copy(c).wait_send()
            return carry

        def finish_early():
            for i in range(early * PARTS):
                dec_copy(i).wait_send()
            for c in range(early):
                full_copy(c).wait_send()
            pair_values().wait_send()
            for copy in values_copies():
                copy.wait_send()
    else:
        plain = chunks

        def goal_of(d):
            return lax.rem(narrow + d, N)

        def rec_copy(c, d):
            return narrow_copy(goal_of(d), rec.at[c, goal_of(d)], rec_in.at[c, d], ns1.at[c, d], nr1.at[c, d])

        def err_copy(c, d):
            return narrow_copy(
                goal_of(d), err_out.at[c, d], err.at[own_rows(narrow), columns(c)], ns2.at[c, d], nr2.at[c, d]
            )

        def send_rec(c, carry):
            rec[c] = decode(c).astype(BF16).reshape(N, own, chunk)
            for d in range(1, N):
                rec_copy(c, d).start()
            return carry

        lax.fori_loop(0, chunks, send_rec, 0)

        def combine(c, carry):
            for d in range(1, N):
                rec_copy(c, d).wait_recv()
            shift = shift_ref[:, columns(c)] - act[own_rows(narrow), columns(c)].astype(F32)
            terms = [rec[c, narrow].astype(F32)]
            terms += [rec_in[c, d].astype(F32) for d in range(1, N)]
            for e in range(N):
                goal = goal_of(e)
                back = (N - goal).astype(F32) * shift
                for d in range(N):
                    origin = lax.rem(narrow + N - d, N)
                    back = back + (N - jnp.maximum(goal, origin)).astype(F32) * terms[d]
                back = (back / N).astype(BF16)
                if e == 0:
                    err[own_rows(narrow), columns(c)] = back
                else:
                    err_out[c, e] = back
                    err_copy(c, e).start()
            return carry

        lax.fori_loop(0, chunks, combine, 0)
        lax.fori_loop(0, latents // LANES, flip, 0)

        def arrive(c):
            for d in range(1, N):
                err_copy(c, d).wait_recv()

        def finish(c, carry):
            for d in range(1, N):
                rec_copy(c, d).wait_send()
                err_copy(c, d).wait_send()
            return carry

        def finish_early():
            pass

    def contract(c):
        return lax.dot_general(
            err[:, columns(c)], dec[:, columns(c)], (((1,), (1,)), ((), ())), preferred_element_type=F32
        )

    def outer(c):
        dg_ref[:, columns(c)] = jnp.dot(lat_t[...], err[:, columns(c)], preferred_element_type=F32).astype(BF16)

    total[...] = jnp.zeros_like(total)

    def local_chunk(c, carry):
        total[...] += contract(c)
        outer(c)
        return carry

    def sent_chunk(c, carry):
        arrive(c)
        return local_chunk(c, carry)

    if early:
        lax.fori_loop(0, plain // 2, sent_chunk, 0)
        lax.fori_loop(0, early, take_full, 0)
        lax.fori_loop(plain, chunks, local_chunk, 0)
        lax.fori_loop(plain // 2, plain - 1, sent_chunk, 0)
    else:
        lax.fori_loop(0, plain - 1, sent_chunk, 0)
    arrive(plain - 1)
    total[...] += contract(plain - 1)

    def pack(w, carry):
        picked = pick_dense(w)
        mine[w] = picked
        lg_packed[w] = picked.astype(BF16)
        return carry

    for w in range(W):
        pack(w, 0)
    for d in range(1, W):
        scatter_copy(d, lg_packed, grad_in, ws3, wr3).start()
    outer(plain - 1)
    summed = mine[wide]
    for d in range(1, W):
        scatter_copy(d, lg_packed, grad_in, ws3, wr3).wait_recv()
        summed = summed + grad_in[d].astype(F32)
    for p in range(fold):
        grad_ref[p * rows : (p + 1) * rows, :] = spread(summed, slot, wide, p)

    for d in range(1, W):
        scatter_copy(d, part, wide_in, ws1, wr1).wait_send()
        wide_copy(d, values.at[wide], values.at[wide], ws2, wr2).wait_send()
        scatter_copy(d, lg_packed, grad_in, ws3, wr3).wait_send()

    lax.fori_loop(0, plain, finish, 0)
    finish_early()


STORES = 4


def store_kernel(dg_ref, grad_ref, dg_hbm, grad_hbm, sem):
    step = dg_ref.shape[0] // STORES
    copies = [pltpu.make_async_copy(grad_ref, grad_hbm, sem.at[STORES])]
    for i in range(STORES):
        at = pl.ds(i * step, step)
        copies.append(pltpu.make_async_copy(dg_ref.at[at], dg_hbm.at[at], sem.at[i]))
    for copy in copies:
        copy.start()
    for copy in copies:
        copy.wait()


def local(activations, enc_weight, enc_bias, dec_weight, dec_bias, active_ids):
    W, N = lax.axis_size("wide"), lax.axis_size("narrow")
    tokens, channels = activations.shape
    latents = enc_weight.shape[1]
    top = active_ids.shape[1]
    fold = LANES // top
    rows = tokens // W // fold
    chunk = min(channels, 256)
    chunks = channels // chunk
    pieces = 4
    own = tokens // N
    early = chunks // 8 if N == 4 else 0
    plain = chunks - early
    half = (plain, tokens // 2, chunk)
    packed_shape = (W, rows, LANES)
    vmem = pl.BlockSpec(memory_space=pltpu.VMEM)
    hbm = pl.BlockSpec(memory_space=pl.ANY)
    dma = pltpu.SemaphoreType.DMA
    if early:
        scratch = [
            pltpu.VMEM((latents, early * chunk), BF16),
            pltpu.VMEM((tokens, latents), jnp.int16),
            pltpu.VMEM(packed_shape, BF16),
            pltpu.VMEM((tokens, latents), BF16),
            pltpu.VMEM((plain, 2, tokens // 2, chunk), BF16),
            *[pltpu.VMEM(half, BF16)] * 4,
            *[pltpu.VMEM((early, tokens, chunk), BF16)] * 2,
            pltpu.VMEM((early, tokens, chunk), F32),
            dma((2 * early,)), dma((2 * early,)), dma((1,)), dma((1,)), dma((W,)), dma((W,)),
            *[dma((plain,))] * 6,
            dma((early,)), dma((early,)),
        ]
    else:
        scratch = [*[pltpu.VMEM((chunks, N, own, chunk), BF16)] * 3, *[dma((chunks, N))] * 4]
    dec_grad, latent_grad = pl.pallas_call(
        functools.partial(step_kernel, W, N, fold, top, chunk, pieces, early),
        out_shape=(
            pltpu.VMEM((latents, channels), BF16),
            pltpu.VMEM((tokens // W, latents), F32),
        ),
        in_specs=[vmem, vmem, vmem, hbm, hbm, hbm],
        out_specs=(vmem, vmem),
        scratch_shapes=[
            pltpu.VMEM((tokens, LANES), jnp.int32),
            pltpu.VMEM((tokens, channels), BF16),
            pltpu.VMEM((channels, latents), BF16),
            pltpu.VMEM((latents, channels), BF16),
            pltpu.VMEM((tokens, latents), jnp.int16),
            pltpu.VMEM((tokens, latents), F32),
            pltpu.VMEM(packed_shape, F32),
            pltpu.VMEM(packed_shape, BF16),
            pltpu.VMEM(packed_shape, BF16),
            pltpu.VMEM(packed_shape, BF16),
            pltpu.VMEM((tokens, latents), BF16),
            pltpu.VMEM((latents, tokens), BF16),
            pltpu.VMEM((tokens, channels), BF16),
            pltpu.VMEM(packed_shape, BF16),
            pltpu.VMEM(packed_shape, BF16),
            dma((3 + pieces,)),
            *[dma((W,))] * 6,
            *scratch,
        ],
        compiler_params=pltpu.CompilerParams(collective_id=0, has_side_effects=True, vmem_limit_bytes=56 * 2**20),
        cost_estimate=pl.CostEstimate(
            flops=8 * tokens * channels * latents, bytes_accessed=6 * channels * (tokens + latents), transcendentals=0
        ),
        name="step",
    )(active_ids.T, enc_bias.reshape(1, -1), dec_bias.reshape(1, -1), activations, enc_weight, dec_weight)
    return pl.pallas_call(
        store_kernel,
        out_shape=(
            jax.ShapeDtypeStruct(dec_grad.shape, BF16),
            jax.ShapeDtypeStruct(latent_grad.shape, F32),
        ),
        in_specs=[vmem, vmem],
        out_specs=(hbm, hbm),
        scratch_shapes=[dma((STORES + 1,))],
        compiler_params=pltpu.CompilerParams(vmem_limit_bytes=2**20),
        name="store",
    )(
        pltpu.with_memory_space_constraint(dec_grad, pltpu.VMEM),
        pltpu.with_memory_space_constraint(latent_grad, pltpu.VMEM),
    )


def solution(mesh):
    in_specs = (
        P(None, "wide"),
        P("wide", "narrow"),
        P("narrow"),
        P("narrow", "wide"),
        P("wide"),
        P(),
    )
    out_specs = (P("narrow", "wide"), P("wide", "narrow"))
    return jax.shard_map(local, mesh=mesh, in_specs=in_specs, out_specs=out_specs, check_vma=False)
```

```python
import functools

import jax
import jax.numpy as jnp
from jax import lax
from jax.experimental import pallas as pl
from jax.experimental.pallas import tpu as pltpu
from jax.sharding import PartitionSpec as P

LANES = 128
MESH = pl.DeviceIdType.MESH
F32, BF16 = jnp.float32, jnp.bfloat16


def lookup(table, index):
    return jnp.take_along_axis(table, index, axis=1, mode="promise_in_bounds")


def pick(tables, ids, fold, top):
    tile, lane = ids >> 7, ids & (LANES - 1)
    half = lax.broadcasted_iota(jnp.int32, ids.shape, 1) // top
    picked = jnp.zeros(ids.shape, F32)
    for part in range(fold):
        here = jnp.where(half == part, tile, -1)
        for j, table in enumerate(tables(part)):
            picked = jnp.where(here == j, lookup(table, lane), picked)
    return picked


def spread_row(table, p, top, tiles, slots):
    rows = table.shape[0]
    table = jnp.concatenate([table[:, p * top : (p + 1) * top], jnp.zeros((rows, LANES - top), F32)], axis=1)
    return jnp.concatenate([lookup(table, slots(j)) for j in range(tiles)], axis=1)


def step_kernel(
    W, N, fold, top, chunk, pieces, early,
    ids_t_ref, bias_ref, shift_ref, act_hbm, enc_hbm, dec_hbm,
    dg_ref, sum_ref, own_slot_ref,
    ids, act, enc, dec, slot, total, part, wide_in, values, lat, lat_t,
    err, lg_packed, grad_in,
    load_sem, ws1, wr1, ws2, wr2, ws3, wr3, *scratch,
):
    wide, narrow = lax.axis_index("wide"), lax.axis_index("narrow")
    tokens, latents = lat.shape
    channels = act.shape[1]
    own, rows = tokens // N, part.shape[1]
    chunks = channels // chunk
    piece = latents // pieces
    low = narrow * latents
    half_rows, quarter = tokens // 2, tokens // 4
    near = wide // (W // 2)

    def mate(d):
        goal = 0
        for b in range(W.bit_length() - 1):
            digit = wide // 2**b % 2
            goal = goal + 2**b * (1 - digit if d >> b & 1 else digit)
        return goal

    def rows_of(h):
        return pl.ds(pl.multiple_of(h * half_rows, half_rows), half_rows)

    def piece_cols(n):
        return pl.ds(pl.multiple_of(n * piece, LANES), piece)

    load_act = pltpu.make_async_copy(act_hbm, act, load_sem.at[0])
    head = channels - early * chunk
    load_dec = pltpu.make_async_copy(dec_hbm.at[:, :head], dec.at[:, :head], load_sem.at[1])

    def load_enc(n):
        return pltpu.make_async_copy(enc_hbm.at[:, piece_cols(n)], enc.at[:, piece_cols(n)], load_sem.at[2 + n])

    if early:
        load_rest = pltpu.make_async_copy(dec_hbm.at[:, head:], dec.at[:, head:], load_sem.at[2 + pieces])
        load_rest.start()
    load_act.start()
    for n in range(pieces):
        load_enc(n).start()
    load_dec.start()

    barrier = pltpu.get_barrier_semaphore()
    for d in range(1, W):
        pl.semaphore_signal(barrier, inc=1, device_id={"wide": mate(d)}, device_id_type=MESH)
    for d in range(1, N):
        pl.semaphore_signal(barrier, inc=1, device_id={"narrow": lax.rem(narrow + d, N)}, device_id_type=MESH)

    stacked = jnp.concatenate([ids_t_ref[...]] * fold, axis=0)
    ids[...] = stacked.T

    GROUP, TALL = 16, 256
    bands = latents // TALL
    groups = bands * (tokens // LANES)

    def fill_slots(i, slot, low):
        band, side = i % bands, i // bands
        at = pl.ds(pl.multiple_of(side * LANES, LANES), LANES)
        offset = low + band * TALL
        place = lax.broadcasted_iota(jnp.int32, (GROUP, LANES), 0)
        places = [(place + j * GROUP).astype(jnp.int16) for j in range(TALL // GROUP)]
        found = [jnp.full((GROUP, LANES), top, jnp.int16) for _ in places]
        for k in range(top):
            here = jnp.broadcast_to(ids_t_ref[k : k + 1, at] - offset, (GROUP, LANES)).astype(jnp.int16)
            found = [jnp.where(here == p, jnp.int16(k), f) for p, f in zip(places, found)]
        slot[at, pl.ds(pl.multiple_of(band * TALL, TALL), TALL)] = jnp.concatenate(found, axis=0).T.astype(jnp.int32)

    def slots_of(i, carry):
        fill_slots(i, slot, low)
        return carry

    lax.fori_loop(0, groups // 4, slots_of, 0)
    pl.semaphore_wait(barrier, W + N - 2)

    def narrow_copy(goal, source, target, send, recv):
        return pltpu.make_async_remote_copy(
            src_ref=source, dst_ref=target, send_sem=send, recv_sem=recv,
            device_id={"narrow": goal}, device_id_type=MESH,
        )

    def wide_copy(d, source, target, send, recv):
        return pltpu.make_async_remote_copy(
            src_ref=source, dst_ref=target, send_sem=send.at[d], recv_sem=recv.at[d],
            device_id={"wide": mate(d)}, device_id_type=MESH,
        )

    def columns(c):
        return pl.ds(pl.multiple_of(c * chunk, chunk), chunk)

    if early:
        (
            dec_in, slot_in, values_in, lat_in, rec, rec_in, msg, msg_in, err_out, full, full_in, base,
            ds, dr, vs, vr, vws, vwr, ns1, nr1, ns2, nr2, ns3, nr3, fs, fr,
        ) = scratch
        side, pair = lax.rem(narrow, 2), narrow // 2
        across, along = narrow + 1 - 2 * side, narrow + 2 - 4 * pair
        plain = chunks - early

        PARTS = 2
        tall = latents // PARTS

        def dec_copy(i):
            c, at = i // PARTS, pl.ds(i % PARTS * tall, tall)
            return narrow_copy(
                across, dec.at[at, columns(plain + c)], dec_in.at[at, columns(c)], ds.at[i], dr.at[i]
            )

        load_rest.wait()
        for i in range(early * PARTS):
            dec_copy(i).start()
    else:
        rec, rec_in, err_out, ns1, nr1, ns2, nr2 = scratch

    load_act.wait()

    def encode(h, n):
        total[rows_of(h), piece_cols(n)] = jnp.dot(
            act[rows_of(h), :], enc[:, piece_cols(n)], preferred_element_type=F32
        )

    def encode_far(n, carry):
        load_enc(n).wait()
        encode(1 - near, n)
        return carry

    def encode_near(n, carry):
        encode(near, n)
        return carry

    half = lax.broadcasted_iota(jnp.int32, (rows, LANES), 1) // top

    def block_rows(w, p):
        return pl.ds(pl.multiple_of((w * fold + p) * rows, rows), rows)

    def packed_ids(w):
        out = ids[block_rows(w, 0), :]
        for p in range(1, fold):
            out = jnp.where(half == p, ids[block_rows(w, p), :], out)
        return out - low

    def pick_dense(w):
        def tables(p):
            return [total[block_rows(w, p), j * LANES : (j + 1) * LANES] for j in range(latents // LANES)]

        return pick(tables, packed_ids(w), fold, top)

    def scatter_copy(d, source, target, send, recv):
        return wide_copy(d, source.at[d], target.at[d], send, recv)

    def scatter(first, last, source, target, send, recv):
        picked = None
        for d in range(last - 1, first - 1, -1):
            picked = pick_dense(mate(d))
            if d > 0:
                source[d] = picked.astype(BF16)
                scatter_copy(d, source, target, send, recv).start()
        return picked

    def gather(picked, source, target, send, recv):
        for d in range(1, W):
            scatter_copy(d, source, target, send, recv).wait_recv()
            picked = picked + target[d].astype(F32)
        return picked

    lax.fori_loop(0, pieces, encode_far, 0)
    scatter(W // 2, W, part, wide_in, ws1, wr1)
    lax.fori_loop(0, pieces, encode_near, 0)
    summed = scatter(0, W // 2, part, wide_in, ws1, wr1)

    def bias_tables(p):
        return [jnp.broadcast_to(bias_ref[:, j * LANES : (j + 1) * LANES], (rows, LANES)) for j in range(latents // LANES)]

    summed = summed + pick(bias_tables, packed_ids(wide), fold, top)

    lax.fori_loop(groups // 4, groups * 3 // 4, slots_of, 0)

    values[wide] = gather(summed, part, wide_in, ws1, wr1).astype(BF16)

    def value_copy(d):
        return wide_copy(d, values.at[wide], values.at[wide], ws2, wr2)

    for d in range(W - 1, 0, -1):
        value_copy(d).start()
    if early:
        def pair_values():
            return narrow_copy(across, values.at[wide], values_in.at[wide], vs.at[0], vr.at[0])

        pair_values().start()

    lax.fori_loop(groups * 3 // 4, groups, slots_of, 0)

    def fill_block(block, values, slot, lat):
        table = values[block].astype(F32)
        for p in range(fold):
            at = block_rows(block, p)
            spread = spread_row(table, p, top, latents // LANES, lambda j: slot[at, j * LANES : (j + 1) * LANES])
            lat[at, :] = spread.astype(BF16)

    def fill_mates(first, last):
        for d in range(first, last):
            if d > 0:
                value_copy(d).wait_recv()
            fill_block(mate(d), values, slot, lat)

    load_dec.wait()

    def own_rows(i):
        return pl.ds(pl.multiple_of(i * own, own), own)

    def keep_slots():
        own_slot_ref[...] = slot[pl.ds(pl.multiple_of(wide * (fold * rows), fold * rows), fold * rows), :]

    def flip(j, carry):
        at = pl.ds(pl.multiple_of(j * LANES, LANES), LANES)
        lat_t[at, :] = lat[:, at].T
        return carry

    def decode(c, at=slice(None)):
        return jnp.dot(lat[at, :], dec[:, columns(c)], preferred_element_type=F32)

    if early:
        def here(h):
            return pl.ds(pl.multiple_of(h * half_rows + side * quarter, quarter), quarter)

        def scale(count):
            return count.astype(F32)

        own_scale, mate_scale = scale(N - narrow), scale(N - across)
        least = scale(N - jnp.maximum(narrow, across))
        own_use, mate_use = scale(1 + pair * (N - 1 - narrow)), scale(1 + pair * (N - 1 - across))

        def rec_copy(c, q):
            h = near if q == 0 else 1 - near
            return narrow_copy(across, rec.at[c, h, 1 - side], rec_in.at[c, h], ns1.at[c, q], nr1.at[c, q])

        def msg_copy(c):
            return narrow_copy(along, msg.at[c], msg_in.at[c], ns2.at[c], nr2.at[c])

        def err_copy(c, h):
            return narrow_copy(across, err_out.at[c, h], err.at[here(h), columns(c)], ns3.at[c, h], nr3.at[c, h])

        def full_copy(c):
            return narrow_copy(along, full.at[c], full_in.at[c], fs.at[c], fr.at[c])

        def send_rec(q):
            h = near if q == 0 else 1 - near

            def send(c, carry):
                rec[c, h] = decode(c, rows_of(h)).astype(BF16).reshape(2, quarter, chunk)
                rec_copy(c, q).start()
                return carry

            lax.fori_loop(0, plain, send, 0)

        fill_mates(0, W // 2)
        send_rec(0)
        fill_mates(W // 2, W)
        send_rec(1)

        def more_slots(i, carry):
            fill_slots(i, slot_in, across * latents)
            return carry

        def send_msg(c):
            for q in range(2):
                rec_copy(c, q).wait_recv()
            msg[c] = (own_use * rec[c, :, side].astype(F32) + mate_use * rec_in[c].astype(F32)).astype(BF16)
            msg_copy(c).start()

        def send_err(c):
            msg_copy(c).wait_recv()
            for h in range(2):
                shift = shift_ref[:, columns(c)] - act[here(h), columns(c)].astype(F32)
                mine_rec, mate_rec = rec[c, h, side].astype(F32), rec_in[c, h].astype(F32)
                other = msg_in[c, h].astype(F32)
                back = mate_scale * (shift + mate_rec) + least * mine_rec + mate_use * other
                err_out[c, h] = (back / N).astype(BF16)
                err_copy(c, h).start()
                back = own_scale * (shift + mine_rec) + least * mate_rec + own_use * other
                err[here(h), columns(c)] = (back / N).astype(BF16)

        def send_full(c, carry):
            mine_rec = decode(plain + c)
            mate_rec = jnp.dot(lat_in[...], dec_in[:, columns(c)], preferred_element_type=F32)
            full[c] = (own_use * mine_rec + mate_use * mate_rec).astype(BF16)
            full_copy(c).start()
            shift = shift_ref[:, columns(plain + c)] - act[:, columns(plain + c)].astype(F32)
            base[c] = own_scale * (shift + mine_rec) + least * mate_rec
            return carry

        def take_full(c, carry):
            full_copy(c).wait_recv()
            err[:, columns(plain + c)] = ((base[c] + own_use * full_in[c].astype(F32)) / N).astype(BF16)
            return carry

        def values_copies():
            return [wide_copy(d, values_in.at[wide], values_in.at[wide], vws, vwr) for d in range(1, W)]

        LAG, HEAD, PER = 2, groups // 2, groups // 4
        keep_slots()
        lax.fori_loop(0, latents // LANES, flip, 0)
        lax.fori_loop(0, HEAD, more_slots, 0)
        for c in range(plain):
            send_msg(c)
            if c >= LAG:
                send_err(c - LAG)
            if c == 0:
                pair_values().wait_recv()
                for copy in values_copies():
                    copy.start()
            if c < 2:
                lax.fori_loop(HEAD + c * PER, HEAD + (c + 1) * PER, more_slots, 0)
            if c == 2:
                for copy in values_copies():
                    copy.wait_recv()
                for block in range(W):
                    fill_block(block, values_in, slot_in, lat_in)
        for i in range(early * PARTS):
            dec_copy(i).wait_recv()
        lax.fori_loop(0, early, send_full, 0)
        for c in range(plain - LAG, plain):
            send_err(c)

        def arrive(c):
            for h in range(2):
                err_copy(c, h).wait_recv()

        def finish(c, carry):
            for q in range(2):
                rec_copy(c, q).wait_send()
                err_copy(c, q).wait_send()
            msg_copy(c).wait_send()
            return carry

        def finish_early():
            for i in range(early * PARTS):
                dec_copy(i).wait_send()
            for c in range(early):
                full_copy(c).wait_send()
            pair_values().wait_send()
            for copy in values_copies():
                copy.wait_send()
    else:
        plain = chunks
        fill_mates(0, W)
        keep_slots()

        def goal_of(d):
            return lax.rem(narrow + d, N)

        def rec_copy(c, d):
            return narrow_copy(goal_of(d), rec.at[c, goal_of(d)], rec_in.at[c, d], ns1.at[c, d], nr1.at[c, d])

        def err_copy(c, d):
            return narrow_copy(
                goal_of(d), err_out.at[c, d], err.at[own_rows(narrow), columns(c)], ns2.at[c, d], nr2.at[c, d]
            )

        def send_rec(c, carry):
            rec[c] = decode(c).astype(BF16).reshape(N, own, chunk)
            for d in range(1, N):
                rec_copy(c, d).start()
            return carry

        lax.fori_loop(0, chunks, send_rec, 0)

        def combine(c, carry):
            for d in range(1, N):
                rec_copy(c, d).wait_recv()
            shift = shift_ref[:, columns(c)] - act[own_rows(narrow), columns(c)].astype(F32)
            terms = [rec[c, narrow].astype(F32)]
            terms += [rec_in[c, d].astype(F32) for d in range(1, N)]
            for e in range(N):
                goal = goal_of(e)
                back = (N - goal).astype(F32) * shift
                for d in range(N):
                    origin = lax.rem(narrow + N - d, N)
                    back = back + (N - jnp.maximum(goal, origin)).astype(F32) * terms[d]
                back = (back / N).astype(BF16)
                if e == 0:
                    err[own_rows(narrow), columns(c)] = back
                else:
                    err_out[c, e] = back
                    err_copy(c, e).start()
            return carry

        lax.fori_loop(0, chunks, combine, 0)
        lax.fori_loop(0, latents // LANES, flip, 0)

        def arrive(c):
            for d in range(1, N):
                err_copy(c, d).wait_recv()

        def finish(c, carry):
            for d in range(1, N):
                rec_copy(c, d).wait_send()
                err_copy(c, d).wait_send()
            return carry

        def finish_early():
            pass

    def contract(c):
        return lax.dot_general(
            err[:, columns(c)], dec[:, columns(c)], (((1,), (1,)), ((), ())), preferred_element_type=F32
        )

    def outer(c):
        dg_ref[:, columns(c)] = jnp.dot(lat_t[...], err[:, columns(c)], preferred_element_type=F32).astype(BF16)

    total[...] = jnp.zeros_like(total)

    def local_chunk(c, carry):
        total[...] += contract(c)
        outer(c)
        return carry

    def sent_chunk(c, carry):
        arrive(c)
        return local_chunk(c, carry)

    if early:
        lax.fori_loop(0, plain // 2, sent_chunk, 0)
        lax.fori_loop(0, early, take_full, 0)
        lax.fori_loop(plain, chunks, local_chunk, 0)
        lax.fori_loop(plain // 2, plain - 1, sent_chunk, 0)
    else:
        lax.fori_loop(0, plain - 1, sent_chunk, 0)
    arrive(plain - 1)
    total[...] += contract(plain - 1)

    summed = scatter(0, W, lg_packed, grad_in, ws3, wr3)
    outer(plain - 1)
    sum_ref[...] = gather(summed, lg_packed, grad_in, ws3, wr3)

    for d in range(1, W):
        scatter_copy(d, part, wide_in, ws1, wr1).wait_send()
        value_copy(d).wait_send()
        scatter_copy(d, lg_packed, grad_in, ws3, wr3).wait_send()

    lax.fori_loop(0, plain, finish, 0)
    finish_early()


STORES = 4


def store_kernel(fold, top, dg_ref, sum_ref, slot_ref, dg_hbm, grad_ref, sem):
    step = dg_ref.shape[0] // STORES
    rows = sum_ref.shape[0]
    copies = []
    for i in range(STORES):
        at = pl.ds(i * step, step)
        copies.append(pltpu.make_async_copy(dg_ref.at[at], dg_hbm.at[at], sem.at[i]))
    for copy in copies:
        copy.start()
    for p in range(fold):
        at = slice(p * rows, (p + 1) * rows)
        grad_ref[at, :] = spread_row(sum_ref[...], p, top, slot_ref.shape[1] // LANES, lambda j: slot_ref[at, j * LANES : (j + 1) * LANES])
    for copy in copies:
        copy.wait()


def local(activations, enc_weight, enc_bias, dec_weight, dec_bias, active_ids):
    W, N = lax.axis_size("wide"), lax.axis_size("narrow")
    tokens, channels = activations.shape
    latents = enc_weight.shape[1]
    top = active_ids.shape[1]
    fold = LANES // top
    rows = tokens // W // fold
    chunk = min(channels, 256)
    chunks = channels // chunk
    pieces = 4
    own = tokens // N
    early = chunks // 8 if N == 4 else 0
    plain = chunks - early
    half = (plain, 2, tokens // 4, chunk)
    packed_shape = (W, rows, LANES)
    vmem = pl.BlockSpec(memory_space=pltpu.VMEM)
    hbm = pl.BlockSpec(memory_space=pl.ANY)
    dma = pltpu.SemaphoreType.DMA
    if early:
        scratch = [
            pltpu.VMEM((latents, early * chunk), BF16),
            pltpu.VMEM((tokens, latents), jnp.int32),
            pltpu.VMEM(packed_shape, BF16),
            pltpu.VMEM((tokens, latents), BF16),
            pltpu.VMEM((plain, 2, 2, tokens // 4, chunk), BF16),
            *[pltpu.VMEM(half, BF16)] * 4,
            *[pltpu.VMEM((early, tokens, chunk), BF16)] * 2,
            pltpu.VMEM((early, tokens, chunk), F32),
            dma((2 * early,)), dma((2 * early,)), dma((1,)), dma((1,)), dma((W,)), dma((W,)),
            *[dma((plain, 2))] * 2, *[dma((plain,))] * 2, *[dma((plain, 2))] * 2,
            dma((early,)), dma((early,)),
        ]
    else:
        scratch = [*[pltpu.VMEM((chunks, N, own, chunk), BF16)] * 3, *[dma((chunks, N))] * 4]
    dec_grad, summed, slots = pl.pallas_call(
        functools.partial(step_kernel, W, N, fold, top, chunk, pieces, early),
        out_shape=(
            pltpu.VMEM((latents, channels), BF16),
            pltpu.VMEM((rows, LANES), F32),
            pltpu.VMEM((tokens // W, latents), jnp.int32),
        ),
        in_specs=[vmem, vmem, vmem, hbm, hbm, hbm],
        out_specs=(vmem, vmem, vmem),
        scratch_shapes=[
            pltpu.VMEM((tokens, LANES), jnp.int32),
            pltpu.VMEM((tokens, channels), BF16),
            pltpu.VMEM((channels, latents), BF16),
            pltpu.VMEM((latents, channels), BF16),
            pltpu.VMEM((tokens, latents), jnp.int32),
            pltpu.VMEM((tokens, latents), F32),
            pltpu.VMEM(packed_shape, BF16),
            pltpu.VMEM(packed_shape, BF16),
            pltpu.VMEM(packed_shape, BF16),
            pltpu.VMEM((tokens, latents), BF16),
            pltpu.VMEM((latents, tokens), BF16),
            pltpu.VMEM((tokens, channels), BF16),
            pltpu.VMEM(packed_shape, BF16),
            pltpu.VMEM(packed_shape, BF16),
            dma((3 + pieces,)),
            *[dma((W,))] * 6,
            *scratch,
        ],
        compiler_params=pltpu.CompilerParams(collective_id=0, has_side_effects=True, vmem_limit_bytes=56 * 2**20),
        cost_estimate=pl.CostEstimate(
            flops=8 * tokens * channels * latents, bytes_accessed=6 * channels * (tokens + latents), transcendentals=0
        ),
        name="step",
    )(active_ids.T, enc_bias.reshape(1, -1), dec_bias.reshape(1, -1), activations, enc_weight, dec_weight)
    resident = [pltpu.with_memory_space_constraint(x, pltpu.VMEM) for x in (dec_grad, summed, slots)]
    return pl.pallas_call(
        functools.partial(store_kernel, fold, top),
        out_shape=(
            jax.ShapeDtypeStruct((latents, channels), BF16),
            jax.ShapeDtypeStruct((tokens // W, latents), F32),
        ),
        in_specs=[vmem, vmem, vmem],
        out_specs=(hbm, vmem),
        scratch_shapes=[dma((STORES,))],
        compiler_params=pltpu.CompilerParams(vmem_limit_bytes=2**20),
        name="store",
    )(*resident)


def solution(mesh):
    in_specs = (
        P(None, "wide"),
        P("wide", "narrow"),
        P("narrow"),
        P("narrow", "wide"),
        P("wide"),
        P(),
    )
    out_specs = (P("narrow", "wide"), P("wide", "narrow"))
    return jax.shard_map(local, mesh=mesh, in_specs=in_specs, out_specs=out_specs, check_vma=False)
```

```python
import functools

import jax
import jax.numpy as jnp
from jax import lax
from jax.experimental import pallas as pl
from jax.experimental.pallas import tpu as pltpu
from jax.sharding import PartitionSpec as P

LANES = 128
MESH = pl.DeviceIdType.MESH
F32, BF16 = jnp.float32, jnp.bfloat16


def lookup(table, index):
    return jnp.take_along_axis(table, index, axis=1, mode="promise_in_bounds")


def pick(tables, ids, fold, top):
    tile, lane = ids >> 7, ids & (LANES - 1)
    half = lax.broadcasted_iota(jnp.int32, ids.shape, 1) // top
    picked = jnp.zeros(ids.shape, F32)
    for part in range(fold):
        here = jnp.where(half == part, tile, -1)
        for j, table in enumerate(tables(part)):
            picked = jnp.where(here == j, lookup(table, lane), picked)
    return picked


def spread_row(table, p, top, tiles, slots):
    rows = table.shape[0]
    table = jnp.concatenate([table[:, p * top : (p + 1) * top], jnp.zeros((rows, LANES - top), F32)], axis=1)
    return jnp.concatenate([lookup(table, slots(j)) for j in range(tiles)], axis=1)


def step_kernel(
    W, N, fold, top, chunk, pieces, early,
    ids_t_ref, bias_ref, shift_ref, act_hbm, enc_hbm, dec_hbm,
    dg_ref, sum_ref, own_slot_ref,
    ids, act, enc, dec, slot, total, part, wide_in, values, lat, lat_t,
    err, lg_packed, grad_in,
    load_sem, ws1, wr1, ws2, wr2, ws3, wr3, *scratch,
):
    wide, narrow = lax.axis_index("wide"), lax.axis_index("narrow")
    tokens, latents = lat.shape
    channels = act.shape[1]
    own, rows = tokens // N, part.shape[1]
    chunks = channels // chunk
    piece = latents // pieces
    low = narrow * latents
    half_rows, quarter = tokens // 2, tokens // 4
    near = wide // (W // 2)

    def mate(d):
        goal = 0
        for b in range(W.bit_length() - 1):
            digit = wide // 2**b % 2
            goal = goal + 2**b * (1 - digit if d >> b & 1 else digit)
        return goal

    def rows_of(h):
        return pl.ds(pl.multiple_of(h * half_rows, half_rows), half_rows)

    def piece_cols(n):
        return pl.ds(pl.multiple_of(n * piece, LANES), piece)

    load_act = pltpu.make_async_copy(act_hbm, act, load_sem.at[0])
    head = channels - early * chunk
    load_dec = pltpu.make_async_copy(dec_hbm.at[:, :head], dec.at[:, :head], load_sem.at[1])

    def load_enc(n):
        return pltpu.make_async_copy(enc_hbm.at[:, piece_cols(n)], enc.at[:, piece_cols(n)], load_sem.at[2 + n])

    if early:
        load_rest = pltpu.make_async_copy(dec_hbm.at[:, head:], dec.at[:, head:], load_sem.at[2 + pieces])
        load_rest.start()
    load_act.start()
    for n in range(pieces):
        load_enc(n).start()
    load_dec.start()

    barrier = pltpu.get_barrier_semaphore()
    for d in range(1, W):
        pl.semaphore_signal(barrier, inc=1, device_id={"wide": mate(d)}, device_id_type=MESH)
    for d in range(1, N):
        pl.semaphore_signal(barrier, inc=1, device_id={"narrow": lax.rem(narrow + d, N)}, device_id_type=MESH)

    stacked = jnp.concatenate([ids_t_ref[...]] * fold, axis=0)
    ids[...] = stacked.T

    GROUP, TALL = 16, 256
    bands = latents // TALL
    groups = bands * (tokens // LANES)

    def fill_slots(i, slot, low):
        band, side = i % bands, i // bands
        at = pl.ds(pl.multiple_of(side * LANES, LANES), LANES)
        offset = low + band * TALL
        place = lax.broadcasted_iota(jnp.int32, (GROUP, LANES), 0)
        places = [(place + j * GROUP).astype(jnp.int16) for j in range(TALL // GROUP)]
        found = [jnp.full((GROUP, LANES), top, jnp.int16) for _ in places]
        for k in range(top):
            here = jnp.broadcast_to(ids_t_ref[k : k + 1, at] - offset, (GROUP, LANES)).astype(jnp.int16)
            found = [jnp.where(here == p, jnp.int16(k), f) for p, f in zip(places, found)]
        slot[at, pl.ds(pl.multiple_of(band * TALL, TALL), TALL)] = jnp.concatenate(found, axis=0).T.astype(jnp.int32)

    def slots_of(i, carry):
        fill_slots(i, slot, low)
        return carry

    lax.fori_loop(0, groups // 4, slots_of, 0)
    pl.semaphore_wait(barrier, W + N - 2)

    def narrow_copy(goal, source, target, send, recv):
        return pltpu.make_async_remote_copy(
            src_ref=source, dst_ref=target, send_sem=send, recv_sem=recv,
            device_id={"narrow": goal}, device_id_type=MESH,
        )

    def wide_copy(d, source, target, send, recv):
        return pltpu.make_async_remote_copy(
            src_ref=source, dst_ref=target, send_sem=send.at[d], recv_sem=recv.at[d],
            device_id={"wide": mate(d)}, device_id_type=MESH,
        )

    def columns(c):
        return pl.ds(pl.multiple_of(c * chunk, chunk), chunk)

    if early:
        (
            dec_in, slot_in, values_in, lat_in, rec, rec_in, msg, msg_in, err_out, full, full_in, base,
            ds, dr, vs, vr, vws, vwr, ns1, nr1, ns2, nr2, ns3, nr3, fs, fr,
        ) = scratch
        side, pair = lax.rem(narrow, 2), narrow // 2
        across, along = narrow + 1 - 2 * side, narrow + 2 - 4 * pair
        plain = chunks - early

        PARTS = 2
        tall = latents // PARTS

        def dec_copy(i):
            c, at = i // PARTS, pl.ds(i % PARTS * tall, tall)
            return narrow_copy(
                across, dec.at[at, columns(plain + c)], dec_in.at[at, columns(c)], ds.at[i], dr.at[i]
            )

        load_rest.wait()
        for i in range(early * PARTS):
            dec_copy(i).start()
    else:
        rec, rec_in, err_out, ns1, nr1, ns2, nr2 = scratch

    load_act.wait()

    def encode(h, n):
        total[rows_of(h), piece_cols(n)] = jnp.dot(
            act[rows_of(h), :], enc[:, piece_cols(n)], preferred_element_type=F32
        )

    def encode_far(n, carry):
        load_enc(n).wait()
        encode(1 - near, n)
        return carry

    def encode_near(n, carry):
        encode(near, n)
        return carry

    half = lax.broadcasted_iota(jnp.int32, (rows, LANES), 1) // top

    def block_rows(w, p):
        return pl.ds(pl.multiple_of((w * fold + p) * rows, rows), rows)

    def packed_ids(w):
        out = ids[block_rows(w, 0), :]
        for p in range(1, fold):
            out = jnp.where(half == p, ids[block_rows(w, p), :], out)
        return out - low

    def pick_dense(w):
        def tables(p):
            return [total[block_rows(w, p), j * LANES : (j + 1) * LANES] for j in range(latents // LANES)]

        return pick(tables, packed_ids(w), fold, top)

    def scatter_copy(d, source, target, send, recv):
        return wide_copy(d, source.at[d], target.at[d], send, recv)

    def scatter(first, last, source, target, send, recv):
        picked = None
        for d in range(last - 1, first - 1, -1):
            picked = pick_dense(mate(d))
            if d > 0:
                source[d] = picked.astype(BF16)
                scatter_copy(d, source, target, send, recv).start()
        return picked

    def gather(picked, source, target, send, recv):
        for d in range(1, W):
            scatter_copy(d, source, target, send, recv).wait_recv()
            picked = picked + target[d].astype(F32)
        return picked

    lax.fori_loop(0, pieces, encode_far, 0)
    scatter(W // 2, W, part, wide_in, ws1, wr1)
    lax.fori_loop(0, pieces, encode_near, 0)
    summed = scatter(0, W // 2, part, wide_in, ws1, wr1)

    def bias_tables(p):
        return [jnp.broadcast_to(bias_ref[:, j * LANES : (j + 1) * LANES], (rows, LANES)) for j in range(latents // LANES)]

    summed = summed + pick(bias_tables, packed_ids(wide), fold, top)

    lax.fori_loop(groups // 4, groups * 3 // 4, slots_of, 0)

    values[wide] = gather(summed, part, wide_in, ws1, wr1).astype(BF16)

    def value_copy(d):
        return wide_copy(d, values.at[wide], values.at[wide], ws2, wr2)

    for d in range(W - 1, 0, -1):
        value_copy(d).start()
    if early:
        def pair_values():
            return narrow_copy(across, values.at[wide], values_in.at[wide], vs.at[0], vr.at[0])

        pair_values().start()

    lax.fori_loop(groups * 3 // 4, groups, slots_of, 0)

    def fill_block(block, values, slot, lat):
        table = values[block].astype(F32)
        for p in range(fold):
            at = block_rows(block, p)
            spread = spread_row(table, p, top, latents // LANES, lambda j: slot[at, j * LANES : (j + 1) * LANES])
            lat[at, :] = spread.astype(BF16)

    def fill_mates(first, last):
        for d in range(first, last):
            if d > 0:
                value_copy(d).wait_recv()
            fill_block(mate(d), values, slot, lat)

    load_dec.wait()

    def own_rows(i):
        return pl.ds(pl.multiple_of(i * own, own), own)

    def keep_slots():
        own_slot_ref[...] = slot[pl.ds(pl.multiple_of(wide * (fold * rows), fold * rows), fold * rows), :]

    def flip(j, carry):
        at = pl.ds(pl.multiple_of(j * LANES, LANES), LANES)
        lat_t[at, :] = lat[:, at].T
        return carry

    def decode(c, at=slice(None)):
        return jnp.dot(lat[at, :], dec[:, columns(c)], preferred_element_type=F32)

    def contract(c):
        return lax.dot_general(
            err[:, columns(c)], dec[:, columns(c)], (((1,), (1,)), ((), ())), preferred_element_type=F32
        )

    def outer(c):
        dg_ref[:, columns(c)] = jnp.dot(lat_t[...], err[:, columns(c)], preferred_element_type=F32).astype(BF16)

    def local_chunk(c, carry):
        total[...] += contract(c)
        outer(c)
        return carry

    if early:
        def here(h):
            return pl.ds(pl.multiple_of(h * half_rows + side * quarter, quarter), quarter)

        def scale(count):
            return count.astype(F32)

        own_scale, mate_scale = scale(N - narrow), scale(N - across)
        least = scale(N - jnp.maximum(narrow, across))
        own_use, mate_use = scale(1 + pair * (N - 1 - narrow)), scale(1 + pair * (N - 1 - across))

        def rec_copy(c, q):
            h = near if q == 0 else 1 - near
            return narrow_copy(across, rec.at[c, h, 1 - side], rec_in.at[c, h], ns1.at[c, q], nr1.at[c, q])

        def msg_copy(c):
            return narrow_copy(along, msg.at[c], msg_in.at[c], ns2.at[c], nr2.at[c])

        def err_copy(c, h):
            return narrow_copy(across, err_out.at[c, h], err.at[here(h), columns(c)], ns3.at[c, h], nr3.at[c, h])

        def full_copy(c):
            return narrow_copy(along, full.at[c], full_in.at[c], fs.at[c], fr.at[c])

        def send_part(c, q):
            h = near if q == 0 else 1 - near
            rec[c, h] = decode(c, rows_of(h)).astype(BF16).reshape(2, quarter, chunk)
            rec_copy(c, q).start()

        def send_rec(c, carry):
            rec[c] = decode(c).astype(BF16).reshape(2, 2, quarter, chunk)
            for q in range(2):
                rec_copy(c, q).start()
            return carry

        fill_mates(0, W // 2)
        for c in range(FIRST):
            send_part(c, 0)
        fill_mates(W // 2, W)
        for c in range(FIRST):
            send_part(c, 1)
        lax.fori_loop(FIRST, plain, send_rec, 0)

        def more_slots(i, carry):
            fill_slots(i, slot_in, across * latents)
            return carry

        def send_msg(c):
            for q in range(2):
                rec_copy(c, q).wait_recv()
            msg[c] = (own_use * rec[c, :, side].astype(F32) + mate_use * rec_in[c].astype(F32)).astype(BF16)
            msg_copy(c).start()

        def send_err(c):
            msg_copy(c).wait_recv()
            for h in range(2):
                shift = shift_ref[:, columns(c)] - act[here(h), columns(c)].astype(F32)
                mine_rec, mate_rec = rec[c, h, side].astype(F32), rec_in[c, h].astype(F32)
                other = msg_in[c, h].astype(F32)
                back = mate_scale * (shift + mate_rec) + least * mine_rec + mate_use * other
                err_out[c, h] = (back / N).astype(BF16)
                err_copy(c, h).start()
                back = own_scale * (shift + mine_rec) + least * mate_rec + own_use * other
                err[here(h), columns(c)] = (back / N).astype(BF16)

        def send_full(c, carry):
            mine_rec = decode(plain + c)
            mate_rec = jnp.dot(lat_in[...], dec_in[:, columns(c)], preferred_element_type=F32)
            full[c] = (own_use * mine_rec + mate_use * mate_rec).astype(BF16)
            full_copy(c).start()
            shift = shift_ref[:, columns(plain + c)] - act[:, columns(plain + c)].astype(F32)
            base[c] = own_scale * (shift + mine_rec) + least * mate_rec
            return carry

        def take_full(c, carry):
            full_copy(c).wait_recv()
            err[:, columns(plain + c)] = ((base[c] + own_use * full_in[c].astype(F32)) / N).astype(BF16)
            return carry

        def values_copies():
            return [wide_copy(d, values_in.at[wide], values_in.at[wide], vws, vwr) for d in range(1, W)]

        def arrive(c):
            for h in range(2):
                err_copy(c, h).wait_recv()

        def take(c):
            arrive(c)
            local_chunk(c, 0)

        pair_values().wait_recv()
        for copy in values_copies():
            copy.start()
        keep_slots()
        lax.fori_loop(0, latents // LANES, flip, 0)
        total[...] = jnp.zeros_like(total)
        lax.fori_loop(0, groups // 2, more_slots, 0)
        for c in range(plain):
            send_msg(c)
            if c >= LAG:
                send_err(c - LAG)
            if c < 2:
                lax.fori_loop((2 + c) * groups // 4, (3 + c) * groups // 4, more_slots, 0)
            if c == 2:
                for copy in values_copies():
                    copy.wait_recv()
                for block in range(W):
                    fill_block(block, values_in, slot_in, lat_in)
        for i in range(early * PARTS):
            dec_copy(i).wait_recv()
        lax.fori_loop(0, early, send_full, 0)
        for c in range(LAG):
            send_err(plain - LAG + c)
            take(c)


        def finish(c, carry):
            for q in range(2):
                rec_copy(c, q).wait_send()
                err_copy(c, q).wait_send()
            msg_copy(c).wait_send()
            return carry

        def finish_early():
            for i in range(early * PARTS):
                dec_copy(i).wait_send()
            for c in range(early):
                full_copy(c).wait_send()
            pair_values().wait_send()
            for copy in values_copies():
                copy.wait_send()
    else:
        plain = chunks
        fill_mates(0, W)
        keep_slots()

        def goal_of(d):
            return lax.rem(narrow + d, N)

        def rec_copy(c, d):
            return narrow_copy(goal_of(d), rec.at[c, goal_of(d)], rec_in.at[c, d], ns1.at[c, d], nr1.at[c, d])

        def err_copy(c, d):
            return narrow_copy(
                goal_of(d), err_out.at[c, d], err.at[own_rows(narrow), columns(c)], ns2.at[c, d], nr2.at[c, d]
            )

        def send_rec(c, carry):
            rec[c] = decode(c).astype(BF16).reshape(N, own, chunk)
            for d in range(1, N):
                rec_copy(c, d).start()
            return carry

        lax.fori_loop(0, chunks, send_rec, 0)

        def combine(c, carry):
            for d in range(1, N):
                rec_copy(c, d).wait_recv()
            shift = shift_ref[:, columns(c)] - act[own_rows(narrow), columns(c)].astype(F32)
            terms = [rec[c, narrow].astype(F32)]
            terms += [rec_in[c, d].astype(F32) for d in range(1, N)]
            for e in range(N):
                goal = goal_of(e)
                back = (N - goal).astype(F32) * shift
                for d in range(N):
                    origin = lax.rem(narrow + N - d, N)
                    back = back + (N - jnp.maximum(goal, origin)).astype(F32) * terms[d]
                back = (back / N).astype(BF16)
                if e == 0:
                    err[own_rows(narrow), columns(c)] = back
                else:
                    err_out[c, e] = back
                    err_copy(c, e).start()
            return carry

        lax.fori_loop(0, chunks, combine, 0)
        lax.fori_loop(0, latents // LANES, flip, 0)

        def arrive(c):
            for d in range(1, N):
                err_copy(c, d).wait_recv()

        def finish(c, carry):
            for d in range(1, N):
                rec_copy(c, d).wait_send()
                err_copy(c, d).wait_send()
            return carry

        def finish_early():
            pass

    def sent_chunk(c, carry):
        arrive(c)
        return local_chunk(c, carry)

    if early:
        lax.fori_loop(LAG, plain - 1, sent_chunk, 0)
        lax.fori_loop(0, early, take_full, 0)
        lax.fori_loop(plain, chunks, local_chunk, 0)
    else:
        total[...] = jnp.zeros_like(total)
        lax.fori_loop(0, plain - 1, sent_chunk, 0)
    arrive(plain - 1)
    total[...] += contract(plain - 1)

    summed = scatter(0, W, lg_packed, grad_in, ws3, wr3)
    outer(plain - 1)
    sum_ref[...] = gather(summed, lg_packed, grad_in, ws3, wr3)

    for d in range(1, W):
        scatter_copy(d, part, wide_in, ws1, wr1).wait_send()
        value_copy(d).wait_send()
        scatter_copy(d, lg_packed, grad_in, ws3, wr3).wait_send()

    lax.fori_loop(0, plain, finish, 0)
    finish_early()


STORES = 4
FIRST, LAG = 3, 3


def store_kernel(fold, top, dg_ref, sum_ref, slot_ref, dg_hbm, grad_ref, sem):
    step = dg_ref.shape[0] // STORES
    rows = sum_ref.shape[0]
    copies = []
    for i in range(STORES):
        at = pl.ds(i * step, step)
        copies.append(pltpu.make_async_copy(dg_ref.at[at], dg_hbm.at[at], sem.at[i]))
    for copy in copies:
        copy.start()
    for p in range(fold):
        at = slice(p * rows, (p + 1) * rows)
        grad_ref[at, :] = spread_row(sum_ref[...], p, top, slot_ref.shape[1] // LANES, lambda j: slot_ref[at, j * LANES : (j + 1) * LANES])
    for copy in copies:
        copy.wait()


def local(activations, enc_weight, enc_bias, dec_weight, dec_bias, active_ids):
    W, N = lax.axis_size("wide"), lax.axis_size("narrow")
    tokens, channels = activations.shape
    latents = enc_weight.shape[1]
    top = active_ids.shape[1]
    fold = LANES // top
    rows = tokens // W // fold
    chunk = min(channels, 256)
    chunks = channels // chunk
    pieces = 4
    own = tokens // N
    early = chunks // 8 if N == 4 else 0
    plain = chunks - early
    half = (plain, 2, tokens // 4, chunk)
    packed_shape = (W, rows, LANES)
    vmem = pl.BlockSpec(memory_space=pltpu.VMEM)
    hbm = pl.BlockSpec(memory_space=pl.ANY)
    dma = pltpu.SemaphoreType.DMA
    if early:
        scratch = [
            pltpu.VMEM((latents, early * chunk), BF16),
            pltpu.VMEM((tokens, latents), jnp.int32),
            pltpu.VMEM(packed_shape, BF16),
            pltpu.VMEM((tokens, latents), BF16),
            pltpu.VMEM((plain, 2, 2, tokens // 4, chunk), BF16),
            *[pltpu.VMEM(half, BF16)] * 4,
            *[pltpu.VMEM((early, tokens, chunk), BF16)] * 2,
            pltpu.VMEM((early, tokens, chunk), F32),
            dma((2 * early,)), dma((2 * early,)), dma((1,)), dma((1,)), dma((W,)), dma((W,)),
            *[dma((plain, 2))] * 2, *[dma((plain,))] * 2, *[dma((plain, 2))] * 2,
            dma((early,)), dma((early,)),
        ]
    else:
        scratch = [*[pltpu.VMEM((chunks, N, own, chunk), BF16)] * 3, *[dma((chunks, N))] * 4]
    dec_grad, summed, slots = pl.pallas_call(
        functools.partial(step_kernel, W, N, fold, top, chunk, pieces, early),
        out_shape=(
            pltpu.VMEM((latents, channels), BF16),
            pltpu.VMEM((rows, LANES), F32),
            pltpu.VMEM((tokens // W, latents), jnp.int32),
        ),
        in_specs=[vmem, vmem, vmem, hbm, hbm, hbm],
        out_specs=(vmem, vmem, vmem),
        scratch_shapes=[
            pltpu.VMEM((tokens, LANES), jnp.int32),
            pltpu.VMEM((tokens, channels), BF16),
            pltpu.VMEM((channels, latents), BF16),
            pltpu.VMEM((latents, channels), BF16),
            pltpu.VMEM((tokens, latents), jnp.int32),
            pltpu.VMEM((tokens, latents), F32),
            pltpu.VMEM(packed_shape, BF16),
            pltpu.VMEM(packed_shape, BF16),
            pltpu.VMEM(packed_shape, BF16),
            pltpu.VMEM((tokens, latents), BF16),
            pltpu.VMEM((latents, tokens), BF16),
            pltpu.VMEM((tokens, channels), BF16),
            pltpu.VMEM(packed_shape, BF16),
            pltpu.VMEM(packed_shape, BF16),
            dma((3 + pieces,)),
            *[dma((W,))] * 6,
            *scratch,
        ],
        compiler_params=pltpu.CompilerParams(collective_id=0, has_side_effects=True, vmem_limit_bytes=56 * 2**20),
        cost_estimate=pl.CostEstimate(
            flops=8 * tokens * channels * latents, bytes_accessed=6 * channels * (tokens + latents), transcendentals=0
        ),
        name="step",
    )(active_ids.T, enc_bias.reshape(1, -1), dec_bias.reshape(1, -1), activations, enc_weight, dec_weight)
    resident = [pltpu.with_memory_space_constraint(x, pltpu.VMEM) for x in (dec_grad, summed, slots)]
    return pl.pallas_call(
        functools.partial(store_kernel, fold, top),
        out_shape=(
            jax.ShapeDtypeStruct((latents, channels), BF16),
            jax.ShapeDtypeStruct((tokens // W, latents), F32),
        ),
        in_specs=[vmem, vmem, vmem],
        out_specs=(hbm, vmem),
        scratch_shapes=[dma((STORES,))],
        compiler_params=pltpu.CompilerParams(vmem_limit_bytes=2**20),
        name="store",
    )(*resident)


def solution(mesh):
    in_specs = (
        P(None, "wide"),
        P("wide", "narrow"),
        P("narrow"),
        P("narrow", "wide"),
        P("wide"),
        P(),
    )
    out_specs = (P("narrow", "wide"), P("wide", "narrow"))
    return jax.shard_map(local, mesh=mesh, in_specs=in_specs, out_specs=out_specs, check_vma=False)
```

```python
import functools

import jax
import jax.numpy as jnp
from jax import lax
from jax.experimental import pallas as pl
from jax.experimental.pallas import tpu as pltpu
from jax.sharding import PartitionSpec as P

LANES = 128
MESH = pl.DeviceIdType.MESH
F32, BF16 = jnp.float32, jnp.bfloat16


def lookup(table, index):
    return jnp.take_along_axis(table, index, axis=1, mode="promise_in_bounds")


def pick(tables, ids, fold, top):
    tile, lane = ids >> 7, ids & (LANES - 1)
    half = lax.broadcasted_iota(jnp.int32, ids.shape, 1) // top
    picked = jnp.zeros(ids.shape, F32)
    for part in range(fold):
        here = jnp.where(half == part, tile, -1)
        for j, table in enumerate(tables(part)):
            picked = jnp.where(here == j, lookup(table, lane), picked)
    return picked


def spread_row(table, p, top, tiles, slots):
    rows = table.shape[0]
    table = jnp.concatenate([table[:, p * top : (p + 1) * top], jnp.zeros((rows, LANES - top), F32)], axis=1)
    return jnp.concatenate([lookup(table, slots(j)) for j in range(tiles)], axis=1)


def step_kernel(
    W, N, fold, top, chunk, pieces, early,
    ids_hbm, bias_hbm, shift_hbm, act_hbm, enc_hbm, dec_hbm,
    dg_ref, sum_ref, own_slot_ref,
    ids_t_ref, bias_ref, shift_ref, ids, act, enc, dec, slot, total, part, wide_in, values, lat, lat_t,
    err, lg_packed, grad_in,
    load_sem, ws1, wr1, ws2, wr2, ws3, wr3, *scratch,
):
    wide, narrow = lax.axis_index("wide"), lax.axis_index("narrow")
    tokens, latents = lat.shape
    channels = act.shape[1]
    own, rows = tokens // N, part.shape[1]
    chunks = channels // chunk
    piece = latents // pieces
    low = narrow * latents
    half_rows, quarter = tokens // 2, tokens // 4
    near = wide // (W // 2)

    def mate(d):
        goal = 0
        for b in range(W.bit_length() - 1):
            digit = wide // 2**b % 2
            goal = goal + 2**b * (1 - digit if d >> b & 1 else digit)
        return goal

    def rows_of(h):
        return pl.ds(pl.multiple_of(h * half_rows, half_rows), half_rows)

    def piece_cols(n):
        return pl.ds(pl.multiple_of(n * piece, LANES), piece)

    def load(source, target, i):
        return pltpu.make_async_copy(source, target, load_sem.at[i])

    def load_act(h, i):
        return load(act_hbm.at[rows_of(h)], act.at[rows_of(h)], i)

    load_dec = load(dec_hbm, dec, 1)
    load_ids = load(ids_hbm, ids_t_ref, 2)
    load_bias = load(bias_hbm, bias_ref, 3)
    load_shift = load(shift_hbm, shift_ref, 4)

    def load_enc(n):
        return load(enc_hbm.at[:, piece_cols(n)], enc.at[:, piece_cols(n)], 5 + n)

    load_ids.start()
    load_act(1 - near, 0).start()
    for n in range(AHEAD):
        load_enc(n).start()
    load_act(near, 5 + pieces).start()
    load_bias.start()
    load_shift.start()

    barrier = pltpu.get_barrier_semaphore()
    for d in range(1, W):
        pl.semaphore_signal(barrier, inc=1, device_id={"wide": mate(d)}, device_id_type=MESH)
    for d in range(1, N):
        pl.semaphore_signal(barrier, inc=1, device_id={"narrow": lax.rem(narrow + d, N)}, device_id_type=MESH)

    load_ids.wait()
    for n in range(AHEAD, pieces):
        load_enc(n).start()
    stacked = jnp.concatenate([ids_t_ref[...]] * fold, axis=0)
    ids[...] = stacked.T

    GROUP, TALL = 16, 256
    bands = latents // TALL
    groups = bands * (tokens // LANES)

    def fill_slots(i, slot, low):
        band, side = i % bands, i // bands
        at = pl.ds(pl.multiple_of(side * LANES, LANES), LANES)
        offset = low + band * TALL
        place = lax.broadcasted_iota(jnp.int32, (GROUP, LANES), 0)
        places = [(place + j * GROUP).astype(jnp.int16) for j in range(TALL // GROUP)]
        found = [jnp.full((GROUP, LANES), top, jnp.int16) for _ in places]
        for k in range(top):
            here = jnp.broadcast_to(ids_t_ref[k : k + 1, at] - offset, (GROUP, LANES)).astype(jnp.int16)
            found = [jnp.where(here == p, jnp.int16(k), f) for p, f in zip(places, found)]
        slot[at, pl.ds(pl.multiple_of(band * TALL, TALL), TALL)] = jnp.concatenate(found, axis=0).T.astype(jnp.int32)

    def slots_of(i, carry):
        fill_slots(i, slot, low)
        return carry

    pl.semaphore_wait(barrier, W + N - 2)

    def narrow_copy(goal, source, target, send, recv):
        return pltpu.make_async_remote_copy(
            src_ref=source, dst_ref=target, send_sem=send, recv_sem=recv,
            device_id={"narrow": goal}, device_id_type=MESH,
        )

    def wide_copy(d, source, target, send, recv):
        return pltpu.make_async_remote_copy(
            src_ref=source, dst_ref=target, send_sem=send.at[d], recv_sem=recv.at[d],
            device_id={"wide": mate(d)}, device_id_type=MESH,
        )

    def columns(c):
        return pl.ds(pl.multiple_of(c * chunk, chunk), chunk)

    if early:
        (
            dec_in, slot_in, values_in, lat_in, rec, rec_in, msg, msg_in, err_out, full, full_in, base,
            ds, dr, vs, vr, vws, vwr, ns1, nr1, ns2, nr2, ns3, nr3, fs, fr,
        ) = scratch
        side, pair = lax.rem(narrow, 2), narrow // 2
        across, along = narrow + 1 - 2 * side, narrow + 2 - 4 * pair
        plain = chunks - early

        PARTS = 2
        tall = latents // PARTS

        def dec_copy(i):
            c, at = i // PARTS, pl.ds(i % PARTS * tall, tall)
            return narrow_copy(
                across, dec_hbm.at[at, columns(plain + c)], dec_in.at[at, columns(c)], ds.at[i], dr.at[i]
            )

        for i in range(early * PARTS):
            dec_copy(i).start()
    else:
        rec, rec_in, err_out, ns1, nr1, ns2, nr2 = scratch

    lax.fori_loop(0, groups // HEAD, slots_of, 0)
    load_act(1 - near, 0).wait()

    def encode(h, n):
        total[rows_of(h), piece_cols(n)] = jnp.dot(
            act[rows_of(h), :], enc[:, piece_cols(n)], preferred_element_type=F32
        )

    def encode_far(n, carry):
        load_enc(n).wait()
        encode(1 - near, n)
        return carry

    def encode_near(n, carry):
        encode(near, n)
        return carry

    half = lax.broadcasted_iota(jnp.int32, (rows, LANES), 1) // top

    def block_rows(w, p):
        return pl.ds(pl.multiple_of((w * fold + p) * rows, rows), rows)

    def packed_ids(w):
        out = ids[block_rows(w, 0), :]
        for p in range(1, fold):
            out = jnp.where(half == p, ids[block_rows(w, p), :], out)
        return out - low

    def pick_dense(w):
        def tables(p):
            return [total[block_rows(w, p), j * LANES : (j + 1) * LANES] for j in range(latents // LANES)]

        return pick(tables, packed_ids(w), fold, top)

    def scatter_copy(d, source, target, send, recv):
        return wide_copy(d, source.at[d], target.at[d], send, recv)

    def scatter(first, last, source, target, send, recv):
        picked = None
        for d in range(last - 1, first - 1, -1):
            picked = pick_dense(mate(d))
            if d > 0:
                source[d] = picked.astype(BF16)
                scatter_copy(d, source, target, send, recv).start()
        return picked

    def gather(picked, source, target, send, recv):
        for d in range(1, W):
            scatter_copy(d, source, target, send, recv).wait_recv()
            picked = picked + target[d].astype(F32)
        return picked

    lax.fori_loop(0, pieces, encode_far, 0)
    load_dec.start()
    scatter(W // 2, W, part, wide_in, ws1, wr1)
    load_act(near, 5 + pieces).wait()
    lax.fori_loop(0, pieces, encode_near, 0)
    summed = scatter(0, W // 2, part, wide_in, ws1, wr1)

    def bias_tables(p):
        return [jnp.broadcast_to(bias_ref[:, j * LANES : (j + 1) * LANES], (rows, LANES)) for j in range(latents // LANES)]

    load_bias.wait()
    load_shift.wait()
    summed = summed + pick(bias_tables, packed_ids(wide), fold, top)

    lax.fori_loop(groups // HEAD, groups * 3 // 4, slots_of, 0)

    values[wide] = gather(summed, part, wide_in, ws1, wr1).astype(BF16)

    def value_copy(d):
        return wide_copy(d, values.at[wide], values.at[wide], ws2, wr2)

    for d in range(W - 1, 0, -1):
        value_copy(d).start()
    if early:
        def pair_values():
            return narrow_copy(across, values.at[wide], values_in.at[wide], vs.at[0], vr.at[0])

        pair_values().start()

    lax.fori_loop(groups * 3 // 4, groups, slots_of, 0)

    def fill_block(block, values, slot, lat):
        table = values[block].astype(F32)
        for p in range(fold):
            at = block_rows(block, p)
            spread = spread_row(table, p, top, latents // LANES, lambda j: slot[at, j * LANES : (j + 1) * LANES])
            lat[at, :] = spread.astype(BF16)

    def fill_mates(first, last):
        for d in range(first, last):
            if d > 0:
                value_copy(d).wait_recv()
            fill_block(mate(d), values, slot, lat)

    load_dec.wait()

    def own_rows(i):
        return pl.ds(pl.multiple_of(i * own, own), own)

    def keep_slots():
        own_slot_ref[...] = slot[pl.ds(pl.multiple_of(wide * (fold * rows), fold * rows), fold * rows), :]

    def flip(j, carry):
        at = pl.ds(pl.multiple_of(j * LANES, LANES), LANES)
        lat_t[at, :] = lat[:, at].T
        return carry

    def decode(c, at=slice(None)):
        return jnp.dot(lat[at, :], dec[:, columns(c)], preferred_element_type=F32)

    def contract(c, at=slice(None)):
        return lax.dot_general(
            err[at, columns(c)], dec[:, columns(c)], (((1,), (1,)), ((), ())), preferred_element_type=F32
        )

    def outer(c):
        dg_ref[:, columns(c)] = jnp.dot(lat_t[...], err[:, columns(c)], preferred_element_type=F32).astype(BF16)

    def local_chunk(c, carry):
        total[...] += contract(c)
        outer(c)
        return carry

    if early:
        def here(h):
            return pl.ds(pl.multiple_of(h * half_rows + side * quarter, quarter), quarter)

        def scale(count):
            return count.astype(F32)

        own_scale, mate_scale = scale(N - narrow), scale(N - across)
        least = scale(N - jnp.maximum(narrow, across))
        own_use, mate_use = scale(1 + pair * (N - 1 - narrow)), scale(1 + pair * (N - 1 - across))

        def rec_copy(c, q):
            h = near if q == 0 else 1 - near
            return narrow_copy(across, rec.at[c, h, 1 - side], rec_in.at[c, h], ns1.at[c, q], nr1.at[c, q])

        def msg_copy(c):
            return narrow_copy(along, msg.at[c], msg_in.at[c], ns2.at[c], nr2.at[c])

        def err_copy(c, h):
            return narrow_copy(across, err_out.at[c, h], err.at[here(h), columns(c)], ns3.at[c, h], nr3.at[c, h])

        def full_copy(c):
            return narrow_copy(along, full.at[c], full_in.at[c], fs.at[c], fr.at[c])

        def send_part(c, q):
            h = near if q == 0 else 1 - near
            rec[c, h] = decode(c, rows_of(h)).astype(BF16).reshape(2, quarter, chunk)
            rec_copy(c, q).start()

        def send_rec(c, carry):
            rec[c] = decode(c).astype(BF16).reshape(2, 2, quarter, chunk)
            for q in range(2):
                rec_copy(c, q).start()
            return carry

        fill_mates(0, W // 2)
        for c in range(FIRST):
            send_part(c, 0)
        fill_mates(W // 2, W)
        for c in range(FIRST):
            send_part(c, 1)
        lax.fori_loop(FIRST, plain, send_rec, 0)

        def more_slots(i, carry):
            fill_slots(i, slot_in, across * latents)
            return carry

        def send_msg(c):
            for q in range(2):
                rec_copy(c, q).wait_recv()
            msg[c] = (own_use * rec[c, :, side].astype(F32) + mate_use * rec_in[c].astype(F32)).astype(BF16)
            msg_copy(c).start()

        def send_err(c):
            msg_copy(c).wait_recv()
            for h in range(2):
                shift = shift_ref[:, columns(c)] - act[here(h), columns(c)].astype(F32)
                mine_rec, mate_rec = rec[c, h, side].astype(F32), rec_in[c, h].astype(F32)
                other = msg_in[c, h].astype(F32)
                back = mate_scale * (shift + mate_rec) + least * mine_rec + mate_use * other
                err_out[c, h] = (back / N).astype(BF16)
                err_copy(c, h).start()
                back = own_scale * (shift + mine_rec) + least * mate_rec + own_use * other
                err[here(h), columns(c)] = (back / N).astype(BF16)

        def send_full(c, carry):
            mine_rec = decode(plain + c)
            mate_rec = jnp.dot(lat_in[...], dec_in[:, columns(c)], preferred_element_type=F32)
            full[c] = (own_use * mine_rec + mate_use * mate_rec).astype(BF16)
            full_copy(c).start()
            shift = shift_ref[:, columns(plain + c)] - act[:, columns(plain + c)].astype(F32)
            base[c] = own_scale * (shift + mine_rec) + least * mate_rec
            return carry

        def take_full(c, carry):
            full_copy(c).wait_recv()
            err[:, columns(plain + c)] = ((base[c] + own_use * full_in[c].astype(F32)) / N).astype(BF16)
            return carry

        def values_copies():
            return [wide_copy(d, values_in.at[wide], values_in.at[wide], vws, vwr) for d in range(1, W)]

        def arrive(c):
            for h in range(2):
                err_copy(c, h).wait_recv()

        def take(c):
            arrive(c)
            local_chunk(c, 0)

        pair_values().wait_recv()
        for copy in values_copies():
            copy.start()
        keep_slots()
        lax.fori_loop(0, latents // LANES, flip, 0)
        total[...] = jnp.zeros_like(total)
        lax.fori_loop(0, groups // 2, more_slots, 0)
        for c in range(plain):
            send_msg(c)
            if c >= LAG:
                send_err(c - LAG)
            if c < 2:
                lax.fori_loop((2 + c) * groups // 4, (3 + c) * groups // 4, more_slots, 0)
            if c == 2:
                for copy in values_copies():
                    copy.wait_recv()
                for block in range(W):
                    fill_block(block, values_in, slot_in, lat_in)
        for i in range(early * PARTS):
            dec_copy(i).wait_recv()
        lax.fori_loop(0, early, send_full, 0)
        for c in range(LAG):
            send_err(plain - LAG + c)
            take(c)


        def finish(c, carry):
            for q in range(2):
                rec_copy(c, q).wait_send()
                err_copy(c, q).wait_send()
            msg_copy(c).wait_send()
            return carry

        def finish_early():
            for i in range(early * PARTS):
                dec_copy(i).wait_send()
            for c in range(early):
                full_copy(c).wait_send()
            pair_values().wait_send()
            for copy in values_copies():
                copy.wait_send()
    else:
        plain = chunks
        fill_mates(0, W)
        keep_slots()

        def goal_of(d):
            return lax.rem(narrow + d, N)

        def rec_copy(c, d):
            return narrow_copy(goal_of(d), rec.at[c, goal_of(d)], rec_in.at[c, d], ns1.at[c, d], nr1.at[c, d])

        def err_copy(c, d):
            return narrow_copy(
                goal_of(d), err_out.at[c, d], err.at[own_rows(narrow), columns(c)], ns2.at[c, d], nr2.at[c, d]
            )

        def send_rec(c, carry):
            rec[c] = decode(c).astype(BF16).reshape(N, own, chunk)
            for d in range(1, N):
                rec_copy(c, d).start()
            return carry

        lax.fori_loop(0, chunks, send_rec, 0)

        def combine(c, carry):
            for d in range(1, N):
                rec_copy(c, d).wait_recv()
            shift = shift_ref[:, columns(c)] - act[own_rows(narrow), columns(c)].astype(F32)
            terms = [rec[c, narrow].astype(F32)]
            terms += [rec_in[c, d].astype(F32) for d in range(1, N)]
            for e in range(N):
                goal = goal_of(e)
                back = (N - goal).astype(F32) * shift
                for d in range(N):
                    origin = lax.rem(narrow + N - d, N)
                    back = back + (N - jnp.maximum(goal, origin)).astype(F32) * terms[d]
                back = (back / N).astype(BF16)
                if e == 0:
                    err[own_rows(narrow), columns(c)] = back
                else:
                    err_out[c, e] = back
                    err_copy(c, e).start()
            return carry

        lax.fori_loop(0, chunks, combine, 0)
        lax.fori_loop(0, latents // LANES, flip, 0)

        def arrive(c):
            for d in range(1, N):
                err_copy(c, d).wait_recv()

        def finish(c, carry):
            for d in range(1, N):
                rec_copy(c, d).wait_send()
                err_copy(c, d).wait_send()
            return carry

        def finish_early():
            pass

    def sent_chunk(c, carry):
        arrive(c)
        return local_chunk(c, carry)

    if early:
        lax.fori_loop(LAG, plain - 1, sent_chunk, 0)
        lax.fori_loop(0, early, take_full, 0)
        lax.fori_loop(plain, chunks, local_chunk, 0)
    else:
        total[...] = jnp.zeros_like(total)
        lax.fori_loop(0, plain - 1, sent_chunk, 0)
    arrive(plain - 1)
    total[rows_of(1 - near), :] += contract(plain - 1, rows_of(1 - near))
    scatter(W // 2, W, lg_packed, grad_in, ws3, wr3)
    total[rows_of(near), :] += contract(plain - 1, rows_of(near))
    summed = scatter(0, W // 2, lg_packed, grad_in, ws3, wr3)
    outer(plain - 1)
    sum_ref[...] = gather(summed, lg_packed, grad_in, ws3, wr3)

    for d in range(1, W):
        scatter_copy(d, part, wide_in, ws1, wr1).wait_send()
        value_copy(d).wait_send()
        scatter_copy(d, lg_packed, grad_in, ws3, wr3).wait_send()

    lax.fori_loop(0, plain, finish, 0)
    finish_early()


STORES = 4
AHEAD, HEAD = 1, 8
FIRST, LAG = 3, 3


def store_kernel(fold, top, dg_ref, sum_ref, slot_ref, dg_hbm, grad_hbm, grad_ref, sem):
    step = dg_ref.shape[0] // STORES
    rows = sum_ref.shape[0]
    copies = []
    for i in range(STORES):
        at = pl.ds(i * step, step)
        copies.append(pltpu.make_async_copy(dg_ref.at[at], dg_hbm.at[at], sem.at[i]))
    for copy in copies:
        copy.start()
    for p in range(fold):
        at = slice(p * rows, (p + 1) * rows)
        grad_ref[at, :] = spread_row(sum_ref[...], p, top, slot_ref.shape[1] // LANES, lambda j: slot_ref[at, j * LANES : (j + 1) * LANES])
    copies.append(pltpu.make_async_copy(grad_ref, grad_hbm, sem.at[STORES]))
    copies[-1].start()
    for copy in copies:
        copy.wait()


def local(activations, enc_weight, enc_bias, dec_weight, dec_bias, active_ids):
    W, N = lax.axis_size("wide"), lax.axis_size("narrow")
    tokens, channels = activations.shape
    latents = enc_weight.shape[1]
    top = active_ids.shape[1]
    fold = LANES // top
    rows = tokens // W // fold
    chunk = min(channels, 256)
    chunks = channels // chunk
    pieces = 1
    own = tokens // N
    early = chunks // 8 if N == 4 else 0
    plain = chunks - early
    half = (plain, 2, tokens // 4, chunk)
    packed_shape = (W, rows, LANES)
    vmem = pl.BlockSpec(memory_space=pltpu.VMEM)
    hbm = pl.BlockSpec(memory_space=pl.ANY)
    dma = pltpu.SemaphoreType.DMA
    if early:
        scratch = [
            pltpu.VMEM((latents, early * chunk), BF16),
            pltpu.VMEM((tokens, latents), jnp.int32),
            pltpu.VMEM(packed_shape, BF16),
            pltpu.VMEM((tokens, latents), BF16),
            pltpu.VMEM((plain, 2, 2, tokens // 4, chunk), BF16),
            *[pltpu.VMEM(half, BF16)] * 4,
            *[pltpu.VMEM((early, tokens, chunk), BF16)] * 2,
            pltpu.VMEM((early, tokens, chunk), F32),
            dma((2 * early,)), dma((2 * early,)), dma((1,)), dma((1,)), dma((W,)), dma((W,)),
            *[dma((plain, 2))] * 2, *[dma((plain,))] * 2, *[dma((plain, 2))] * 2,
            dma((early,)), dma((early,)),
        ]
    else:
        scratch = [*[pltpu.VMEM((chunks, N, own, chunk), BF16)] * 3, *[dma((chunks, N))] * 4]
    dec_grad, summed, slots = pl.pallas_call(
        functools.partial(step_kernel, W, N, fold, top, chunk, pieces, early),
        out_shape=(
            pltpu.VMEM((latents, channels), BF16),
            pltpu.VMEM((rows, LANES), F32),
            pltpu.VMEM((tokens // W, latents), jnp.int32),
        ),
        in_specs=[hbm] * 6,
        out_specs=(vmem, vmem, vmem),
        scratch_shapes=[
            pltpu.VMEM((top, tokens), jnp.int32),
            pltpu.VMEM((1, latents), F32),
            pltpu.VMEM((1, channels), F32),
            pltpu.VMEM((tokens, LANES), jnp.int32),
            pltpu.VMEM((tokens, channels), BF16),
            pltpu.VMEM((channels, latents), BF16),
            pltpu.VMEM((latents, channels), BF16),
            pltpu.VMEM((tokens, latents), jnp.int32),
            pltpu.VMEM((tokens, latents), F32),
            pltpu.VMEM(packed_shape, BF16),
            pltpu.VMEM(packed_shape, BF16),
            pltpu.VMEM(packed_shape, BF16),
            pltpu.VMEM((tokens, latents), BF16),
            pltpu.VMEM((latents, tokens), BF16),
            pltpu.VMEM((tokens, channels), BF16),
            pltpu.VMEM(packed_shape, BF16),
            pltpu.VMEM(packed_shape, BF16),
            dma((6 + pieces,)),
            *[dma((W,))] * 6,
            *scratch,
        ],
        compiler_params=pltpu.CompilerParams(collective_id=0, has_side_effects=True, vmem_limit_bytes=56 * 2**20),
        cost_estimate=pl.CostEstimate(
            flops=8 * tokens * channels * latents, bytes_accessed=6 * channels * (tokens + latents), transcendentals=0
        ),
        name="step",
    )(active_ids.T, enc_bias.reshape(1, -1), dec_bias.reshape(1, -1), activations, enc_weight, dec_weight)
    resident = [pltpu.with_memory_space_constraint(x, pltpu.VMEM) for x in (dec_grad, summed, slots)]
    return pl.pallas_call(
        functools.partial(store_kernel, fold, top),
        out_shape=(
            jax.ShapeDtypeStruct((latents, channels), BF16),
            jax.ShapeDtypeStruct((tokens // W, latents), F32),
        ),
        in_specs=[vmem, vmem, vmem],
        out_specs=(hbm, hbm),
        scratch_shapes=[pltpu.VMEM((tokens // W, latents), F32), dma((STORES + 1,))],
        compiler_params=pltpu.CompilerParams(vmem_limit_bytes=2**20),
        name="store",
    )(*resident)


def solution(mesh):
    in_specs = (
        P(None, "wide"),
        P("wide", "narrow"),
        P("narrow"),
        P("narrow", "wide"),
        P("wide"),
        P(),
    )
    out_specs = (P("narrow", "wide"), P("wide", "narrow"))
    return jax.shard_map(local, mesh=mesh, in_specs=in_specs, out_specs=out_specs, check_vma=False)
```

```python
import functools

import jax
import jax.numpy as jnp
from jax import lax
from jax.experimental import pallas as pl
from jax.experimental.pallas import tpu as pltpu
from jax.sharding import PartitionSpec as P

LANES = 128
MESH = pl.DeviceIdType.MESH
F32, BF16 = jnp.float32, jnp.bfloat16


def lookup(table, index):
    return jnp.take_along_axis(table, index, axis=1, mode="promise_in_bounds")


def pick(tables, ids, fold, top):
    tile, lane = ids >> 7, ids & (LANES - 1)
    half = lax.broadcasted_iota(jnp.int32, ids.shape, 1) // top
    picked = jnp.zeros(ids.shape, F32)
    for part in range(fold):
        here = jnp.where(half == part, tile, -1)
        for j, table in enumerate(tables(part)):
            picked = jnp.where(here == j, lookup(table, lane), picked)
    return picked


def spread_row(table, p, top, tiles, slots):
    rows = table.shape[0]
    table = jnp.concatenate([table[:, p * top : (p + 1) * top], jnp.zeros((rows, LANES - top), F32)], axis=1)
    return jnp.concatenate([lookup(table, slots(j)) for j in range(tiles)], axis=1)


def step_kernel(
    W, N, fold, top, chunk, pieces, early,
    ids_hbm, bias_hbm, shift_hbm, act_hbm, enc_hbm, dec_hbm,
    dg_ref, sum_ref, own_slot_ref,
    ids_t_ref, bias_ref, shift_ref, ids, act, enc, dec, slot, total, part, wide_in, values, lat, lat_t,
    err, lg_packed, grad_in,
    load_sem, ws1, wr1, ws2, wr2, ws3, wr3, *scratch,
):
    wide, narrow = lax.axis_index("wide"), lax.axis_index("narrow")
    tokens, latents = lat.shape
    channels = act.shape[1]
    own, rows = tokens // N, part.shape[1]
    chunks = channels // chunk
    piece = latents // pieces
    low = narrow * latents
    half_rows, quarter = tokens // 2, tokens // 4
    near = wide // (W // 2)

    def mate(d):
        goal = 0
        for b in range(W.bit_length() - 1):
            digit = wide // 2**b % 2
            goal = goal + 2**b * (1 - digit if d >> b & 1 else digit)
        return goal

    def rows_of(h):
        return pl.ds(pl.multiple_of(h * half_rows, half_rows), half_rows)

    def piece_cols(n):
        return pl.ds(pl.multiple_of(n * piece, LANES), piece)

    def load(source, target, i):
        return pltpu.make_async_copy(source, target, load_sem.at[i])

    def load_act(h, i):
        return load(act_hbm.at[rows_of(h)], act.at[rows_of(h)], i)

    load_dec = load(dec_hbm, dec, 1)
    load_ids = load(ids_hbm, ids_t_ref, 2)
    load_bias = load(bias_hbm, bias_ref, 3)
    load_shift = load(shift_hbm, shift_ref, 4)

    def load_enc(n):
        return load(enc_hbm.at[:, piece_cols(n)], enc.at[:, piece_cols(n)], 5 + n)

    barrier = pltpu.get_barrier_semaphore()
    for d in range(1, W):
        pl.semaphore_signal(barrier, inc=1, device_id={"wide": mate(d)}, device_id_type=MESH)
    for d in range(1, N):
        pl.semaphore_signal(barrier, inc=1, device_id={"narrow": lax.rem(narrow + d, N)}, device_id_type=MESH)

    load_ids.start()
    load_act(1 - near, 0).start()
    for n in range(AHEAD):
        load_enc(n).start()
    load_act(near, 5 + pieces).start()
    load_bias.start()
    load_shift.start()

    load_ids.wait()
    for n in range(AHEAD, pieces):
        load_enc(n).start()
    stacked = jnp.concatenate([ids_t_ref[...]] * fold, axis=0)
    ids[...] = stacked.T

    GROUP, TALL = 16, 256
    bands = latents // TALL
    groups = bands * (tokens // LANES)

    def fill_slots(i, slot, low):
        band, side = i % bands, i // bands
        at = pl.ds(pl.multiple_of(side * LANES, LANES), LANES)
        offset = low + band * TALL
        place = lax.broadcasted_iota(jnp.int32, (GROUP, LANES), 0)
        places = [(place + j * GROUP).astype(jnp.int16) for j in range(TALL // GROUP)]
        found = [jnp.full((GROUP, LANES), top, jnp.int16) for _ in places]
        for k in range(top):
            here = jnp.broadcast_to(ids_t_ref[k : k + 1, at] - offset, (GROUP, LANES)).astype(jnp.int16)
            found = [jnp.where(here == p, jnp.int16(k), f) for p, f in zip(places, found)]
        slot[at, pl.ds(pl.multiple_of(band * TALL, TALL), TALL)] = jnp.concatenate(found, axis=0).T.astype(jnp.int32)

    def slots_of(i, carry):
        fill_slots(i, slot, low)
        return carry

    pl.semaphore_wait(barrier, W + N - 2)

    def narrow_copy(goal, source, target, send, recv):
        return pltpu.make_async_remote_copy(
            src_ref=source, dst_ref=target, send_sem=send, recv_sem=recv,
            device_id={"narrow": goal}, device_id_type=MESH,
        )

    def wide_copy(d, source, target, send, recv):
        return pltpu.make_async_remote_copy(
            src_ref=source, dst_ref=target, send_sem=send.at[d], recv_sem=recv.at[d],
            device_id={"wide": mate(d)}, device_id_type=MESH,
        )

    def columns(c):
        return pl.ds(pl.multiple_of(c * chunk, chunk), chunk)

    if early:
        (
            dec_in, slot_in, values_in, lat_in, rec, rec_in, msg, msg_in, err_out, full, full_in, base,
            ds, dr, vs, vr, vws, vwr, ns1, nr1, ns2, nr2, ns3, nr3, fs, fr,
        ) = scratch
        side, pair = lax.rem(narrow, 2), narrow // 2
        across, along = narrow + 1 - 2 * side, narrow + 2 - 4 * pair
        plain = chunks - early

        PARTS = 2
        tall = latents // PARTS

        def dec_copy(i):
            c, at = i // PARTS, pl.ds(i % PARTS * tall, tall)
            return narrow_copy(
                across, dec_hbm.at[at, columns(plain + c)], dec_in.at[at, columns(c)], ds.at[i], dr.at[i]
            )

        for i in range(early * PARTS):
            dec_copy(i).start()
    else:
        rec, rec_in, err_out, ns1, nr1, ns2, nr2 = scratch

    lax.fori_loop(0, groups // HEAD, slots_of, 0)
    load_act(1 - near, 0).wait()

    def encode(h, n):
        total[rows_of(h), piece_cols(n)] = jnp.dot(
            act[rows_of(h), :], enc[:, piece_cols(n)], preferred_element_type=F32
        )

    def encode_far(n, carry):
        load_enc(n).wait()
        encode(1 - near, n)
        return carry

    def encode_near(n, carry):
        encode(near, n)
        return carry

    half = lax.broadcasted_iota(jnp.int32, (rows, LANES), 1) // top

    def block_rows(w, p):
        return pl.ds(pl.multiple_of((w * fold + p) * rows, rows), rows)

    def packed_ids(w):
        out = ids[block_rows(w, 0), :]
        for p in range(1, fold):
            out = jnp.where(half == p, ids[block_rows(w, p), :], out)
        return out - low

    def pick_dense(w):
        def tables(p):
            return [total[block_rows(w, p), j * LANES : (j + 1) * LANES] for j in range(latents // LANES)]

        return pick(tables, packed_ids(w), fold, top)

    def scatter_copy(d, source, target, send, recv):
        return wide_copy(d, source.at[d], target.at[d], send, recv)

    def scatter(first, last, source, target, send, recv):
        picked = None
        for d in range(last - 1, first - 1, -1):
            picked = pick_dense(mate(d))
            if d > 0:
                source[d] = picked.astype(BF16)
                scatter_copy(d, source, target, send, recv).start()
        return picked

    def gather(picked, source, target, send, recv):
        for d in range(1, W):
            scatter_copy(d, source, target, send, recv).wait_recv()
            picked = picked + target[d].astype(F32)
        return picked

    lax.fori_loop(0, pieces, encode_far, 0)
    load_dec.start()
    scatter(W // 2, W, part, wide_in, ws1, wr1)
    load_act(near, 5 + pieces).wait()
    lax.fori_loop(0, pieces, encode_near, 0)
    summed = scatter(0, W // 2, part, wide_in, ws1, wr1)

    def bias_tables(p):
        return [jnp.broadcast_to(bias_ref[:, j * LANES : (j + 1) * LANES], (rows, LANES)) for j in range(latents // LANES)]

    load_bias.wait()
    load_shift.wait()
    summed = summed + pick(bias_tables, packed_ids(wide), fold, top)

    lax.fori_loop(groups // HEAD, groups * TURN // 16, slots_of, 0)

    values[wide] = gather(summed, part, wide_in, ws1, wr1).astype(BF16)

    def value_copy(d):
        return wide_copy(d, values.at[wide], values.at[wide], ws2, wr2)

    for d in range(W - 1, 0, -1):
        value_copy(d).start()
    if early:
        def pair_values():
            return narrow_copy(across, values.at[wide], values_in.at[wide], vs.at[0], vr.at[0])

        pair_values().start()

    lax.fori_loop(groups * TURN // 16, groups, slots_of, 0)

    def fill_block(block, values, slot, lat):
        table = values[block].astype(F32)
        for p in range(fold):
            at = block_rows(block, p)
            spread = spread_row(table, p, top, latents // LANES, lambda j: slot[at, j * LANES : (j + 1) * LANES])
            lat[at, :] = spread.astype(BF16)

    def fill_mates(first, last):
        for d in range(first, last):
            if d > 0:
                value_copy(d).wait_recv()
            fill_block(mate(d), values, slot, lat)

    load_dec.wait()

    def own_rows(i):
        return pl.ds(pl.multiple_of(i * own, own), own)

    def keep_slots():
        own_slot_ref[...] = slot[pl.ds(pl.multiple_of(wide * (fold * rows), fold * rows), fold * rows), :]

    def flip(j, carry):
        at = pl.ds(pl.multiple_of(j * LANES, LANES), LANES)
        lat_t[at, :] = lat[:, at].T
        return carry

    def decode(c, at=slice(None)):
        return jnp.dot(lat[at, :], dec[:, columns(c)], preferred_element_type=F32)

    def contract(c, at=slice(None)):
        return lax.dot_general(
            err[at, columns(c)], dec[:, columns(c)], (((1,), (1,)), ((), ())), preferred_element_type=F32
        )

    def outer(c):
        dg_ref[:, columns(c)] = jnp.dot(lat_t[...], err[:, columns(c)], preferred_element_type=F32).astype(BF16)

    def local_chunk(c, carry):
        total[...] += contract(c)
        outer(c)
        return carry

    if early:
        def here(h):
            return pl.ds(pl.multiple_of(h * half_rows + side * quarter, quarter), quarter)

        def scale(count):
            return count.astype(F32)

        own_scale, mate_scale = scale(N - narrow), scale(N - across)
        least = scale(N - jnp.maximum(narrow, across))
        own_use, mate_use = scale(1 + pair * (N - 1 - narrow)), scale(1 + pair * (N - 1 - across))

        def rec_copy(c, q):
            h = near if q == 0 else 1 - near
            return narrow_copy(across, rec.at[c, h, 1 - side], rec_in.at[c, h], ns1.at[c, q], nr1.at[c, q])

        def msg_copy(c):
            return narrow_copy(along, msg.at[c], msg_in.at[c], ns2.at[c], nr2.at[c])

        def err_copy(c, h):
            return narrow_copy(across, err_out.at[c, h], err.at[here(h), columns(c)], ns3.at[c, h], nr3.at[c, h])

        def full_copy(c):
            return narrow_copy(along, full.at[c], full_in.at[c], fs.at[c], fr.at[c])

        def send_part(c, q):
            h = near if q == 0 else 1 - near
            rec[c, h] = decode(c, rows_of(h)).astype(BF16).reshape(2, quarter, chunk)
            rec_copy(c, q).start()

        def send_rec(c, carry):
            rec[c] = decode(c).astype(BF16).reshape(2, 2, quarter, chunk)
            for q in range(2):
                rec_copy(c, q).start()
            return carry

        fill_mates(0, W // 2)
        for c in range(FIRST):
            send_part(c, 0)
        fill_mates(W // 2, W)
        for c in range(FIRST):
            send_part(c, 1)
        lax.fori_loop(FIRST, plain, send_rec, 0)

        def more_slots(i, carry):
            fill_slots(i, slot_in, across * latents)
            return carry

        def send_msg(c):
            for q in range(2):
                rec_copy(c, q).wait_recv()
            msg[c] = (own_use * rec[c, :, side].astype(F32) + mate_use * rec_in[c].astype(F32)).astype(BF16)
            msg_copy(c).start()

        def send_err(c):
            msg_copy(c).wait_recv()
            for h in range(2):
                shift = shift_ref[:, columns(c)] - act[here(h), columns(c)].astype(F32)
                mine_rec, mate_rec = rec[c, h, side].astype(F32), rec_in[c, h].astype(F32)
                other = msg_in[c, h].astype(F32)
                back = mate_scale * (shift + mate_rec) + least * mine_rec + mate_use * other
                err_out[c, h] = (back / N).astype(BF16)
                err_copy(c, h).start()
                back = own_scale * (shift + mine_rec) + least * mate_rec + own_use * other
                err[here(h), columns(c)] = (back / N).astype(BF16)

        def send_full(c, carry):
            mine_rec = decode(plain + c)
            mate_rec = jnp.dot(lat_in[...], dec_in[:, columns(c)], preferred_element_type=F32)
            full[c] = (own_use * mine_rec + mate_use * mate_rec).astype(BF16)
            full_copy(c).start()
            shift = shift_ref[:, columns(plain + c)] - act[:, columns(plain + c)].astype(F32)
            base[c] = own_scale * (shift + mine_rec) + least * mate_rec
            return carry

        def take_full(c, carry):
            full_copy(c).wait_recv()
            err[:, columns(plain + c)] = ((base[c] + own_use * full_in[c].astype(F32)) / N).astype(BF16)
            return carry

        def values_copies():
            return [wide_copy(d, values_in.at[wide], values_in.at[wide], vws, vwr) for d in range(1, W)]

        def arrive(c):
            for h in range(2):
                err_copy(c, h).wait_recv()

        def take(c):
            arrive(c)
            local_chunk(c, 0)

        pair_values().wait_recv()
        for copy in values_copies():
            copy.start()
        keep_slots()
        lax.fori_loop(0, latents // LANES, flip, 0)
        total[...] = jnp.zeros_like(total)
        lax.fori_loop(0, groups // 2, more_slots, 0)
        for c in range(plain):
            send_msg(c)
            if c >= LAG:
                send_err(c - LAG)
            if c < 2:
                lax.fori_loop((2 + c) * groups // 4, (3 + c) * groups // 4, more_slots, 0)
            if c == 2:
                for copy in values_copies():
                    copy.wait_recv()
                for block in range(W):
                    fill_block(block, values_in, slot_in, lat_in)
        for i in range(early * PARTS):
            dec_copy(i).wait_recv()
        lax.fori_loop(0, early, send_full, 0)
        for c in range(LAG):
            send_err(plain - LAG + c)
            take(c)


        def finish(c, carry):
            for q in range(2):
                rec_copy(c, q).wait_send()
                err_copy(c, q).wait_send()
            msg_copy(c).wait_send()
            return carry

        def finish_early():
            for i in range(early * PARTS):
                dec_copy(i).wait_send()
            for c in range(early):
                full_copy(c).wait_send()
            pair_values().wait_send()
            for copy in values_copies():
                copy.wait_send()
    else:
        plain = chunks
        fill_mates(0, W)
        keep_slots()

        def goal_of(d):
            return lax.rem(narrow + d, N)

        def rec_copy(c, d):
            return narrow_copy(goal_of(d), rec.at[c, goal_of(d)], rec_in.at[c, d], ns1.at[c, d], nr1.at[c, d])

        def err_copy(c, d):
            return narrow_copy(
                goal_of(d), err_out.at[c, d], err.at[own_rows(narrow), columns(c)], ns2.at[c, d], nr2.at[c, d]
            )

        def send_rec(c, carry):
            rec[c] = decode(c).astype(BF16).reshape(N, own, chunk)
            for d in range(1, N):
                rec_copy(c, d).start()
            return carry

        lax.fori_loop(0, chunks, send_rec, 0)

        def combine(c, carry):
            for d in range(1, N):
                rec_copy(c, d).wait_recv()
            shift = shift_ref[:, columns(c)] - act[own_rows(narrow), columns(c)].astype(F32)
            terms = [rec[c, narrow].astype(F32)]
            terms += [rec_in[c, d].astype(F32) for d in range(1, N)]
            for e in range(N):
                goal = goal_of(e)
                back = (N - goal).astype(F32) * shift
                for d in range(N):
                    origin = lax.rem(narrow + N - d, N)
                    back = back + (N - jnp.maximum(goal, origin)).astype(F32) * terms[d]
                back = (back / N).astype(BF16)
                if e == 0:
                    err[own_rows(narrow), columns(c)] = back
                else:
                    err_out[c, e] = back
                    err_copy(c, e).start()
            return carry

        lax.fori_loop(0, chunks, combine, 0)
        lax.fori_loop(0, latents // LANES, flip, 0)

        def arrive(c):
            for d in range(1, N):
                err_copy(c, d).wait_recv()

        def finish(c, carry):
            for d in range(1, N):
                rec_copy(c, d).wait_send()
                err_copy(c, d).wait_send()
            return carry

        def finish_early():
            pass

    def sent_chunk(c, carry):
        arrive(c)
        return local_chunk(c, carry)

    if early:
        lax.fori_loop(LAG, plain - 1, sent_chunk, 0)
        lax.fori_loop(0, early, take_full, 0)
        lax.fori_loop(plain, chunks, local_chunk, 0)
    else:
        total[...] = jnp.zeros_like(total)
        lax.fori_loop(0, plain - 1, sent_chunk, 0)
    arrive(plain - 1)
    total[rows_of(1 - near), :] += contract(plain - 1, rows_of(1 - near))
    scatter(W // 2, W, lg_packed, grad_in, ws3, wr3)
    total[rows_of(near), :] += contract(plain - 1, rows_of(near))
    summed = scatter(0, W // 2, lg_packed, grad_in, ws3, wr3)
    outer(plain - 1)
    sum_ref[...] = gather(summed, lg_packed, grad_in, ws3, wr3)

    for d in range(1, W):
        scatter_copy(d, part, wide_in, ws1, wr1).wait_send()
        value_copy(d).wait_send()
        scatter_copy(d, lg_packed, grad_in, ws3, wr3).wait_send()

    lax.fori_loop(0, plain, finish, 0)
    finish_early()


STORES = 1
AHEAD, HEAD, TURN = 1, 8, 9
FIRST, LAG = 3, 3


def store_kernel(fold, top, dg_ref, sum_ref, slot_ref, dg_hbm, grad_hbm, grad_ref, sem):
    step = dg_ref.shape[0] // STORES
    rows = sum_ref.shape[0]
    copies = []
    for i in range(STORES):
        at = pl.ds(i * step, step)
        copies.append(pltpu.make_async_copy(dg_ref.at[at], dg_hbm.at[at], sem.at[i]))
    for copy in copies:
        copy.start()
    for p in range(fold):
        at = slice(p * rows, (p + 1) * rows)
        grad_ref[at, :] = spread_row(sum_ref[...], p, top, slot_ref.shape[1] // LANES, lambda j: slot_ref[at, j * LANES : (j + 1) * LANES])
    copies.append(pltpu.make_async_copy(grad_ref, grad_hbm, sem.at[STORES]))
    copies[-1].start()
    for copy in copies:
        copy.wait()


def local(activations, enc_weight, enc_bias, dec_weight, dec_bias, active_ids):
    W, N = lax.axis_size("wide"), lax.axis_size("narrow")
    tokens, channels = activations.shape
    latents = enc_weight.shape[1]
    top = active_ids.shape[1]
    fold = LANES // top
    rows = tokens // W // fold
    chunk = min(channels, 256)
    chunks = channels // chunk
    pieces = 1
    own = tokens // N
    early = chunks // 8 if N == 4 else 0
    plain = chunks - early
    half = (plain, 2, tokens // 4, chunk)
    packed_shape = (W, rows, LANES)
    vmem = pl.BlockSpec(memory_space=pltpu.VMEM)
    hbm = pl.BlockSpec(memory_space=pl.ANY)
    dma = pltpu.SemaphoreType.DMA
    if early:
        scratch = [
            pltpu.VMEM((latents, early * chunk), BF16),
            pltpu.VMEM((tokens, latents), jnp.int32),
            pltpu.VMEM(packed_shape, BF16),
            pltpu.VMEM((tokens, latents), BF16),
            pltpu.VMEM((plain, 2, 2, tokens // 4, chunk), BF16),
            *[pltpu.VMEM(half, BF16)] * 4,
            *[pltpu.VMEM((early, tokens, chunk), BF16)] * 2,
            pltpu.VMEM((early, tokens, chunk), F32),
            dma((2 * early,)), dma((2 * early,)), dma((1,)), dma((1,)), dma((W,)), dma((W,)),
            *[dma((plain, 2))] * 2, *[dma((plain,))] * 2, *[dma((plain, 2))] * 2,
            dma((early,)), dma((early,)),
        ]
    else:
        scratch = [*[pltpu.VMEM((chunks, N, own, chunk), BF16)] * 3, *[dma((chunks, N))] * 4]
    dec_grad, summed, slots = pl.pallas_call(
        functools.partial(step_kernel, W, N, fold, top, chunk, pieces, early),
        out_shape=(
            pltpu.VMEM((latents, channels), BF16),
            pltpu.VMEM((rows, LANES), F32),
            pltpu.VMEM((tokens // W, latents), jnp.int32),
        ),
        in_specs=[hbm] * 6,
        out_specs=(vmem, vmem, vmem),
        scratch_shapes=[
            pltpu.VMEM((top, tokens), jnp.int32),
            pltpu.VMEM((1, latents), F32),
            pltpu.VMEM((1, channels), F32),
            pltpu.VMEM((tokens, LANES), jnp.int32),
            pltpu.VMEM((tokens, channels), BF16),
            pltpu.VMEM((channels, latents), BF16),
            pltpu.VMEM((latents, channels), BF16),
            pltpu.VMEM((tokens, latents), jnp.int32),
            pltpu.VMEM((tokens, latents), F32),
            pltpu.VMEM(packed_shape, BF16),
            pltpu.VMEM(packed_shape, BF16),
            pltpu.VMEM(packed_shape, BF16),
            pltpu.VMEM((tokens, latents), BF16),
            pltpu.VMEM((latents, tokens), BF16),
            pltpu.VMEM((tokens, channels), BF16),
            pltpu.VMEM(packed_shape, BF16),
            pltpu.VMEM(packed_shape, BF16),
            dma((6 + pieces,)),
            *[dma((W,))] * 6,
            *scratch,
        ],
        compiler_params=pltpu.CompilerParams(collective_id=0, has_side_effects=True, vmem_limit_bytes=56 * 2**20),
        cost_estimate=pl.CostEstimate(
            flops=8 * tokens * channels * latents, bytes_accessed=6 * channels * (tokens + latents), transcendentals=0
        ),
        name="step",
    )(active_ids.T, enc_bias.reshape(1, -1), dec_bias.reshape(1, -1), activations, enc_weight, dec_weight)
    resident = [pltpu.with_memory_space_constraint(x, pltpu.VMEM) for x in (dec_grad, summed, slots)]
    return pl.pallas_call(
        functools.partial(store_kernel, fold, top),
        out_shape=(
            jax.ShapeDtypeStruct((latents, channels), BF16),
            jax.ShapeDtypeStruct((tokens // W, latents), F32),
        ),
        in_specs=[vmem, vmem, vmem],
        out_specs=(hbm, hbm),
        scratch_shapes=[pltpu.VMEM((tokens // W, latents), F32), dma((STORES + 1,))],
        compiler_params=pltpu.CompilerParams(vmem_limit_bytes=2**20),
        name="store",
    )(*resident)


def solution(mesh):
    in_specs = (
        P(None, "wide"),
        P("wide", "narrow"),
        P("narrow"),
        P("narrow", "wide"),
        P("wide"),
        P(),
    )
    out_specs = (P("narrow", "wide"), P("wide", "narrow"))
    return jax.shard_map(local, mesh=mesh, in_specs=in_specs, out_specs=out_specs, check_vma=False)
```

```python
import functools

import jax
import jax.numpy as jnp
from jax import lax
from jax.experimental import pallas as pl
from jax.experimental.pallas import tpu as pltpu
from jax.sharding import PartitionSpec as P

LANES = 128
MESH = pl.DeviceIdType.MESH
F32, BF16 = jnp.float32, jnp.bfloat16


def lookup(table, index):
    return jnp.take_along_axis(table, index, axis=1, mode="promise_in_bounds")


def pick(tables, ids, fold, top):
    tile, lane = ids >> 7, ids & (LANES - 1)
    half = lax.broadcasted_iota(jnp.int32, ids.shape, 1) // top
    picked = jnp.zeros(ids.shape, F32)
    for part in range(fold):
        here = jnp.where(half == part, tile, -1)
        for j, table in enumerate(tables(part)):
            picked = jnp.where(here == j, lookup(table, lane), picked)
    return picked


def spread_row(table, p, top, tiles, slots):
    rows = table.shape[0]
    table = jnp.concatenate([table[:, p * top : (p + 1) * top], jnp.zeros((rows, LANES - top), F32)], axis=1)
    return jnp.concatenate([lookup(table, slots(j)) for j in range(tiles)], axis=1)


def step_kernel(
    W, N, fold, top, chunk, pieces, early,
    ids_hbm, bias_hbm, shift_hbm, act_hbm, enc_hbm, dec_hbm,
    dg_ref, sum_ref, own_slot_ref,
    ids_t_ref, bias_ref, shift_ref, ids, act, enc, dec, slot, total, part, wide_in, values, lat, lat_t,
    err, lg_packed, grad_in,
    load_sem, ws1, wr1, ws2, wr2, ws3, wr3, *scratch,
):
    wide, narrow = lax.axis_index("wide"), lax.axis_index("narrow")
    tokens, latents = lat.shape
    channels = act.shape[1]
    own, rows = tokens // N, part.shape[1]
    chunks = channels // chunk
    piece = latents // pieces
    low = narrow * latents
    half_rows, quarter = tokens // 2, tokens // 4
    near = wide // (W // 2)

    def mate(d):
        goal = 0
        for b in range(W.bit_length() - 1):
            digit = wide // 2**b % 2
            goal = goal + 2**b * (1 - digit if d >> b & 1 else digit)
        return goal

    def rows_of(h):
        return pl.ds(pl.multiple_of(h * half_rows, half_rows), half_rows)

    def piece_cols(n):
        return pl.ds(pl.multiple_of(n * piece, LANES), piece)

    def load(source, target, i):
        return pltpu.make_async_copy(source, target, load_sem.at[i])

    def load_act(h, i):
        return load(act_hbm.at[rows_of(h)], act.at[rows_of(h)], i)

    load_dec = load(dec_hbm, dec, 1)
    load_ids = load(ids_hbm, ids_t_ref, 2)
    load_bias = load(bias_hbm, bias_ref, 3)
    load_shift = load(shift_hbm, shift_ref, 4)

    def load_enc(n):
        return load(enc_hbm.at[:, piece_cols(n)], enc.at[:, piece_cols(n)], 5 + n)

    barrier = pltpu.get_barrier_semaphore()
    for d in range(1, W):
        pl.semaphore_signal(barrier, inc=1, device_id={"wide": mate(d)}, device_id_type=MESH)
    for d in range(1, N):
        pl.semaphore_signal(barrier, inc=1, device_id={"narrow": lax.rem(narrow + d, N)}, device_id_type=MESH)

    load_ids.start()
    load_act(1 - near, 0).start()
    for n in range(AHEAD):
        load_enc(n).start()
    load_act(near, 5 + pieces).start()
    load_bias.start()
    load_shift.start()

    load_ids.wait()
    for n in range(AHEAD, pieces):
        load_enc(n).start()
    stacked = jnp.concatenate([ids_t_ref[...]] * fold, axis=0)
    ids[...] = stacked.T

    GROUP, TALL = 16, 256
    bands = latents // TALL
    groups = bands * (tokens // LANES)

    def fill_slots(i, slot, low):
        band, side = i % bands, i // bands
        at = pl.ds(pl.multiple_of(side * LANES, LANES), LANES)
        offset = low + band * TALL
        place = lax.broadcasted_iota(jnp.int32, (GROUP, LANES), 0)
        places = [(place + j * GROUP).astype(jnp.int16) for j in range(TALL // GROUP)]
        found = [jnp.full((GROUP, LANES), top, jnp.int16) for _ in places]
        for k in range(top):
            here = jnp.broadcast_to(ids_t_ref[k : k + 1, at] - offset, (GROUP, LANES)).astype(jnp.int16)
            found = [jnp.where(here == p, jnp.int16(k), f) for p, f in zip(places, found)]
        slot[at, pl.ds(pl.multiple_of(band * TALL, TALL), TALL)] = jnp.concatenate(found, axis=0).T.astype(jnp.int32)

    def slots_of(i, carry):
        fill_slots(i, slot, low)
        return carry

    pl.semaphore_wait(barrier, W + N - 2)

    def narrow_copy(goal, source, target, send, recv):
        return pltpu.make_async_remote_copy(
            src_ref=source, dst_ref=target, send_sem=send, recv_sem=recv,
            device_id={"narrow": goal}, device_id_type=MESH,
        )

    def wide_copy(d, source, target, send, recv):
        return pltpu.make_async_remote_copy(
            src_ref=source, dst_ref=target, send_sem=send, recv_sem=recv,
            device_id={"wide": mate(d)}, device_id_type=MESH,
        )

    def columns(c):
        return pl.ds(pl.multiple_of(c * chunk, chunk), chunk)

    if early:
        (
            dec_in, slot_in, values_in, lat_in, rec, rec_in, msg, msg_in, err_out, full, full_in, base,
            ds, dr, vs, vr, vws, vwr, ns1, nr1, ns2, nr2, ns3, nr3, fs, fr,
        ) = scratch
        side, pair = lax.rem(narrow, 2), narrow // 2
        across, along = narrow + 1 - 2 * side, narrow + 2 - 4 * pair
        plain = chunks - early

        PARTS = 1
        tall = latents // PARTS

        def dec_copy(i):
            c, at = i // PARTS, pl.ds(i % PARTS * tall, tall)
            return narrow_copy(
                across, dec_hbm.at[at, columns(plain + c)], dec_in.at[at, columns(c)], ds.at[i], dr.at[i]
            )

        for i in range(early * PARTS):
            dec_copy(i).start()
    else:
        rec, rec_in, err_out, ns1, nr1, ns2, nr2 = scratch

    lax.fori_loop(0, groups // HEAD, slots_of, 0)
    load_act(1 - near, 0).wait()

    def encode(h, n):
        total[rows_of(h), piece_cols(n)] = jnp.dot(
            act[rows_of(h), :], enc[:, piece_cols(n)], preferred_element_type=F32
        )

    def encode_far(n, carry):
        load_enc(n).wait()
        encode(1 - near, n)
        return carry

    def encode_near(n, carry):
        encode(near, n)
        return carry

    half = lax.broadcasted_iota(jnp.int32, (rows, LANES), 1) // top

    def block_rows(w, p):
        return pl.ds(pl.multiple_of((w * fold + p) * rows, rows), rows)

    def packed_ids(w):
        out = ids[block_rows(w, 0), :]
        for p in range(1, fold):
            out = jnp.where(half == p, ids[block_rows(w, p), :], out)
        return out - low

    def pick_dense(w):
        def tables(p):
            return [total[block_rows(w, p), j * LANES : (j + 1) * LANES] for j in range(latents // LANES)]

        return pick(tables, packed_ids(w), fold, top)

    def scatter_copy(d, source, target, send, recv):
        return wide_copy(d, source.at[d - 1], target.at[d - 1], send.at[0], recv.at[0])

    def scatter_all(source, target, send, recv):
        return wide_copy(1, source, target, send.at[0], recv.at[0])

    def scatter(first, last, source, target, send, recv):
        picked = None
        for d in range(last - 1, first - 1, -1):
            picked = pick_dense(mate(d))
            if d > 0:
                source[d - 1] = picked.astype(BF16)
                scatter_copy(d, source, target, send, recv).start()
        return picked

    def gather(picked, source, target, send, recv):
        scatter_all(source, target, send, recv).wait_recv()
        for d in range(1, W):
            picked = picked + target[d - 1].astype(F32)
        return picked

    lax.fori_loop(0, pieces, encode_far, 0)
    load_dec.start()
    scatter(W // 2, W, part, wide_in, ws1, wr1)
    load_act(near, 5 + pieces).wait()
    lax.fori_loop(0, pieces, encode_near, 0)
    summed = scatter(0, W // 2, part, wide_in, ws1, wr1)

    def bias_tables(p):
        return [jnp.broadcast_to(bias_ref[:, j * LANES : (j + 1) * LANES], (rows, LANES)) for j in range(latents // LANES)]

    load_bias.wait()
    load_shift.wait()
    summed = summed + pick(bias_tables, packed_ids(wide), fold, top)

    lax.fori_loop(groups // HEAD, groups * TURN // 16, slots_of, 0)

    values[wide] = gather(summed, part, wide_in, ws1, wr1).astype(BF16)

    def value_copy(d):
        return wide_copy(d, values.at[wide], values.at[wide], ws2.at[0], wr2.at[d // (W // 2)])

    def values_of(ref, first, last, send, recv):
        blocks = ref.at[pl.ds(0, last - first)]
        return wide_copy(1, blocks, blocks, send, recv)

    for d in range(W - 1, 0, -1):
        value_copy(d).start()
    if early:
        def pair_values():
            return narrow_copy(across, values.at[wide], values_in.at[wide], vs.at[0], vr.at[0])

        pair_values().start()

    lax.fori_loop(groups * TURN // 16, groups, slots_of, 0)

    def fill_block(block, values, slot, lat):
        table = values[block].astype(F32)
        for p in range(fold):
            at = block_rows(block, p)
            spread = spread_row(table, p, top, latents // LANES, lambda j: slot[at, j * LANES : (j + 1) * LANES])
            lat[at, :] = spread.astype(BF16)

    def fill_mates(first, last, group):
        values_of(values, first, last, ws2.at[0], wr2.at[group]).wait_recv()
        for d in range(first, last):
            fill_block(mate(d), values, slot, lat)

    load_dec.wait()

    def own_rows(i):
        return pl.ds(pl.multiple_of(i * own, own), own)

    def keep_slots():
        own_slot_ref[...] = slot[pl.ds(pl.multiple_of(wide * (fold * rows), fold * rows), fold * rows), :]

    def flip(j, carry):
        at = pl.ds(pl.multiple_of(j * LANES, LANES), LANES)
        lat_t[at, :] = lat[:, at].T
        return carry

    def decode(c, at=slice(None)):
        return jnp.dot(lat[at, :], dec[:, columns(c)], preferred_element_type=F32)

    def contract(c, at=slice(None)):
        return lax.dot_general(
            err[at, columns(c)], dec[:, columns(c)], (((1,), (1,)), ((), ())), preferred_element_type=F32
        )

    def outer(c):
        dg_ref[:, columns(c)] = jnp.dot(lat_t[...], err[:, columns(c)], preferred_element_type=F32).astype(BF16)

    def local_chunk(c, carry):
        total[...] += contract(c)
        outer(c)
        return carry

    if early:
        def here(h):
            return pl.ds(pl.multiple_of(h * half_rows + side * quarter, quarter), quarter)

        def scale(count):
            return count.astype(F32)

        own_scale, mate_scale = scale(N - narrow), scale(N - across)
        least = scale(N - jnp.maximum(narrow, across))
        own_use, mate_use = scale(1 + pair * (N - 1 - narrow)), scale(1 + pair * (N - 1 - across))

        def rec_copy(c, q):
            h = near if q == 0 else 1 - near
            return narrow_copy(across, rec.at[c, h, 1 - side], rec_in.at[c, h], ns1.at[0], nr1.at[c])

        def msg_copy(c):
            return narrow_copy(along, msg.at[c], msg_in.at[c], ns2.at[0], nr2.at[c])

        def err_copy(c, h):
            return narrow_copy(across, err_out.at[c, h], err.at[here(h), columns(c)], ns3.at[0], nr3.at[c])

        def full_copy(c):
            return narrow_copy(along, full.at[c], full_in.at[c], fs.at[c], fr.at[c])

        def send_part(c, q):
            h = near if q == 0 else 1 - near
            rec[c, h] = decode(c, rows_of(h)).astype(BF16).reshape(2, quarter, chunk)
            rec_copy(c, q).start()

        def send_rec(c, carry):
            rec[c] = decode(c).astype(BF16).reshape(2, 2, quarter, chunk)
            for q in range(2):
                rec_copy(c, q).start()
            return carry

        fill_block(wide, values, slot, lat)
        fill_mates(1, W // 2, 0)
        for c in range(FIRST):
            send_part(c, 0)
        fill_mates(W // 2, W, 1)
        for c in range(FIRST):
            send_part(c, 1)
        lax.fori_loop(FIRST, plain, send_rec, 0)

        def more_slots(i, carry):
            fill_slots(i, slot_in, across * latents)
            return carry

        def send_msg(c):
            narrow_copy(across, rec_in.at[c], rec_in.at[c], ns1.at[0], nr1.at[c]).wait_recv()
            msg[c] = (own_use * rec[c, :, side].astype(F32) + mate_use * rec_in[c].astype(F32)).astype(BF16)
            msg_copy(c).start()

        def send_err(c):
            msg_copy(c).wait_recv()
            for h in range(2):
                shift = shift_ref[:, columns(c)] - act[here(h), columns(c)].astype(F32)
                mine_rec, mate_rec = rec[c, h, side].astype(F32), rec_in[c, h].astype(F32)
                other = msg_in[c, h].astype(F32)
                back = mate_scale * (shift + mate_rec) + least * mine_rec + mate_use * other
                err_out[c, h] = (back / N).astype(BF16)
                err_copy(c, h).start()
                back = own_scale * (shift + mine_rec) + least * mate_rec + own_use * other
                err[here(h), columns(c)] = (back / N).astype(BF16)

        def send_full(c, carry):
            mine_rec = decode(plain + c)
            mate_rec = jnp.dot(lat_in[...], dec_in[:, columns(c)], preferred_element_type=F32)
            full[c] = (own_use * mine_rec + mate_use * mate_rec).astype(BF16)
            full_copy(c).start()
            shift = shift_ref[:, columns(plain + c)] - act[:, columns(plain + c)].astype(F32)
            base[c] = own_scale * (shift + mine_rec) + least * mate_rec
            return carry

        def take_full(c, carry):
            full_copy(c).wait_recv()
            err[:, columns(plain + c)] = ((base[c] + own_use * full_in[c].astype(F32)) / N).astype(BF16)
            return carry

        def values_copies():
            return [wide_copy(d, values_in.at[wide], values_in.at[wide], vws.at[0], vwr.at[0]) for d in range(1, W)]

        def values_all():
            return values_of(values_in, 1, W, vws.at[0], vwr.at[0])

        def arrive(c):
            narrow_copy(across, err_out.at[c], err_out.at[c], ns3.at[0], nr3.at[c]).wait_recv()

        def take(c):
            arrive(c)
            local_chunk(c, 0)

        pair_values().wait_recv()
        for copy in values_copies():
            copy.start()
        keep_slots()
        lax.fori_loop(0, latents // LANES, flip, 0)
        total[...] = jnp.zeros_like(total)
        lax.fori_loop(0, groups // 2, more_slots, 0)
        for c in range(plain):
            send_msg(c)
            if c >= LAG:
                send_err(c - LAG)
            if c < 2:
                lax.fori_loop((2 + c) * groups // 4, (3 + c) * groups // 4, more_slots, 0)
            if c == 2:
                values_all().wait_recv()
                for block in range(W):
                    fill_block(block, values_in, slot_in, lat_in)
        for i in range(early * PARTS):
            dec_copy(i).wait_recv()
        lax.fori_loop(0, early, send_full, 0)
        for c in range(LAG):
            send_err(plain - LAG + c)
            take(c)


        def finish():
            narrow_copy(across, rec_in, rec_in, ns1.at[0], nr1.at[0]).wait_send()
            narrow_copy(along, msg, msg, ns2.at[0], nr2.at[0]).wait_send()
            narrow_copy(across, err_out, err_out, ns3.at[0], nr3.at[0]).wait_send()
            for i in range(early * PARTS):
                dec_copy(i).wait_send()
            for c in range(early):
                full_copy(c).wait_send()
            pair_values().wait_send()
            values_all().wait_send()
    else:
        plain = chunks
        fill_block(wide, values, slot, lat)
        fill_mates(1, W // 2, 0)
        fill_mates(W // 2, W, 1)
        keep_slots()

        def goal_of(d):
            return lax.rem(narrow + d, N)

        def rec_copy(c, d):
            return narrow_copy(goal_of(d), rec.at[c, goal_of(d)], rec_in.at[c, d], ns1.at[c, d], nr1.at[c, d])

        def err_copy(c, d):
            return narrow_copy(
                goal_of(d), err_out.at[c, d], err.at[own_rows(narrow), columns(c)], ns2.at[c, d], nr2.at[c, d]
            )

        def send_rec(c, carry):
            rec[c] = decode(c).astype(BF16).reshape(N, own, chunk)
            for d in range(1, N):
                rec_copy(c, d).start()
            return carry

        lax.fori_loop(0, chunks, send_rec, 0)

        def combine(c, carry):
            for d in range(1, N):
                rec_copy(c, d).wait_recv()
            shift = shift_ref[:, columns(c)] - act[own_rows(narrow), columns(c)].astype(F32)
            terms = [rec[c, narrow].astype(F32)]
            terms += [rec_in[c, d].astype(F32) for d in range(1, N)]
            for e in range(N):
                goal = goal_of(e)
                back = (N - goal).astype(F32) * shift
                for d in range(N):
                    origin = lax.rem(narrow + N - d, N)
                    back = back + (N - jnp.maximum(goal, origin)).astype(F32) * terms[d]
                back = (back / N).astype(BF16)
                if e == 0:
                    err[own_rows(narrow), columns(c)] = back
                else:
                    err_out[c, e] = back
                    err_copy(c, e).start()
            return carry

        lax.fori_loop(0, chunks, combine, 0)
        lax.fori_loop(0, latents // LANES, flip, 0)

        def arrive(c):
            for d in range(1, N):
                err_copy(c, d).wait_recv()

        def finish_chunk(c, carry):
            for d in range(1, N):
                rec_copy(c, d).wait_send()
                err_copy(c, d).wait_send()
            return carry

        def finish():
            lax.fori_loop(0, plain, finish_chunk, 0)

    def sent_chunk(c, carry):
        arrive(c)
        return local_chunk(c, carry)

    if early:
        lax.fori_loop(LAG, plain - 1, sent_chunk, 0)
        lax.fori_loop(0, early, take_full, 0)
        lax.fori_loop(plain, chunks, local_chunk, 0)
    else:
        total[...] = jnp.zeros_like(total)
        lax.fori_loop(0, plain - 1, sent_chunk, 0)
    arrive(plain - 1)
    total[rows_of(1 - near), :] += contract(plain - 1, rows_of(1 - near))
    scatter(W // 2, W, lg_packed, grad_in, ws3, wr3)
    total[rows_of(near), :] += contract(plain - 1, rows_of(near))
    summed = scatter(0, W // 2, lg_packed, grad_in, ws3, wr3)
    outer(plain - 1)
    sum_ref[...] = gather(summed, lg_packed, grad_in, ws3, wr3)

    scatter_all(part, wide_in, ws1, wr1).wait_send()
    values_of(values, 1, W, ws2.at[0], wr2.at[0]).wait_send()
    scatter_all(lg_packed, grad_in, ws3, wr3).wait_send()

    finish()


STORES = 1
AHEAD, HEAD, TURN = 1, 8, 9
FIRST, LAG = 3, 3


def store_kernel(fold, top, dg_ref, sum_ref, slot_ref, dg_hbm, grad_hbm, grad_ref, sem):
    step = dg_ref.shape[0] // STORES
    rows = sum_ref.shape[0]
    copies = []
    for i in range(STORES):
        at = pl.ds(i * step, step)
        copies.append(pltpu.make_async_copy(dg_ref.at[at], dg_hbm.at[at], sem.at[i]))
    for copy in copies:
        copy.start()
    for p in range(fold):
        at = slice(p * rows, (p + 1) * rows)
        grad_ref[at, :] = spread_row(sum_ref[...], p, top, slot_ref.shape[1] // LANES, lambda j: slot_ref[at, j * LANES : (j + 1) * LANES])
    copies.append(pltpu.make_async_copy(grad_ref, grad_hbm, sem.at[STORES]))
    copies[-1].start()
    for copy in copies:
        copy.wait()


def local(activations, enc_weight, enc_bias, dec_weight, dec_bias, active_ids):
    W, N = lax.axis_size("wide"), lax.axis_size("narrow")
    tokens, channels = activations.shape
    latents = enc_weight.shape[1]
    top = active_ids.shape[1]
    fold = LANES // top
    rows = tokens // W // fold
    chunk = min(channels, 256)
    chunks = channels // chunk
    pieces = 1
    own = tokens // N
    early = chunks // 8 if N == 4 else 0
    plain = chunks - early
    half = (plain, 2, tokens // 4, chunk)
    packed_shape, mates_shape = (W, rows, LANES), (W - 1, rows, LANES)
    vmem = pl.BlockSpec(memory_space=pltpu.VMEM)
    hbm = pl.BlockSpec(memory_space=pl.ANY)
    dma = pltpu.SemaphoreType.DMA
    if early:
        scratch = [
            pltpu.VMEM((latents, early * chunk), BF16),
            pltpu.VMEM((tokens, latents), jnp.int32),
            pltpu.VMEM(packed_shape, BF16),
            pltpu.VMEM((tokens, latents), BF16),
            pltpu.VMEM((plain, 2, 2, tokens // 4, chunk), BF16),
            *[pltpu.VMEM(half, BF16)] * 4,
            *[pltpu.VMEM((early, tokens, chunk), BF16)] * 2,
            pltpu.VMEM((early, tokens, chunk), F32),
            dma((early,)), dma((early,)), *[dma((1,))] * 4,
            *[dma((1,)), dma((plain,))] * 3,
            dma((early,)), dma((early,)),
        ]
    else:
        scratch = [*[pltpu.VMEM((chunks, N, own, chunk), BF16)] * 3, *[dma((chunks, N))] * 4]
    dec_grad, summed, slots = pl.pallas_call(
        functools.partial(step_kernel, W, N, fold, top, chunk, pieces, early),
        out_shape=(
            pltpu.VMEM((latents, channels), BF16),
            pltpu.VMEM((rows, LANES), F32),
            pltpu.VMEM((tokens // W, latents), jnp.int32),
        ),
        in_specs=[hbm] * 6,
        out_specs=(vmem, vmem, vmem),
        scratch_shapes=[
            pltpu.VMEM((top, tokens), jnp.int32),
            pltpu.VMEM((1, latents), F32),
            pltpu.VMEM((1, channels), F32),
            pltpu.VMEM((tokens, LANES), jnp.int32),
            pltpu.VMEM((tokens, channels), BF16),
            pltpu.VMEM((channels, latents), BF16),
            pltpu.VMEM((latents, channels), BF16),
            pltpu.VMEM((tokens, latents), jnp.int32),
            pltpu.VMEM((tokens, latents), F32),
            pltpu.VMEM(mates_shape, BF16),
            pltpu.VMEM(mates_shape, BF16),
            pltpu.VMEM(packed_shape, BF16),
            pltpu.VMEM((tokens, latents), BF16),
            pltpu.VMEM((latents, tokens), BF16),
            pltpu.VMEM((tokens, channels), BF16),
            pltpu.VMEM(mates_shape, BF16),
            pltpu.VMEM(mates_shape, BF16),
            dma((6 + pieces,)),
            dma((1,)), dma((1,)), dma((1,)), dma((2,)), dma((1,)), dma((1,)),
            *scratch,
        ],
        compiler_params=pltpu.CompilerParams(collective_id=0, has_side_effects=True, vmem_limit_bytes=56 * 2**20),
        cost_estimate=pl.CostEstimate(
            flops=8 * tokens * channels * latents, bytes_accessed=6 * channels * (tokens + latents), transcendentals=0
        ),
        name="step",
    )(active_ids.T, enc_bias.reshape(1, -1), dec_bias.reshape(1, -1), activations, enc_weight, dec_weight)
    resident = [pltpu.with_memory_space_constraint(x, pltpu.VMEM) for x in (dec_grad, summed, slots)]
    return pl.pallas_call(
        functools.partial(store_kernel, fold, top),
        out_shape=(
            jax.ShapeDtypeStruct((latents, channels), BF16),
            jax.ShapeDtypeStruct((tokens // W, latents), F32),
        ),
        in_specs=[vmem, vmem, vmem],
        out_specs=(hbm, hbm),
        scratch_shapes=[pltpu.VMEM((tokens // W, latents), F32), dma((STORES + 1,))],
        compiler_params=pltpu.CompilerParams(vmem_limit_bytes=2**20),
        name="store",
    )(*resident)


def solution(mesh):
    in_specs = (
        P(None, "wide"),
        P("wide", "narrow"),
        P("narrow"),
        P("narrow", "wide"),
        P("wide"),
        P(),
    )
    out_specs = (P("narrow", "wide"), P("wide", "narrow"))
    return jax.shard_map(local, mesh=mesh, in_specs=in_specs, out_specs=out_specs, check_vma=False)
```

```python
import functools

import jax
import jax.numpy as jnp
from jax import lax
from jax.experimental import pallas as pl
from jax.experimental.pallas import tpu as pltpu
from jax.sharding import PartitionSpec as P

LANES = 128
MESH = pl.DeviceIdType.MESH
F32, BF16 = jnp.float32, jnp.bfloat16


def lookup(table, index):
    return jnp.take_along_axis(table, index, axis=1, mode="promise_in_bounds")


def pick(tables, ids, fold, top):
    tile, lane = ids >> 7, ids & (LANES - 1)
    half = lax.broadcasted_iota(jnp.int32, ids.shape, 1) // top
    picked = jnp.zeros(ids.shape, F32)
    for part in range(fold):
        here = jnp.where(half == part, tile, -1)
        for j, table in enumerate(tables(part)):
            picked = jnp.where(here == j, lookup(table, lane), picked)
    return picked


def spread_row(table, p, top, tiles, slots):
    rows = table.shape[0]
    table = jnp.concatenate([table[:, p * top : (p + 1) * top], jnp.zeros((rows, LANES - top), F32)], axis=1)
    return jnp.concatenate([lookup(table, slots(j)) for j in range(tiles)], axis=1)


def step_kernel(
    W, N, fold, top, chunk, pieces, early,
    ids_hbm, bias_hbm, shift_hbm, act_hbm, enc_hbm, dec_hbm,
    dg_ref, sum_ref, own_slot_ref,
    ids_t_ref, bias_ref, shift_ref, ids, act, enc, dec, slot, total, part, wide_in, values, lat, lat_t,
    err, lg_packed, grad_in,
    load_sem, ws1, wr1, ws2, wr2, ws3, wr3, *scratch,
):
    wide, narrow = lax.axis_index("wide"), lax.axis_index("narrow")
    tokens, latents = lat.shape
    channels = act.shape[1]
    own, rows = tokens // N, part.shape[1]
    chunks = channels // chunk
    piece = latents // pieces
    low = narrow * latents
    half_rows, quarter = tokens // 2, tokens // 4
    near = wide // (W // 2)

    def mate(d):
        goal = 0
        for b in range(W.bit_length() - 1):
            digit = wide // 2**b % 2
            goal = goal + 2**b * (1 - digit if d >> b & 1 else digit)
        return goal

    def rows_of(h):
        return pl.ds(pl.multiple_of(h * half_rows, half_rows), half_rows)

    def piece_cols(n):
        return pl.ds(pl.multiple_of(n * piece, LANES), piece)

    def load(source, target, i):
        return pltpu.make_async_copy(source, target, load_sem.at[i])

    def load_act(h, i):
        return load(act_hbm.at[rows_of(h)], act.at[rows_of(h)], i)

    load_dec = load(dec_hbm, dec, 1)
    load_ids = load(ids_hbm, ids_t_ref, 2)
    load_bias = load(bias_hbm, bias_ref, 3)
    load_shift = load(shift_hbm, shift_ref, 4)

    def load_enc(n):
        return load(enc_hbm.at[:, piece_cols(n)], enc.at[:, piece_cols(n)], 5 + n)

    barrier = pltpu.get_barrier_semaphore()
    for d in range(1, W):
        pl.semaphore_signal(barrier, inc=1, device_id={"wide": mate(d)}, device_id_type=MESH)
    for d in range(1, N):
        pl.semaphore_signal(barrier, inc=1, device_id={"narrow": lax.rem(narrow + d, N)}, device_id_type=MESH)

    load_ids.start()
    load_act(1 - near, 0).start()
    for n in range(AHEAD):
        load_enc(n).start()
    load_act(near, 5 + pieces).start()
    load_bias.start()
    load_shift.start()

    load_ids.wait()
    for n in range(AHEAD, pieces):
        load_enc(n).start()
    stacked = jnp.concatenate([ids_t_ref[...]] * fold, axis=0)
    ids[...] = stacked.T

    GROUP, TALL = 16, 256
    bands = latents // TALL
    groups = bands * (tokens // LANES)

    def fill_slots(i, slot, low):
        band, side = i % bands, i // bands
        at = pl.ds(pl.multiple_of(side * LANES, LANES), LANES)
        offset = low + band * TALL
        place = lax.broadcasted_iota(jnp.int32, (GROUP, LANES), 0)
        places = [(place + j * GROUP).astype(jnp.int16) for j in range(TALL // GROUP)]
        found = [jnp.full((GROUP, LANES), top, jnp.int16) for _ in places]
        for k in range(top):
            here = jnp.broadcast_to(ids_t_ref[k : k + 1, at] - offset, (GROUP, LANES)).astype(jnp.int16)
            found = [jnp.where(here == p, jnp.int16(k), f) for p, f in zip(places, found)]
        slot[at, pl.ds(pl.multiple_of(band * TALL, TALL), TALL)] = jnp.concatenate(found, axis=0).T.astype(jnp.int32)

    def slots_of(i, carry):
        fill_slots(i, slot, low)
        return carry

    pl.semaphore_wait(barrier, W + N - 2)

    def narrow_copy(goal, source, target, send, recv):
        return pltpu.make_async_remote_copy(
            src_ref=source, dst_ref=target, send_sem=send, recv_sem=recv,
            device_id={"narrow": goal}, device_id_type=MESH,
        )

    def wide_copy(d, source, target, send, recv):
        return pltpu.make_async_remote_copy(
            src_ref=source, dst_ref=target, send_sem=send, recv_sem=recv,
            device_id={"wide": mate(d)}, device_id_type=MESH,
        )

    def columns(c):
        return pl.ds(pl.multiple_of(c * chunk, chunk), chunk)

    if early:
        (
            dec_in, slot_in, values_in, lat_in, rec, rec_in, msg, msg_in, err_out, full, full_in, base,
            ds, dr, vs, vr, vws, vwr, ns1, nr1, ns2, nr2, ns3, nr3, fs, fr,
        ) = scratch
        side, pair = lax.rem(narrow, 2), narrow // 2
        across, along = narrow + 1 - 2 * side, narrow + 2 - 4 * pair
        plain = chunks - early

        PARTS = 1
        tall = latents // PARTS

        def dec_copy(i):
            c, at = i // PARTS, pl.ds(i % PARTS * tall, tall)
            return narrow_copy(
                across, dec_hbm.at[at, columns(plain + c)], dec_in.at[at, columns(c)], ds.at[i], dr.at[i]
            )

        for i in range(early * PARTS):
            dec_copy(i).start()
    else:
        rec, rec_in, err_out, ns1, nr1, ns2, nr2 = scratch

    lax.fori_loop(0, groups // HEAD, slots_of, 0)
    load_act(1 - near, 0).wait()

    def encode(h, n):
        total[rows_of(h), piece_cols(n)] = jnp.dot(
            act[rows_of(h), :], enc[:, piece_cols(n)], preferred_element_type=F32
        )

    def encode_far(n, carry):
        load_enc(n).wait()
        encode(1 - near, n)
        return carry

    def encode_near(n, carry):
        encode(near, n)
        return carry

    half = lax.broadcasted_iota(jnp.int32, (rows, LANES), 1) // top

    def block_rows(w, p):
        return pl.ds(pl.multiple_of((w * fold + p) * rows, rows), rows)

    def packed_ids(w):
        out = ids[block_rows(w, 0), :]
        for p in range(1, fold):
            out = jnp.where(half == p, ids[block_rows(w, p), :], out)
        return out - low

    def pick_dense(w):
        def tables(p):
            return [total[block_rows(w, p), j * LANES : (j + 1) * LANES] for j in range(latents // LANES)]

        return pick(tables, packed_ids(w), fold, top)

    def scatter_copy(d, source, target, send, recv):
        return wide_copy(d, source.at[d - 1], target.at[d - 1], send.at[0], recv.at[0])

    def scatter_all(source, target, send, recv):
        return wide_copy(1, source, target, send.at[0], recv.at[0])

    def scatter(first, last, source, target, send, recv):
        picked = None
        for d in range(last - 1, first - 1, -1):
            picked = pick_dense(mate(d))
            if d > 0:
                source[d - 1] = picked.astype(BF16)
                scatter_copy(d, source, target, send, recv).start()
        return picked

    def gather(picked, source, target, send, recv):
        scatter_all(source, target, send, recv).wait_recv()
        for d in range(1, W):
            picked = picked + target[d - 1].astype(F32)
        return picked

    lax.fori_loop(0, pieces, encode_far, 0)
    load_dec.start()
    scatter(W // 2, W, part, wide_in, ws1, wr1)
    load_act(near, 5 + pieces).wait()
    lax.fori_loop(0, pieces, encode_near, 0)
    summed = scatter(0, W // 2, part, wide_in, ws1, wr1)

    def bias_tables(p):
        return [jnp.broadcast_to(bias_ref[:, j * LANES : (j + 1) * LANES], (rows, LANES)) for j in range(latents // LANES)]

    load_bias.wait()
    load_shift.wait()
    summed = summed + pick(bias_tables, packed_ids(wide), fold, top)

    lax.fori_loop(groups // HEAD, groups * TURN // 16, slots_of, 0)

    values[wide] = gather(summed, part, wide_in, ws1, wr1).astype(BF16)

    def value_copy(d):
        return wide_copy(d, values.at[wide], values.at[wide], ws2.at[0], wr2.at[d // (W // 2)])

    def values_of(ref, first, last, send, recv):
        blocks = ref.at[pl.ds(0, last - first)]
        return wide_copy(1, blocks, blocks, send, recv)

    for d in (*range(1, W // 2), *range(W - 1, W // 2 - 1, -1)):
        value_copy(d).start()
    if early:
        def pair_values():
            return narrow_copy(across, values.at[wide], values_in.at[wide], vs.at[0], vr.at[0])

        pair_values().start()

    lax.fori_loop(groups * TURN // 16, groups, slots_of, 0)

    def fill_block(block, values, slot, lat):
        table = values[block].astype(F32)
        for p in range(fold):
            at = block_rows(block, p)
            spread = spread_row(table, p, top, latents // LANES, lambda j: slot[at, j * LANES : (j + 1) * LANES])
            lat[at, :] = spread.astype(BF16)

    def fill_mates(first, last, group):
        values_of(values, first, last, ws2.at[0], wr2.at[group]).wait_recv()
        for d in range(first, last):
            fill_block(mate(d), values, slot, lat)

    load_dec.wait()

    def own_rows(i):
        return pl.ds(pl.multiple_of(i * own, own), own)

    def keep_slots():
        own_slot_ref[...] = slot[pl.ds(pl.multiple_of(wide * (fold * rows), fold * rows), fold * rows), :]

    def flip(j, carry):
        at = pl.ds(pl.multiple_of(j * LANES, LANES), LANES)
        lat_t[at, :] = lat[:, at].T
        return carry

    def decode(c, at=slice(None)):
        return jnp.dot(lat[at, :], dec[:, columns(c)], preferred_element_type=F32)

    def contract(c, at=slice(None)):
        return lax.dot_general(
            err[at, columns(c)], dec[:, columns(c)], (((1,), (1,)), ((), ())), preferred_element_type=F32
        )

    def outer(c):
        dg_ref[:, columns(c)] = jnp.dot(lat_t[...], err[:, columns(c)], preferred_element_type=F32).astype(BF16)

    def local_chunk(c, carry):
        total[...] += contract(c)
        outer(c)
        return carry

    if early:
        def here(h):
            return pl.ds(pl.multiple_of(h * half_rows + side * quarter, quarter), quarter)

        def scale(count):
            return count.astype(F32)

        own_scale, mate_scale = scale(N - narrow), scale(N - across)
        least = scale(N - jnp.maximum(narrow, across))
        own_use, mate_use = scale(1 + pair * (N - 1 - narrow)), scale(1 + pair * (N - 1 - across))

        def rec_copy(c, q):
            h = near if q == 0 else 1 - near
            return narrow_copy(across, rec.at[c, h, 1 - side], rec_in.at[c, h], ns1.at[0], nr1.at[c])

        def msg_copy(c):
            return narrow_copy(along, msg.at[c], msg_in.at[c], ns2.at[0], nr2.at[c])

        def err_copy(c, h, q):
            at = c + q if c == plain - 1 else c
            return narrow_copy(across, err_out.at[c, h], err.at[here(h), columns(c)], ns3.at[0], nr3.at[at])

        def full_copy(c):
            return narrow_copy(along, full.at[c], full_in.at[c], fs.at[c], fr.at[c])

        def send_part(c, q):
            h = near if q == 0 else 1 - near
            rec[c, h] = decode(c, rows_of(h)).astype(BF16).reshape(2, quarter, chunk)
            rec_copy(c, q).start()

        def send_rec(c, carry):
            rec[c] = decode(c).astype(BF16).reshape(2, 2, quarter, chunk)
            for q in range(2):
                rec_copy(c, q).start()
            return carry

        fill_block(wide, values, slot, lat)
        fill_mates(1, W // 2, 0)
        for c in range(FIRST):
            send_part(c, 0)
        fill_mates(W // 2, W, 1)
        for c in range(FIRST):
            send_part(c, 1)
        lax.fori_loop(FIRST, plain, send_rec, 0)

        def more_slots(i, carry):
            fill_slots(i, slot_in, across * latents)
            return carry

        def send_msg(c):
            narrow_copy(across, rec_in.at[c], rec_in.at[c], ns1.at[0], nr1.at[c]).wait_recv()
            msg[c] = (own_use * rec[c, :, side].astype(F32) + mate_use * rec_in[c].astype(F32)).astype(BF16)
            msg_copy(c).start()

        def send_err(c):
            msg_copy(c).wait_recv()
            for q, h in enumerate((1 - near, near)):
                shift = shift_ref[:, columns(c)] - act[here(h), columns(c)].astype(F32)
                mine_rec, mate_rec = rec[c, h, side].astype(F32), rec_in[c, h].astype(F32)
                other = msg_in[c, h].astype(F32)
                back = mate_scale * (shift + mate_rec) + least * mine_rec + mate_use * other
                err_out[c, h] = (back / N).astype(BF16)
                err_copy(c, h, q).start()
                back = own_scale * (shift + mine_rec) + least * mate_rec + own_use * other
                err[here(h), columns(c)] = (back / N).astype(BF16)

        def send_full(c, carry):
            mine_rec = decode(plain + c)
            mate_rec = jnp.dot(lat_in[...], dec_in[:, columns(c)], preferred_element_type=F32)
            full[c] = (own_use * mine_rec + mate_use * mate_rec).astype(BF16)
            full_copy(c).start()
            shift = shift_ref[:, columns(plain + c)] - act[:, columns(plain + c)].astype(F32)
            base[c] = own_scale * (shift + mine_rec) + least * mate_rec
            return carry

        def take_full(c, carry):
            full_copy(c).wait_recv()
            err[:, columns(plain + c)] = ((base[c] + own_use * full_in[c].astype(F32)) / N).astype(BF16)
            return carry

        def values_copies():
            return [wide_copy(d, values_in.at[wide], values_in.at[wide], vws.at[0], vwr.at[0]) for d in range(1, W)]

        def values_all():
            return values_of(values_in, 1, W, vws.at[0], vwr.at[0])

        def arrive_last(q):
            half = err_out.at[plain - 1, 0]
            narrow_copy(across, half, half, ns3.at[0], nr3.at[plain - 1 + q]).wait_recv()

        def arrive(c):
            narrow_copy(across, err_out.at[c], err_out.at[c], ns3.at[0], nr3.at[c]).wait_recv()

        def take(c):
            arrive(c)
            local_chunk(c, 0)

        pair_values().wait_recv()
        for copy in values_copies():
            copy.start()
        keep_slots()
        lax.fori_loop(0, latents // LANES, flip, 0)
        total[...] = jnp.zeros_like(total)
        lax.fori_loop(0, groups // 2, more_slots, 0)
        for c in range(plain):
            send_msg(c)
            if c >= LAG:
                send_err(c - LAG)
            if c < 2:
                lax.fori_loop((2 + c) * groups // 4, (3 + c) * groups // 4, more_slots, 0)
            if c == 2:
                values_all().wait_recv()
                for block in range(W):
                    fill_block(block, values_in, slot_in, lat_in)
        for i in range(early * PARTS):
            dec_copy(i).wait_recv()
        lax.fori_loop(0, early, send_full, 0)
        for c in range(LAG):
            send_err(plain - LAG + c)
            take(c)


        def finish():
            narrow_copy(across, rec_in, rec_in, ns1.at[0], nr1.at[0]).wait_send()
            narrow_copy(along, msg, msg, ns2.at[0], nr2.at[0]).wait_send()
            narrow_copy(across, err_out, err_out, ns3.at[0], nr3.at[0]).wait_send()
            for i in range(early * PARTS):
                dec_copy(i).wait_send()
            for c in range(early):
                full_copy(c).wait_send()
            pair_values().wait_send()
            values_all().wait_send()
    else:
        plain = chunks
        fill_block(wide, values, slot, lat)
        fill_mates(1, W // 2, 0)
        fill_mates(W // 2, W, 1)
        keep_slots()

        def goal_of(d):
            return lax.rem(narrow + d, N)

        def rec_copy(c, d):
            return narrow_copy(goal_of(d), rec.at[c, goal_of(d)], rec_in.at[c, d], ns1.at[c, d], nr1.at[c, d])

        def err_copy(c, d):
            return narrow_copy(
                goal_of(d), err_out.at[c, d], err.at[own_rows(narrow), columns(c)], ns2.at[c, d], nr2.at[c, d]
            )

        def send_rec(c, carry):
            rec[c] = decode(c).astype(BF16).reshape(N, own, chunk)
            for d in range(1, N):
                rec_copy(c, d).start()
            return carry

        lax.fori_loop(0, chunks, send_rec, 0)

        def combine(c, carry):
            for d in range(1, N):
                rec_copy(c, d).wait_recv()
            shift = shift_ref[:, columns(c)] - act[own_rows(narrow), columns(c)].astype(F32)
            terms = [rec[c, narrow].astype(F32)]
            terms += [rec_in[c, d].astype(F32) for d in range(1, N)]
            for e in range(N):
                goal = goal_of(e)
                back = (N - goal).astype(F32) * shift
                for d in range(N):
                    origin = lax.rem(narrow + N - d, N)
                    back = back + (N - jnp.maximum(goal, origin)).astype(F32) * terms[d]
                back = (back / N).astype(BF16)
                if e == 0:
                    err[own_rows(narrow), columns(c)] = back
                else:
                    err_out[c, e] = back
                    err_copy(c, e).start()
            return carry

        lax.fori_loop(0, chunks, combine, 0)
        lax.fori_loop(0, latents // LANES, flip, 0)

        def arrive_last(q):
            if q == 0:
                arrive(plain - 1)

        def arrive(c):
            for d in range(1, N):
                err_copy(c, d).wait_recv()

        def finish_chunk(c, carry):
            for d in range(1, N):
                rec_copy(c, d).wait_send()
                err_copy(c, d).wait_send()
            return carry

        def finish():
            lax.fori_loop(0, plain, finish_chunk, 0)

    def sent_chunk(c, carry):
        arrive(c)
        return local_chunk(c, carry)

    if early:
        lax.fori_loop(LAG, plain - 1, sent_chunk, 0)
        lax.fori_loop(0, early, take_full, 0)
        lax.fori_loop(plain, chunks, local_chunk, 0)
    else:
        total[...] = jnp.zeros_like(total)
        lax.fori_loop(0, plain - 1, sent_chunk, 0)
    arrive_last(0)
    total[rows_of(1 - near), :] += contract(plain - 1, rows_of(1 - near))
    scatter(W // 2, W, lg_packed, grad_in, ws3, wr3)
    arrive_last(1)
    total[rows_of(near), :] += contract(plain - 1, rows_of(near))
    summed = scatter(0, W // 2, lg_packed, grad_in, ws3, wr3)
    outer(plain - 1)
    sum_ref[...] = gather(summed, lg_packed, grad_in, ws3, wr3)

    scatter_all(part, wide_in, ws1, wr1).wait_send()
    values_of(values, 1, W, ws2.at[0], wr2.at[0]).wait_send()
    scatter_all(lg_packed, grad_in, ws3, wr3).wait_send()

    finish()


STORES = 1
AHEAD, HEAD, TURN = 1, 8, 9
FIRST, LAG = 3, 3


def store_kernel(fold, top, dg_ref, sum_ref, slot_ref, dg_hbm, grad_hbm, grad_ref, sem):
    step = dg_ref.shape[0] // STORES
    rows = sum_ref.shape[0]
    copies = []
    for i in range(STORES):
        at = pl.ds(i * step, step)
        copies.append(pltpu.make_async_copy(dg_ref.at[at], dg_hbm.at[at], sem.at[i]))
    for copy in copies:
        copy.start()
    for p in range(fold):
        at = slice(p * rows, (p + 1) * rows)
        grad_ref[at, :] = spread_row(sum_ref[...], p, top, slot_ref.shape[1] // LANES, lambda j: slot_ref[at, j * LANES : (j + 1) * LANES])
    copies.append(pltpu.make_async_copy(grad_ref, grad_hbm, sem.at[STORES]))
    copies[-1].start()
    for copy in copies:
        copy.wait()


def local(activations, enc_weight, enc_bias, dec_weight, dec_bias, active_ids):
    W, N = lax.axis_size("wide"), lax.axis_size("narrow")
    tokens, channels = activations.shape
    latents = enc_weight.shape[1]
    top = active_ids.shape[1]
    fold = LANES // top
    rows = tokens // W // fold
    chunk = min(channels, 256)
    chunks = channels // chunk
    pieces = 1
    own = tokens // N
    early = chunks // 8 if N == 4 else 0
    plain = chunks - early
    half = (plain, 2, tokens // 4, chunk)
    packed_shape, mates_shape = (W, rows, LANES), (W - 1, rows, LANES)
    vmem = pl.BlockSpec(memory_space=pltpu.VMEM)
    hbm = pl.BlockSpec(memory_space=pl.ANY)
    dma = pltpu.SemaphoreType.DMA
    if early:
        scratch = [
            pltpu.VMEM((latents, early * chunk), BF16),
            pltpu.VMEM((tokens, latents), jnp.int32),
            pltpu.VMEM(packed_shape, BF16),
            pltpu.VMEM((tokens, latents), BF16),
            pltpu.VMEM((plain, 2, 2, tokens // 4, chunk), BF16),
            *[pltpu.VMEM(half, BF16)] * 4,
            *[pltpu.VMEM((early, tokens, chunk), BF16)] * 2,
            pltpu.VMEM((early, tokens, chunk), F32),
            dma((early,)), dma((early,)), *[dma((1,))] * 4,
            *[dma((1,)), dma((plain,))] * 2, dma((1,)), dma((plain + 1,)),
            dma((early,)), dma((early,)),
        ]
    else:
        scratch = [*[pltpu.VMEM((chunks, N, own, chunk), BF16)] * 3, *[dma((chunks, N))] * 4]
    dec_grad, summed, slots = pl.pallas_call(
        functools.partial(step_kernel, W, N, fold, top, chunk, pieces, early),
        out_shape=(
            pltpu.VMEM((latents, channels), BF16),
            pltpu.VMEM((rows, LANES), F32),
            pltpu.VMEM((tokens // W, latents), jnp.int32),
        ),
        in_specs=[hbm] * 6,
        out_specs=(vmem, vmem, vmem),
        scratch_shapes=[
            pltpu.VMEM((top, tokens), jnp.int32),
            pltpu.VMEM((1, latents), F32),
            pltpu.VMEM((1, channels), F32),
            pltpu.VMEM((tokens, LANES), jnp.int32),
            pltpu.VMEM((tokens, channels), BF16),
            pltpu.VMEM((channels, latents), BF16),
            pltpu.VMEM((latents, channels), BF16),
            pltpu.VMEM((tokens, latents), jnp.int32),
            pltpu.VMEM((tokens, latents), F32),
            pltpu.VMEM(mates_shape, BF16),
            pltpu.VMEM(mates_shape, BF16),
            pltpu.VMEM(packed_shape, BF16),
            pltpu.VMEM((tokens, latents), BF16),
            pltpu.VMEM((latents, tokens), BF16),
            pltpu.VMEM((tokens, channels), BF16),
            pltpu.VMEM(mates_shape, BF16),
            pltpu.VMEM(mates_shape, BF16),
            dma((6 + pieces,)),
            dma((1,)), dma((1,)), dma((1,)), dma((2,)), dma((1,)), dma((1,)),
            *scratch,
        ],
        compiler_params=pltpu.CompilerParams(collective_id=0, has_side_effects=True, vmem_limit_bytes=56 * 2**20),
        cost_estimate=pl.CostEstimate(
            flops=8 * tokens * channels * latents, bytes_accessed=6 * channels * (tokens + latents), transcendentals=0
        ),
        name="step",
    )(active_ids.T, enc_bias.reshape(1, -1), dec_bias.reshape(1, -1), activations, enc_weight, dec_weight)
    resident = [pltpu.with_memory_space_constraint(x, pltpu.VMEM) for x in (dec_grad, summed, slots)]
    return pl.pallas_call(
        functools.partial(store_kernel, fold, top),
        out_shape=(
            jax.ShapeDtypeStruct((latents, channels), BF16),
            jax.ShapeDtypeStruct((tokens // W, latents), F32),
        ),
        in_specs=[vmem, vmem, vmem],
        out_specs=(hbm, hbm),
        scratch_shapes=[pltpu.VMEM((tokens // W, latents), F32), dma((STORES + 1,))],
        compiler_params=pltpu.CompilerParams(vmem_limit_bytes=2**20),
        name="store",
    )(*resident)


def solution(mesh):
    in_specs = (
        P(None, "wide"),
        P("wide", "narrow"),
        P("narrow"),
        P("narrow", "wide"),
        P("wide"),
        P(),
    )
    out_specs = (P("narrow", "wide"), P("wide", "narrow"))
    return jax.shard_map(local, mesh=mesh, in_specs=in_specs, out_specs=out_specs, check_vma=False)
```

```python
import functools

import jax
import jax.numpy as jnp
from jax import lax
from jax.experimental import pallas as pl
from jax.experimental.pallas import tpu as pltpu
from jax.sharding import PartitionSpec as P

LANES = 128
MESH = pl.DeviceIdType.MESH
F32, BF16 = jnp.float32, jnp.bfloat16


def lookup(table, index):
    return jnp.take_along_axis(table, index, axis=1, mode="promise_in_bounds")


def pick(tables, ids, fold, top):
    tile, lane = ids >> 7, ids & (LANES - 1)
    half = lax.broadcasted_iota(jnp.int32, ids.shape, 1) // top
    picked = jnp.zeros(ids.shape, F32)
    for part in range(fold):
        here = jnp.where(half == part, tile, -1)
        for j, table in enumerate(tables(part)):
            picked = jnp.where(here == j, lookup(table, lane), picked)
    return picked


def spread_row(table, p, top, tiles, slots):
    rows = table.shape[0]
    table = jnp.concatenate([table[:, p * top : (p + 1) * top], jnp.zeros((rows, LANES - top), F32)], axis=1)
    return jnp.concatenate([lookup(table, slots(j)) for j in range(tiles)], axis=1)


def step_kernel(
    W, N, fold, top, chunk, pieces, early,
    ids_hbm, bias_hbm, shift_hbm, act_hbm, enc_hbm, dec_hbm,
    dg_ref, sum_ref, own_slot_ref,
    ids_t_ref, bias_ref, shift_ref, ids, act, enc, dec, slot, total, part, wide_in, values, lat, lat_t,
    err, lg_packed, grad_in,
    load_sem, ws1, wr1, ws2, wr2, ws3, wr3, *scratch,
):
    wide, narrow = lax.axis_index("wide"), lax.axis_index("narrow")
    tokens, latents = lat.shape
    channels = act.shape[1]
    own, rows = tokens // N, part.shape[1]
    chunks = channels // chunk
    piece = latents // pieces
    low = narrow * latents
    half_rows, quarter = tokens // 2, tokens // 4
    near = wide // (W // 2)

    def mate(d):
        goal = 0
        for b in range(W.bit_length() - 1):
            digit = wide // 2**b % 2
            goal = goal + 2**b * (1 - digit if d >> b & 1 else digit)
        return goal

    def rows_of(h):
        return pl.ds(pl.multiple_of(h * half_rows, half_rows), half_rows)

    def piece_cols(n):
        return pl.ds(pl.multiple_of(n * piece, LANES), piece)

    def load(source, target, i):
        return pltpu.make_async_copy(source, target, load_sem.at[i])

    def load_act(h, i):
        return load(act_hbm.at[rows_of(h)], act.at[rows_of(h)], i)

    load_dec = load(dec_hbm, dec, 1)
    load_ids = load(ids_hbm, ids_t_ref, 2)
    load_bias = load(bias_hbm, bias_ref, 3)
    load_shift = load(shift_hbm, shift_ref, 4)

    def load_enc(n):
        return load(enc_hbm.at[:, piece_cols(n)], enc.at[:, piece_cols(n)], 5 + n)

    barrier = pltpu.get_barrier_semaphore()
    for d in range(1, W):
        pl.semaphore_signal(barrier, inc=1, device_id={"wide": mate(d)}, device_id_type=MESH)
    for d in range(1, N):
        pl.semaphore_signal(barrier, inc=1, device_id={"narrow": lax.rem(narrow + d, N)}, device_id_type=MESH)

    load_ids.start()
    load_act(1 - near, 0).start()
    for n in range(AHEAD):
        load_enc(n).start()
    load_act(near, 5 + pieces).start()
    load_bias.start()
    load_shift.start()

    load_ids.wait()
    for n in range(AHEAD, pieces):
        load_enc(n).start()
    stacked = jnp.concatenate([ids_t_ref[...]] * fold, axis=0)
    ids[...] = stacked.T

    GROUP, TALL = 16, 256
    bands = latents // TALL
    groups = bands * (tokens // LANES)

    def fill_slots(i, slot, low):
        band, side = i % bands, i // bands
        at = pl.ds(pl.multiple_of(side * LANES, LANES), LANES)
        offset = low + band * TALL
        place = lax.broadcasted_iota(jnp.int32, (GROUP, LANES), 0)
        places = [(place + j * GROUP).astype(jnp.int16) for j in range(TALL // GROUP)]
        found = [jnp.full((GROUP, LANES), top, jnp.int16) for _ in places]
        for k in range(top):
            here = jnp.broadcast_to(ids_t_ref[k : k + 1, at] - offset, (GROUP, LANES)).astype(jnp.int16)
            found = [jnp.where(here == p, jnp.int16(k), f) for p, f in zip(places, found)]
        slot[at, pl.ds(pl.multiple_of(band * TALL, TALL), TALL)] = jnp.concatenate(found, axis=0).T.astype(jnp.int32)

    def slots_of(i, carry):
        fill_slots(i, slot, low)
        return carry

    pl.semaphore_wait(barrier, W + N - 2)

    def narrow_copy(goal, source, target, send, recv):
        return pltpu.make_async_remote_copy(
            src_ref=source, dst_ref=target, send_sem=send, recv_sem=recv,
            device_id={"narrow": goal}, device_id_type=MESH,
        )

    def wide_copy(d, source, target, send, recv):
        return pltpu.make_async_remote_copy(
            src_ref=source, dst_ref=target, send_sem=send, recv_sem=recv,
            device_id={"wide": mate(d)}, device_id_type=MESH,
        )

    def columns(c):
        return pl.ds(pl.multiple_of(c * chunk, chunk), chunk)

    if early:
        (
            dec_in, slot_in, values_in, lat_in, rec, rec_in, msg, msg_in, err_out, full, full_in, base,
            ds, dr, vs, vr, vws, vwr, ns1, nr1, ns2, nr2, ns3, nr3, fs, fr,
        ) = scratch
        side, pair = lax.rem(narrow, 2), narrow // 2
        across, along = narrow + 1 - 2 * side, narrow + 2 - 4 * pair
        plain = chunks - early

        PARTS = 1
        tall = latents // PARTS

        def dec_copy(i):
            c, at = i // PARTS, pl.ds(i % PARTS * tall, tall)
            return narrow_copy(
                across, dec_hbm.at[at, columns(plain + c)], dec_in.at[at, columns(c)], ds.at[i], dr.at[i]
            )

        for i in range(early * PARTS):
            dec_copy(i).start()
    else:
        rec, rec_in, err_out, ns1, nr1, ns2, nr2 = scratch

    lax.fori_loop(0, groups // HEAD, slots_of, 0)
    load_act(1 - near, 0).wait()

    def encode(h, n):
        total[rows_of(h), piece_cols(n)] = jnp.dot(
            act[rows_of(h), :], enc[:, piece_cols(n)], preferred_element_type=F32
        )

    def encode_far(n, carry):
        load_enc(n).wait()
        encode(1 - near, n)
        return carry

    def encode_near(n, carry):
        encode(near, n)
        return carry

    half = lax.broadcasted_iota(jnp.int32, (rows, LANES), 1) // top

    def block_rows(w, p):
        return pl.ds(pl.multiple_of((w * fold + p) * rows, rows), rows)

    def packed_ids(w):
        out = ids[block_rows(w, 0), :]
        for p in range(1, fold):
            out = jnp.where(half == p, ids[block_rows(w, p), :], out)
        return out - low

    def pick_dense(w):
        def tables(p):
            return [total[block_rows(w, p), j * LANES : (j + 1) * LANES] for j in range(latents // LANES)]

        return pick(tables, packed_ids(w), fold, top)

    def scatter_copy(d, source, target, send, recv):
        return wide_copy(d, source.at[d - 1], target.at[d - 1], send.at[0], recv.at[0])

    def scatter_all(source, target, send, recv):
        return wide_copy(1, source, target, send.at[0], recv.at[0])

    def scatter(first, last, source, target, send, recv):
        picked = None
        for d in range(last - 1, first - 1, -1):
            picked = pick_dense(mate(d))
            if d > 0:
                source[d - 1] = picked.astype(BF16)
                scatter_copy(d, source, target, send, recv).start()
        return picked

    def gather(picked, source, target, send, recv):
        scatter_all(source, target, send, recv).wait_recv()
        for d in range(1, W):
            picked = picked + target[d - 1].astype(F32)
        return picked

    lax.fori_loop(0, pieces, encode_far, 0)
    load_dec.start()
    scatter(W // 2, W, part, wide_in, ws1, wr1)
    load_act(near, 5 + pieces).wait()
    lax.fori_loop(0, pieces, encode_near, 0)
    summed = scatter(0, W // 2, part, wide_in, ws1, wr1)

    def bias_tables(p):
        return [jnp.broadcast_to(bias_ref[:, j * LANES : (j + 1) * LANES], (rows, LANES)) for j in range(latents // LANES)]

    load_bias.wait()
    load_shift.wait()
    summed = summed + pick(bias_tables, packed_ids(wide), fold, top)

    lax.fori_loop(groups // HEAD, groups * TURN // 16, slots_of, 0)

    values[wide] = gather(summed, part, wide_in, ws1, wr1).astype(BF16)

    def value_copy(d):
        return wide_copy(d, values.at[wide], values.at[wide], ws2.at[0], wr2.at[d // (W // 2)])

    def values_of(ref, first, last, send, recv):
        blocks = ref.at[pl.ds(0, last - first)]
        return wide_copy(1, blocks, blocks, send, recv)

    for d in (*range(1, W // 2), *range(W - 1, W // 2 - 1, -1)):
        value_copy(d).start()
    if early:
        def pair_values():
            return narrow_copy(across, values.at[wide], values_in.at[wide], vs.at[0], vr.at[0])

        pair_values().start()

    lax.fori_loop(groups * TURN // 16, groups, slots_of, 0)

    def fill_block(block, values, slot, lat):
        table = values[block].astype(F32)
        for p in range(fold):
            at = block_rows(block, p)
            spread = spread_row(table, p, top, latents // LANES, lambda j: slot[at, j * LANES : (j + 1) * LANES])
            lat[at, :] = spread.astype(BF16)

    def fill_mates(first, last, group):
        values_of(values, first, last, ws2.at[0], wr2.at[group]).wait_recv()
        for d in range(first, last):
            fill_block(mate(d), values, slot, lat)

    load_dec.wait()

    def own_rows(i):
        return pl.ds(pl.multiple_of(i * own, own), own)

    def keep_slots():
        own_slot_ref[...] = slot[pl.ds(pl.multiple_of(wide * (fold * rows), fold * rows), fold * rows), :]

    def flip(j, carry):
        at = pl.ds(pl.multiple_of(j * LANES, LANES), LANES)
        lat_t[at, :] = lat[:, at].T
        return carry

    def decode(c, at=slice(None)):
        return jnp.dot(lat[at, :], dec[:, columns(c)], preferred_element_type=F32)

    def contract(c, at=slice(None)):
        return lax.dot_general(
            err[at, columns(c)], dec[:, columns(c)], (((1,), (1,)), ((), ())), preferred_element_type=F32
        )

    def outer(c):
        dg_ref[:, columns(c)] = jnp.dot(lat_t[...], err[:, columns(c)], preferred_element_type=F32).astype(BF16)

    def local_chunk(c, carry):
        total[...] += contract(c)
        outer(c)
        return carry

    if early:
        def here(h):
            return pl.ds(pl.multiple_of(h * half_rows + side * quarter, quarter), quarter)

        def scale(count):
            return count.astype(F32)

        own_scale, mate_scale = scale(N - narrow), scale(N - across)
        least = scale(N - jnp.maximum(narrow, across))
        own_use, mate_use = scale(1 + pair * (N - 1 - narrow)), scale(1 + pair * (N - 1 - across))

        def rec_copy(c, q):
            h = near if q == 0 else 1 - near
            return narrow_copy(across, rec.at[c, h, 1 - side], rec_in.at[c, h], ns1.at[0], nr1.at[c])

        def msg_copy(c):
            return narrow_copy(along, msg.at[c], msg_in.at[c], ns2.at[0], nr2.at[c])

        def err_copy(c, h, q):
            at = c + q if c == plain - 1 else c
            return narrow_copy(across, err_out.at[c, h], err.at[here(h), columns(c)], ns3.at[0], nr3.at[at])

        def full_copy(c):
            return narrow_copy(along, full.at[c], full_in.at[c], fs.at[c], fr.at[c])

        def send_part(c, q):
            h = near if q == 0 else 1 - near
            rec[c, h] = decode(c, rows_of(h)).astype(BF16).reshape(2, quarter, chunk)
            rec_copy(c, q).start()

        def send_rec(c, carry):
            rec[c] = decode(c).astype(BF16).reshape(2, 2, quarter, chunk)
            for q in range(2):
                rec_copy(c, q).start()
            return carry

        fill_block(wide, values, slot, lat)
        fill_mates(1, W // 2, 0)
        for c in range(FIRST):
            send_part(c, 0)
        fill_mates(W // 2, W, 1)
        for c in range(FIRST):
            send_part(c, 1)
        lax.fori_loop(FIRST, plain, send_rec, 0)

        def more_slots(i, carry):
            fill_slots(i, slot_in, across * latents)
            return carry

        def send_msg(c):
            narrow_copy(across, rec_in.at[c], rec_in.at[c], ns1.at[0], nr1.at[c]).wait_recv()
            msg[c] = (own_use * rec[c, :, side].astype(F32) + mate_use * rec_in[c].astype(F32)).astype(BF16)
            msg_copy(c).start()

        def send_err(c):
            msg_copy(c).wait_recv()
            for q, h in enumerate((1 - near, near)):
                shift = shift_ref[:, columns(c)] - act[here(h), columns(c)].astype(F32)
                mine_rec, mate_rec = rec[c, h, side].astype(F32), rec_in[c, h].astype(F32)
                other = msg_in[c, h].astype(F32)
                back = mate_scale * (shift + mate_rec) + least * mine_rec + mate_use * other
                err_out[c, h] = (back / N).astype(BF16)
                err_copy(c, h, q).start()
                back = own_scale * (shift + mine_rec) + least * mate_rec + own_use * other
                err[here(h), columns(c)] = (back / N).astype(BF16)

        def send_full(c, carry):
            mine_rec = decode(plain + c)
            mate_rec = jnp.dot(lat_in[...], dec_in[:, columns(c)], preferred_element_type=F32)
            full[c] = (own_use * mine_rec + mate_use * mate_rec).astype(BF16)
            full_copy(c).start()
            shift = shift_ref[:, columns(plain + c)] - act[:, columns(plain + c)].astype(F32)
            base[c] = own_scale * (shift + mine_rec) + least * mate_rec
            return carry

        def take_full(c, carry):
            full_copy(c).wait_recv()
            err[:, columns(plain + c)] = ((base[c] + own_use * full_in[c].astype(F32)) / N).astype(BF16)
            return carry

        def values_copies():
            return [wide_copy(d, values_in.at[wide], values_in.at[wide], vws.at[0], vwr.at[0]) for d in range(1, W)]

        def values_all():
            return values_of(values_in, 1, W, vws.at[0], vwr.at[0])

        def arrive_last(q):
            half = err_out.at[plain - 1, 0]
            narrow_copy(across, half, half, ns3.at[0], nr3.at[plain - 1 + q]).wait_recv()

        def arrive(c):
            narrow_copy(across, err_out.at[c], err_out.at[c], ns3.at[0], nr3.at[c]).wait_recv()

        def take(c):
            arrive(c)
            local_chunk(c, 0)

        pair_values().wait_recv()
        for copy in values_copies():
            copy.start()
        keep_slots()
        lax.fori_loop(0, latents // LANES, flip, 0)
        total[...] = jnp.zeros_like(total)
        lax.fori_loop(0, groups // 2, more_slots, 0)
        for c in range(plain):
            send_msg(c)
            if c >= LAG:
                send_err(c - LAG)
            if c < 2:
                lax.fori_loop((2 + c) * groups // 4, (3 + c) * groups // 4, more_slots, 0)
            if c == 2:
                values_all().wait_recv()
                for block in range(W):
                    fill_block(block, values_in, slot_in, lat_in)
        for i in range(early * PARTS):
            dec_copy(i).wait_recv()
        lax.fori_loop(0, early, send_full, 0)
        for c in range(LAG):
            send_err(plain - LAG + c)
            take(c)


        def finish():
            narrow_copy(across, rec_in, rec_in, ns1.at[0], nr1.at[0]).wait_send()
            narrow_copy(along, msg, msg, ns2.at[0], nr2.at[0]).wait_send()
            narrow_copy(across, err_out, err_out, ns3.at[0], nr3.at[0]).wait_send()
            for i in range(early * PARTS):
                dec_copy(i).wait_send()
            for c in range(early):
                full_copy(c).wait_send()
            pair_values().wait_send()
            values_all().wait_send()
    else:
        plain = chunks
        fill_block(wide, values, slot, lat)
        fill_mates(1, W // 2, 0)
        fill_mates(W // 2, W, 1)
        keep_slots()

        def goal_of(d):
            return lax.rem(narrow + d, N)

        def rec_copy(c, d):
            return narrow_copy(goal_of(d), rec.at[c, goal_of(d)], rec_in.at[c, d], ns1.at[c, d], nr1.at[c, d])

        def err_copy(c, d):
            return narrow_copy(
                goal_of(d), err_out.at[c, d], err.at[own_rows(narrow), columns(c)], ns2.at[c, d], nr2.at[c, d]
            )

        def send_rec(c, carry):
            rec[c] = decode(c).astype(BF16).reshape(N, own, chunk)
            for d in range(1, N):
                rec_copy(c, d).start()
            return carry

        lax.fori_loop(0, chunks, send_rec, 0)

        def combine(c, carry):
            for d in range(1, N):
                rec_copy(c, d).wait_recv()
            shift = shift_ref[:, columns(c)] - act[own_rows(narrow), columns(c)].astype(F32)
            terms = [rec[c, narrow].astype(F32)]
            terms += [rec_in[c, d].astype(F32) for d in range(1, N)]
            for e in range(N):
                goal = goal_of(e)
                back = (N - goal).astype(F32) * shift
                for d in range(N):
                    origin = lax.rem(narrow + N - d, N)
                    back = back + (N - jnp.maximum(goal, origin)).astype(F32) * terms[d]
                back = (back / N).astype(BF16)
                if e == 0:
                    err[own_rows(narrow), columns(c)] = back
                else:
                    err_out[c, e] = back
                    err_copy(c, e).start()
            return carry

        lax.fori_loop(0, chunks, combine, 0)
        lax.fori_loop(0, latents // LANES, flip, 0)

        def arrive_last(q):
            if q == 0:
                arrive(plain - 1)

        def arrive(c):
            for d in range(1, N):
                err_copy(c, d).wait_recv()

        def finish_chunk(c, carry):
            for d in range(1, N):
                rec_copy(c, d).wait_send()
                err_copy(c, d).wait_send()
            return carry

        def finish():
            lax.fori_loop(0, plain, finish_chunk, 0)

    def sent_chunk(c, carry):
        arrive(c)
        return local_chunk(c, carry)

    if early:
        lax.fori_loop(LAG, plain - 1, sent_chunk, 0)
        lax.fori_loop(0, early, take_full, 0)
        lax.fori_loop(plain, chunks, local_chunk, 0)
    else:
        total[...] = jnp.zeros_like(total)
        lax.fori_loop(0, plain - 1, sent_chunk, 0)
    arrive_last(0)
    total[rows_of(1 - near), :] += contract(plain - 1, rows_of(1 - near))
    scatter(W // 2, W, lg_packed, grad_in, ws3, wr3)
    arrive_last(1)
    total[rows_of(near), :] += contract(plain - 1, rows_of(near))
    summed = scatter(0, W // 2, lg_packed, grad_in, ws3, wr3)
    outer(plain - 1)
    sum_ref[...] = gather(summed, lg_packed, grad_in, ws3, wr3)

    scatter_all(part, wide_in, ws1, wr1).wait_send()
    values_of(values, 1, W, ws2.at[0], wr2.at[0]).wait_send()
    scatter_all(lg_packed, grad_in, ws3, wr3).wait_send()

    finish()


STORES = 1
AHEAD, HEAD, TURN = 1, 8, 8
FIRST, LAG = 3, 3


def store_kernel(fold, top, dg_ref, sum_ref, slot_ref, dg_hbm, grad_hbm, grad_ref, sem):
    step = dg_ref.shape[0] // STORES
    rows = sum_ref.shape[0]
    copies = []
    for i in range(STORES):
        at = pl.ds(i * step, step)
        copies.append(pltpu.make_async_copy(dg_ref.at[at], dg_hbm.at[at], sem.at[i]))
    for copy in copies:
        copy.start()
    for p in range(fold):
        at = slice(p * rows, (p + 1) * rows)
        grad_ref[at, :] = spread_row(sum_ref[...], p, top, slot_ref.shape[1] // LANES, lambda j: slot_ref[at, j * LANES : (j + 1) * LANES])
    copies.append(pltpu.make_async_copy(grad_ref, grad_hbm, sem.at[STORES]))
    copies[-1].start()
    for copy in copies:
        copy.wait()


def local(activations, enc_weight, enc_bias, dec_weight, dec_bias, active_ids):
    W, N = lax.axis_size("wide"), lax.axis_size("narrow")
    tokens, channels = activations.shape
    latents = enc_weight.shape[1]
    top = active_ids.shape[1]
    fold = LANES // top
    rows = tokens // W // fold
    chunk = min(channels, 256)
    chunks = channels // chunk
    pieces = 1
    own = tokens // N
    early = chunks // 8 if N == 4 else 0
    plain = chunks - early
    half = (plain, 2, tokens // 4, chunk)
    packed_shape, mates_shape = (W, rows, LANES), (W - 1, rows, LANES)
    vmem = pl.BlockSpec(memory_space=pltpu.VMEM)
    hbm = pl.BlockSpec(memory_space=pl.ANY)
    dma = pltpu.SemaphoreType.DMA
    if early:
        scratch = [
            pltpu.VMEM((latents, early * chunk), BF16),
            pltpu.VMEM((tokens, latents), jnp.int32),
            pltpu.VMEM(packed_shape, BF16),
            pltpu.VMEM((tokens, latents), BF16),
            pltpu.VMEM((plain, 2, 2, tokens // 4, chunk), BF16),
            *[pltpu.VMEM(half, BF16)] * 4,
            *[pltpu.VMEM((early, tokens, chunk), BF16)] * 2,
            pltpu.VMEM((early, tokens, chunk), F32),
            dma((early,)), dma((early,)), *[dma((1,))] * 4,
            *[dma((1,)), dma((plain,))] * 2, dma((1,)), dma((plain + 1,)),
            dma((early,)), dma((early,)),
        ]
    else:
        scratch = [*[pltpu.VMEM((chunks, N, own, chunk), BF16)] * 3, *[dma((chunks, N))] * 4]
    dec_grad, summed, slots = pl.pallas_call(
        functools.partial(step_kernel, W, N, fold, top, chunk, pieces, early),
        out_shape=(
            pltpu.VMEM((latents, channels), BF16),
            pltpu.VMEM((rows, LANES), F32),
            pltpu.VMEM((tokens // W, latents), jnp.int32),
        ),
        in_specs=[hbm] * 6,
        out_specs=(vmem, vmem, vmem),
        scratch_shapes=[
            pltpu.VMEM((top, tokens), jnp.int32),
            pltpu.VMEM((1, latents), F32),
            pltpu.VMEM((1, channels), F32),
            pltpu.VMEM((tokens, LANES), jnp.int32),
            pltpu.VMEM((tokens, channels), BF16),
            pltpu.VMEM((channels, latents), BF16),
            pltpu.VMEM((latents, channels), BF16),
            pltpu.VMEM((tokens, latents), jnp.int32),
            pltpu.VMEM((tokens, latents), F32),
            pltpu.VMEM(mates_shape, BF16),
            pltpu.VMEM(mates_shape, BF16),
            pltpu.VMEM(packed_shape, BF16),
            pltpu.VMEM((tokens, latents), BF16),
            pltpu.VMEM((latents, tokens), BF16),
            pltpu.VMEM((tokens, channels), BF16),
            pltpu.VMEM(mates_shape, BF16),
            pltpu.VMEM(mates_shape, BF16),
            dma((6 + pieces,)),
            dma((1,)), dma((1,)), dma((1,)), dma((2,)), dma((1,)), dma((1,)),
            *scratch,
        ],
        compiler_params=pltpu.CompilerParams(collective_id=0, has_side_effects=True, vmem_limit_bytes=56 * 2**20),
        cost_estimate=pl.CostEstimate(
            flops=8 * tokens * channels * latents, bytes_accessed=6 * channels * (tokens + latents), transcendentals=0
        ),
        name="step",
    )(active_ids.T, enc_bias.reshape(1, -1), dec_bias.reshape(1, -1), activations, enc_weight, dec_weight)
    resident = [pltpu.with_memory_space_constraint(x, pltpu.VMEM) for x in (dec_grad, summed, slots)]
    return pl.pallas_call(
        functools.partial(store_kernel, fold, top),
        out_shape=(
            jax.ShapeDtypeStruct((latents, channels), BF16),
            jax.ShapeDtypeStruct((tokens // W, latents), F32),
        ),
        in_specs=[vmem, vmem, vmem],
        out_specs=(hbm, hbm),
        scratch_shapes=[pltpu.VMEM((tokens // W, latents), F32), dma((STORES + 1,))],
        compiler_params=pltpu.CompilerParams(vmem_limit_bytes=2**20),
        name="store",
    )(*resident)


def solution(mesh):
    in_specs = (
        P(None, "wide"),
        P("wide", "narrow"),
        P("narrow"),
        P("narrow", "wide"),
        P("wide"),
        P(),
    )
    out_specs = (P("narrow", "wide"), P("wide", "narrow"))
    return jax.shard_map(local, mesh=mesh, in_specs=in_specs, out_specs=out_specs, check_vma=False)
```
